32 devices in a mesh: dp: 8 (over z, y), tensor: 4 (over x, core).
Axes of the slice: x: 2, y: 2, z: 4, core: 2. Of those that a mesh axis runs over, the one named last changes fastest.
Arguments:
- tokens: bfloat16 [8192, 1024], P('dp'), may hold values from -6 to 6
- cotangent: bfloat16 [8192, 1024], P('dp'), may hold values from -6 to 6
- norm_params: float32 [4, 1024], replicated, may hold values from 0.25 to 1.75
- attention_weight: bfloat16 [1024, 3, 1024], P('dp', None, 'tensor'), may hold values from -0.1875 to 0.1875
- attention_bias: float32 [3, 1024], P(None, 'tensor'), may hold values from -3 to 3
- merge_weight: bfloat16 [1024, 1024], P('dp', 'tensor'), may hold values from -1.5 to 1.5
- branch_bias: float32 [2, 1024], replicated, may hold values from -3 to 3
- up_weight: bfloat16 [1024, 4096], P('dp', 'tensor'), may hold values from -0.1875 to 0.1875
- up_bias: float32 [4096], P('tensor'), may hold values from -3 to 3
- down_weight: bfloat16 [1024, 4096], P('dp', 'tensor'), may hold values from -0.09375 to 0.09375
- prefix_ids: int32 [10], replicated, may hold values from 0 to 9, each once
- prefix_table: float32 [10, 1024], replicated, may hold values from -1.25 to 1.25
- encoder_weight: float32 [1024, 512], P('dp'), may hold values from -0.625 to 0.625
- encoder_bias: float32 [512], replicated, may hold values from -0.625 to 0.625
- decoder_weight: float32 [512, 2, 1024], P('dp', None, 'tensor'), may hold values from -0.625 to 0.625
- decoder_bias: float32 [2, 1024], P(None, 'tensor'), may hold values from -0.625 to 0.625
- first_table: float32 [10, 1024], replicated, may hold values from -1.9073486e-06 to 1.9073486e-06
- second_table: float32 [10, 1024], replicated, may hold values from 5.3138434e-15 to 8.5369944e-14
- first_encoder: float32 [1024, 512], P('dp'), may hold values from -5.9604645e-07 to 5.9604645e-07
- second_encoder: float32 [1024, 512], P('dp'), may hold values from 3.8329363e-16 to 6.0978533e-15
- first_encoder_bias: float32 [512], replicated, may hold values from -3.33786e-06 to 3.33786e-06
- second_encoder_bias: float32 [512], replicated, may hold values from 1.0540575e-14 to 1.6899766e-13
- first_decoder: float32 [512, 2, 1024], P('dp', None, 'tensor'), may hold values from -4.7683716e-07 to 4.7683716e-07
- second_decoder: float32 [512, 2, 1024], P('dp', None, 'tensor'), may hold values from 2.230072e-16 to 3.5716e-15
- first_decoder_bias: float32 [2, 1024], P(None, 'tensor'), may hold values from -9.536743e-07 to 9.536743e-07
- second_decoder_bias: float32 [2, 1024], P(None, 'tensor'), may hold values from 8.885443e-16 to 1.42864e-14
Outputs:
- output: bfloat16 [8192, 1024], P(('dp', 'tensor'))
- input_grad: bfloat16 [8192, 1024], P(('dp', 'tensor'))
- grad_norm: float32 [], replicated
- new_table: float32 [10, 1024], replicated
- new_first_table: float32 [10, 1024], replicated
- new_second_table: float32 [10, 1024], replicated
- new_encoder: float32 [1024, 512], P('dp')
- new_first_encoder: float32 [1024, 512], P('dp')
- new_second_encoder: float32 [1024, 512], P('dp')
- new_encoder_bias: float32 [512], replicated
- new_first_encoder_bias: float32 [512], replicated
- new_second_encoder_bias: float32 [512], replicated
- new_decoder: float32 [512, 2, 1024], P('dp', None, 'tensor')
- new_first_decoder: float32 [512, 2, 1024], P('dp', None, 'tensor')
- new_second_decoder: float32 [512, 2, 1024], P('dp', None, 'tensor')
- new_decoder_bias: float32 [2, 1024], P(None, 'tensor')
- new_first_decoder_bias: float32 [2, 1024], P(None, 'tensor')
- new_second_decoder_bias: float32 [2, 1024], P(None, 'tensor')
The draws below stay inside these ranges and needn't reach their ends.
Inputs may be any that keep to these rules, and one draw needn't show every extreme that they name: `prefix_ids`: every table row is used by exactly one prefix position.
All inputs are finite; a program needn't handle non-finite values.
Results may differ from the reference program's by a relative error of at most 0.017.
Values may be sent and summed in bfloat16 or wider, within the bound.
No kernel may reach another device: no remote copies, remote signals or barrier semaphores. Data moves between devices by JAX's collectives and lax.ppermute only.
A program may use at most 128 MiB of HBM per device.

```python
import math
import jax
import jax.numpy as jnp
from jax import lax

D = 1024
HEADS = 16
HD = 64
FF = 4096
PH = 512
PRE = 10
SEQ = 1024
STEP = 10
TOKENS = 8192
GRADSQ = 57397248


def levels(rng, dims, cuts, least, high):
    factor_of, own = 1.0, jax.random.fold_in(rng, 6)
    for axis_at, parts in cuts:
        heights = jnp.exp(jax.random.uniform(jax.random.fold_in(own, axis_at), (parts,), jnp.float32, least / len(cuts), high / len(cuts)))
        factor_of = factor_of * jnp.repeat(heights, dims[axis_at] // parts).reshape([-1 if axis == axis_at else 1 for axis in range(len(dims))])
    return factor_of


def centred(stream_key, shape, width, bound, split=(), dtype=jnp.bfloat16):
    entries = width * jax.random.normal(stream_key, shape, jnp.float32)
    if split:
        entries = entries * levels(stream_key, shape, split, -0.22, 0.18)
    return jnp.clip(entries, -bound, bound).astype(dtype)


def setup_inputs(seed: int = 0) -> dict:
    streams_of = jax.random.split(jax.random.key(seed), 27)
    return {
        "tokens": centred(streams_of[0], (TOKENS, D), 1.0, 6.0, ((0, 8),)),
        "cotangent": centred(streams_of[1], (TOKENS, D), 1.0, 6.0, ((0, 8),)),
        "norm_params": jnp.clip(1.0 + 0.15 * jax.random.normal(streams_of[2], (4, D), jnp.float32), 0.25, 1.75),
        "attention_weight": centred(streams_of[3], (D, 3, D), D ** -0.5, 0.1875, ((0, 8), (2, 4))),
        "attention_bias": centred(streams_of[4], (3, D), 0.5, 3.0, ((1, 4),), jnp.float32),
        "merge_weight": centred(streams_of[5], (D, D), (D // 64) ** -0.5, 1.5, ((0, 8), (1, 4))),
        "branch_bias": centred(streams_of[6], (2, D), 0.5, 3.0, (), jnp.float32),
        "up_weight": centred(streams_of[7], (D, FF), D ** -0.5, 0.1875, ((0, 8), (1, 4))),
        "up_bias": centred(streams_of[8], (FF,), 0.5, 3.0, ((0, 4),), jnp.float32),
        "down_weight": centred(streams_of[9], (D, FF), FF ** -0.5, 0.09375, ((0, 8), (1, 4))),
        "prefix_ids": jax.random.permutation(streams_of[10], PRE).astype(jnp.int32),
        "prefix_table": centred(streams_of[11], (PRE, D), 0.2, 1.25, (), jnp.float32),
        "encoder_weight": centred(streams_of[12], (D, PH), 0.1, 0.625, ((0, 8),), jnp.float32),
        "encoder_bias": centred(streams_of[13], (PH,), 0.1, 0.625, (), jnp.float32),
        "decoder_weight": centred(streams_of[14], (PH, 2, D), 0.1, 0.625, ((0, 8), (2, 4)), jnp.float32),
        "decoder_bias": centred(streams_of[15], (2, D), 0.1, 0.625, ((1, 4),), jnp.float32),
        "first_table": centred(streams_of[16], (PRE, D), (0.0027 * GRADSQ ** -0.5), 1.9073486328125e-06, (), jnp.float32),
        "second_table": jnp.clip(jnp.exp(jax.random.uniform(streams_of[17], (PRE, D), jnp.float32, math.log(5.313843406907961e-15), math.log(8.536994353623706e-14))), 5.313843406907961e-15, 8.536994353623706e-14),
        "first_encoder": centred(streams_of[18], (D, PH), (0.00074 * GRADSQ ** -0.5), 5.960464477539062e-07, ((0, 8),), jnp.float32),
        "second_encoder": jnp.clip(jnp.exp(math.log(6.0978532912382786e-15) - 2.7668907 * jax.random.uniform(streams_of[19], (D, PH), jnp.float32) ** levels(streams_of[19], (D, PH), ((0, 8),), -0.2, 0.2)), 3.83293631819122e-16, 6.0978532912382786e-15),
        "first_encoder_bias": centred(streams_of[20], (PH,), (0.0039 * GRADSQ ** -0.5), 3.337860107421875e-06, (), jnp.float32),
        "second_encoder_bias": jnp.clip(jnp.exp(jax.random.uniform(streams_of[21], (PH,), jnp.float32, math.log(1.0540575404421448e-14), math.log(1.6899765549645285e-13))), 1.0540575404421448e-14, 1.6899765549645285e-13),
        "first_decoder": centred(streams_of[22], (PH, 2, D), (0.00056 * GRADSQ ** -0.5), 4.76837158203125e-07, ((0, 8), (2, 4)), jnp.float32),
        "second_decoder": jnp.clip(jnp.exp(math.log(3.57159997242543e-15) - 2.7735649 * jax.random.uniform(streams_of[23], (PH, 2, D), jnp.float32) ** levels(streams_of[23], (PH, 2, D), ((0, 8), (2, 4)), -0.2, 0.2)), 2.230072049300266e-16, 3.57159997242543e-15),
        "first_decoder_bias": centred(streams_of[24], (2, D), (0.00112 * GRADSQ ** -0.5), 9.5367431640625e-07, ((1, 4),), jnp.float32),
        "second_decoder_bias": jnp.clip(jnp.exp(math.log(1.428639988970172e-14) - 2.7774788 * jax.random.uniform(streams_of[25], (2, D), jnp.float32) ** levels(streams_of[25], (2, D), ((1, 4),), -0.2, 0.2)), 8.88544337933339e-16, 1.428639988970172e-14),
    }


@jax.custom_vjp
def low(v):
    return lax.optimization_barrier(v.astype(jnp.bfloat16)).astype(jnp.float32)

@jax.custom_vjp
def low_back(v):
    return v

def low_keep(v):
    return (low(v), None)

def low_pass(kept, grad):
    return (grad,)

def back_keep(v):
    return (v, None)

def back_low(kept, grad):
    return (low(grad),)
low.defvjp(low_keep, low_pass)
low_back.defvjp(back_keep, back_low)
NORM_EPS = 1e-05
CLIP_LIMIT = 0.001
LEARN_RATE = 0.05
WEIGHT_DECAY = 0.01
BETA_FIRST = 0.9
BETA_SECOND = 0.999
ADAM_EPS = 1e-08
MASKED = -1e+30
GELU_COEF = 0.7978845608028654

def layer_norm(rows, gain, shift):
    center = lax.optimization_barrier(jnp.mean(rows, axis=-1, keepdims=True))
    offsets = rows - center
    spread = lax.optimization_barrier(jnp.mean(offsets * offsets, axis=-1, keepdims=True))
    return offsets * lax.rsqrt(spread + NORM_EPS) * gain + shift

def gelu_tanh(values):
    return 0.5 * values * (1.0 + jnp.tanh(GELU_COEF * (values + 0.044715 * values * values * values)))

def adam_update(weight, grad, first, second, factor):
    clipped = grad * factor
    new_first = BETA_FIRST * first + (1.0 - BETA_FIRST) * clipped
    new_second = BETA_SECOND * second + (1.0 - BETA_SECOND) * clipped * clipped
    fix_first = 1.0 - BETA_FIRST ** STEP
    fix_second = 1.0 - BETA_SECOND ** STEP
    new_weight = weight * (1.0 - LEARN_RATE * WEIGHT_DECAY) - LEARN_RATE * (new_first / fix_first) / (jnp.sqrt(new_second / fix_second) + ADAM_EPS)
    return (new_weight, new_first, new_second)

def reference(tokens, cotangent, norm_params, attention_weight, attention_bias, merge_weight, branch_bias, up_weight, up_bias, down_weight, prefix_ids, prefix_table, encoder_weight, encoder_bias, decoder_weight, decoder_bias, first_table, second_table, first_encoder, second_encoder, first_encoder_bias, second_encoder_bias, first_decoder, second_decoder, first_decoder_bias, second_decoder_bias):
    highest = lax.Precision.HIGHEST
    attend_full = attention_weight.astype(jnp.float32)
    merge_full = merge_weight.astype(jnp.float32)
    up_full = up_weight.astype(jnp.float32)
    down_full = down_weight.astype(jnp.float32)
    block_rows = min(512, SEQ)
    score_scale = float(HD) ** (-0.5)
    onehot = (prefix_ids[:, None] == jnp.arange(PRE)[None, :]).astype(jnp.float32)

    def attend(query_rows, offset, keys, values, prefix_keys, prefix_values):
        pre_scores = jnp.einsum('qhe,jhe->hqj', query_rows, prefix_keys, precision=highest) * score_scale
        own_scores = jnp.einsum('qhe,khe->hqk', query_rows, keys, precision=highest) * score_scale
        visible = (offset + jnp.arange(block_rows))[:, None] >= jnp.arange(SEQ)[None, :]
        own_scores = jnp.where(visible[None], own_scores, MASKED)
        scores = low_back(jnp.concatenate([pre_scores, own_scores], -1))
        highest_score = lax.optimization_barrier(jnp.max(scores, -1, keepdims=True))
        expo = jnp.exp(scores - highest_score)
        probs = low(expo / lax.optimization_barrier(jnp.sum(expo, -1, keepdims=True)))
        mixture = jnp.einsum('hqj,jhe->qhe', probs[..., :PRE], prefix_values, precision=highest)
        return mixture + jnp.einsum('hqk,khe->qhe', probs[..., PRE:], values, precision=highest)

    def sequence_layer(rows, prefix_keys, prefix_values):
        normed_one = low(layer_norm(rows, norm_params[0], norm_params[1]))
        projected = jnp.einsum('td,dcm->tcm', normed_one, attend_full, precision=highest) + attention_bias[None]
        projected = low(low_back(projected)).reshape(SEQ, 3, HEADS, HD)
        queries, keys, values = (projected[:, 0], projected[:, 1], projected[:, 2])
        query_blocks = queries.reshape(SEQ // block_rows, block_rows, HEADS, HD)
        offsets = jnp.arange(SEQ // block_rows) * block_rows
        mixture = lax.map(lambda item: jax.checkpoint(attend)(item[0], item[1], keys, values, prefix_keys, prefix_values), (query_blocks, offsets))
        mixture = low(low_back(mixture.reshape(SEQ, D)))
        merged = low_back(jnp.einsum('tm,dm->td', mixture, merge_full, precision=highest))
        resid = rows + merged + branch_bias[0]
        normed_two = low(layer_norm(resid, norm_params[2], norm_params[3]))
        hidden_pre = low_back(jnp.dot(normed_two, up_full, precision=highest) + up_bias)
        hidden_act = low(gelu_tanh(hidden_pre))
        branch_out = low_back(jnp.einsum('tf,df->td', hidden_act, down_full, precision=highest))
        return resid + branch_out + branch_bias[1]

    def forward(inputs, table, enc_weight, enc_bias, dec_weight, dec_bias):
        selected = jnp.dot(onehot, table, precision=highest)
        encoded = low_back(jnp.dot(low(selected), low(enc_weight), precision=highest) + enc_bias)
        hidden_prefix = jnp.tanh(encoded)
        prefix_kv = jnp.einsum('jp,pcd->jcd', low(hidden_prefix), low(dec_weight), precision=highest) + dec_bias[None]
        prefix_kv = low(low_back(prefix_kv)).reshape(PRE, 2, HEADS, HD)
        prefix_keys = prefix_kv[:, 0]
        prefix_values = prefix_kv[:, 1]
        sequences = inputs.reshape(TOKENS // SEQ, SEQ, D)
        outputs = lax.map(lambda rows: jax.checkpoint(sequence_layer)(rows, prefix_keys, prefix_values), sequences)
        return outputs.reshape(TOKENS, D)
    inputs = tokens.astype(jnp.float32)
    output, pull_back = jax.vjp(forward, inputs, prefix_table, encoder_weight, encoder_bias, decoder_weight, decoder_bias)
    grads = pull_back(cotangent.astype(jnp.float32))
    input_grad, grad_table, grad_encoder, grad_encoder_bias, grad_decoder, grad_decoder_bias = grads
    squares = jnp.sum(grad_table * grad_table) + jnp.sum(grad_encoder * grad_encoder) + jnp.sum(grad_encoder_bias * grad_encoder_bias)
    squares = squares + jnp.sum(grad_decoder * grad_decoder) + jnp.sum(grad_decoder_bias * grad_decoder_bias)
    grad_norm = jnp.sqrt(squares)
    factor = CLIP_LIMIT / (grad_norm + 1e-06)
    table_new = adam_update(prefix_table, grad_table, first_table, second_table, factor)
    encoder_new = adam_update(encoder_weight, grad_encoder, first_encoder, second_encoder, factor)
    enc_bias_new = adam_update(encoder_bias, grad_encoder_bias, first_encoder_bias, second_encoder_bias, factor)
    decoder_new = adam_update(decoder_weight, grad_decoder, first_decoder, second_decoder, factor)
    dec_bias_new = adam_update(decoder_bias, grad_decoder_bias, first_decoder_bias, second_decoder_bias, factor)
    return (output.astype(jnp.bfloat16), input_grad.astype(jnp.bfloat16), grad_norm, table_new[0], table_new[1], table_new[2], encoder_new[0], encoder_new[1], encoder_new[2], enc_bias_new[0], enc_bias_new[1], enc_bias_new[2], decoder_new[0], decoder_new[1], decoder_new[2], dec_bias_new[0], dec_bias_new[1], dec_bias_new[2])
```

```python
import jax
import jax.numpy as jnp
from jax import lax
from jax.experimental import pallas as pl
from jax.experimental.pallas import tpu as pltpu
from jax.sharding import PartitionSpec as P

HD = 64
PRE = 10
SEQ = 1024
STEP = 10


NORM_EPS = 1e-05
CLIP_LIMIT = 0.001
LEARN_RATE = 0.05
WEIGHT_DECAY = 0.01
BETA_FIRST = 0.9
BETA_SECOND = 0.999
ADAM_EPS = 1e-08
MASKED = -1e30
GELU_COEF = 0.7978845608028654


def layer_norm(rows, gain, shift):
    center = jnp.mean(rows, axis=-1, keepdims=True)
    offsets = rows - center
    spread = jnp.mean(offsets * offsets, axis=-1, keepdims=True)
    return offsets * lax.rsqrt(spread + NORM_EPS) * gain + shift


def norm_back(rows, gain, shift, grad_rows):
    _, pull_back = jax.vjp(lambda values: layer_norm(values, gain, shift), rows)
    return pull_back(grad_rows)[0]


def gelu_tanh(values):
    return (
        0.5 * values * (1.0 + jnp.tanh(GELU_COEF * (values + 0.044715 * values * values * values)))
    )


def adam_update(weight, grad, first, second, factor):
    clipped = grad * factor
    new_first = BETA_FIRST * first + (1.0 - BETA_FIRST) * clipped
    new_second = BETA_SECOND * second + (1.0 - BETA_SECOND) * clipped * clipped
    fix_first = 1.0 - BETA_FIRST**STEP
    fix_second = 1.0 - BETA_SECOND**STEP
    new_weight = weight * (1.0 - LEARN_RATE * WEIGHT_DECAY) - LEARN_RATE * (
        new_first / fix_first
    ) / (jnp.sqrt(new_second / fix_second) + ADAM_EPS)
    return (new_weight, new_first, new_second)


def score_blocks(query_rows, keys, prefix_keys, offset, finish, score_scale):
    pre_scores = (
        jnp.einsum("qhe,jhe->hqj", query_rows, prefix_keys, preferred_element_type=jnp.float32)
        * score_scale
    )
    own_scores = (
        jnp.einsum("qhe,khe->hqk", query_rows, keys[:finish], preferred_element_type=jnp.float32)
        * score_scale
    )
    visible = (offset + jnp.arange(finish - offset))[:, None] >= jnp.arange(finish)[None, :]
    own_scores = jnp.where(visible[None], own_scores, MASKED)
    return (pre_scores, own_scores)


def attend_forward(queries, keys, values, prefix_keys, prefix_values):
    length = queries.shape[0]
    block_rows = min(512, length)
    score_scale = float(queries.shape[2]) ** (-0.5)
    mixtures = []
    log_sums = []
    for offset in range(0, length, block_rows):
        finish = offset + block_rows
        pre_scores, own_scores = score_blocks(
            queries[offset:finish], keys, prefix_keys, offset, finish, score_scale
        )
        highest = jnp.maximum(jnp.max(pre_scores, -1), jnp.max(own_scores, -1))
        pre_exp = jnp.exp(pre_scores - highest[..., None])
        own_exp = jnp.exp(own_scores - highest[..., None])
        totals = jnp.sum(pre_exp, -1) + jnp.sum(own_exp, -1)
        pre_prob = (pre_exp / totals[..., None]).astype(jnp.bfloat16)
        own_prob = (own_exp / totals[..., None]).astype(jnp.bfloat16)
        mixture = jnp.einsum(
            "hqj,jhe->qhe", pre_prob, prefix_values, preferred_element_type=jnp.float32
        )
        mixture = mixture + jnp.einsum(
            "hqk,khe->qhe", own_prob, values[:finish], preferred_element_type=jnp.float32
        )
        mixtures.append(mixture)
        log_sums.append(highest + jnp.log(totals))
    return (jnp.concatenate(mixtures, 0), jnp.concatenate(log_sums, 1))


def attend_backward(queries, keys, values, prefix_keys, prefix_values, grad_out, log_sums):
    length = queries.shape[0]
    block_rows = min(512, length)
    score_scale = float(queries.shape[2]) ** (-0.5)
    grad_queries = []
    grad_keys = jnp.zeros(keys.shape, jnp.float32)
    grad_values = jnp.zeros(values.shape, jnp.float32)
    grad_pre_keys = jnp.zeros(prefix_keys.shape, jnp.float32)
    grad_pre_values = jnp.zeros(prefix_values.shape, jnp.float32)
    for offset in range(0, length, block_rows):
        finish = offset + block_rows
        query_rows = queries[offset:finish]
        grad_rows = grad_out[offset:finish]
        pre_scores, own_scores = score_blocks(
            query_rows, keys, prefix_keys, offset, finish, score_scale
        )
        block_sums = log_sums[:, offset:finish, None]
        pre_prob = jnp.exp(pre_scores - block_sums)
        own_prob = jnp.exp(own_scores - block_sums)
        pre_dprob = jnp.einsum(
            "qhe,jhe->hqj", grad_rows, prefix_values, preferred_element_type=jnp.float32
        )
        own_dprob = jnp.einsum(
            "qhe,khe->hqk", grad_rows, values[:finish], preferred_element_type=jnp.float32
        )
        inner = jnp.sum(pre_prob * pre_dprob, -1) + jnp.sum(own_prob * own_dprob, -1)
        pre_dscore = (pre_prob * (pre_dprob - inner[..., None])).astype(jnp.bfloat16)
        own_dscore = (own_prob * (own_dprob - inner[..., None])).astype(jnp.bfloat16)
        grad_query = jnp.einsum(
            "hqj,jhe->qhe", pre_dscore, prefix_keys, preferred_element_type=jnp.float32
        )
        grad_query = grad_query + jnp.einsum(
            "hqk,khe->qhe", own_dscore, keys[:finish], preferred_element_type=jnp.float32
        )
        grad_queries.append(grad_query * score_scale)
        grad_keys = grad_keys.at[:finish].add(
            jnp.einsum("hqk,qhe->khe", own_dscore, query_rows, preferred_element_type=jnp.float32)
            * score_scale
        )
        grad_values = grad_values.at[:finish].add(
            jnp.einsum(
                "hqk,qhe->khe",
                own_prob.astype(jnp.bfloat16),
                grad_rows,
                preferred_element_type=jnp.float32,
            )
        )
        grad_pre_keys = (
            grad_pre_keys
            + jnp.einsum("hqj,qhe->jhe", pre_dscore, query_rows, preferred_element_type=jnp.float32)
            * score_scale
        )
        grad_pre_values = grad_pre_values + jnp.einsum(
            "hqj,qhe->jhe",
            pre_prob.astype(jnp.bfloat16),
            grad_rows,
            preferred_element_type=jnp.float32,
        )
    grad_seq = jnp.stack([jnp.concatenate(grad_queries, 0), grad_keys, grad_values], 1)
    grad_prefix = jnp.stack([grad_pre_keys, grad_pre_values], 1)
    return (grad_seq, grad_prefix)


def swap(values, axis, bit):
    size = lax.axis_size(axis)
    return lax.ppermute(values, axis, [(i, i ^ bit) for i in range(size)])


def assemble_kernel(own, far, near, side, side_rest, out, sems):
    here = lax.axis_index("dp")
    pieces = [(own, 0), (far, 4), (near.at[0], 2), (near.at[1], 6)]
    pieces += [(side, 1), (side_rest.at[0], 5), (side_rest.at[1], 3), (side_rest.at[2], 7)]
    copies = []
    for slot, (piece, offset) in enumerate(pieces):
        place = lax.bitwise_xor(here, offset)
        copies.append(pltpu.make_async_copy(piece, out.at[place], sems.at[slot]))
        copies[-1].start()
    for copy in copies:
        copy.wait()


def gather_start(shard):
    return swap(shard, "dp", 1), swap(shard, "dp", 4)


def gather_rest(shard, side, far):
    near = swap(jnp.stack([shard, far]), "dp", 2)
    side_rest = swap(jnp.concatenate([far[None], near]), "dp", 1)
    return near, side_rest


def assemble(shard, far, near, side, side_rest):
    return pl.pallas_call(
        assemble_kernel,
        out_shape=jax.ShapeDtypeStruct((8,) + shard.shape, shard.dtype),
        in_specs=[pl.BlockSpec(memory_space=pl.ANY)] * 5,
        out_specs=pl.BlockSpec(memory_space=pl.ANY),
        scratch_shapes=[pltpu.SemaphoreType.DMA((8,))],
    )(shard, far, near, side, side_rest)


def gather_all(shards):
    if lax.axis_size("dp") != 8:
        return [lax.all_gather(shard, "dp", axis=0) for shard in shards]
    fulls = []
    after = None
    for shard in shards:
        if after is not None:
            shard, after = lax.optimization_barrier((shard, after))
        side, far = gather_start(shard)
        after = far
        near, side_rest = gather_rest(shard, side, far)
        fulls.append(assemble(shard, far, near, side, side_rest))
    return fulls


def sum_over(values, axis):
    bit = 1
    while bit < lax.axis_size(axis):
        values = jax.tree.map(lambda v, b=bit: v + swap(v, axis, b), values)
        bit *= 2
    return values


def scatter_rows(part):
    low = part.astype(jnp.bfloat16)
    rows, width = part.shape
    here = lax.axis_index("tensor")
    core, side = here % 2, here // 2
    blocks = low.reshape(2, 2, rows // 4, width)
    keep = lax.dynamic_index_in_dim(blocks, core, 1, keepdims=False)
    got = swap(lax.dynamic_index_in_dim(blocks, 1 - core, 1, keepdims=False), "tensor", 1)
    both = keep.astype(jnp.float32) + got.astype(jnp.float32)
    mine = lax.dynamic_index_in_dim(both, side, 0, keepdims=False)
    other = lax.dynamic_index_in_dim(both, 1 - side, 0, keepdims=False).astype(jnp.bfloat16)
    return mine + swap(other, "tensor", 2).astype(jnp.float32)


def split_low(values):
    high = lax.reduce_precision(values, 8, 7)
    return jnp.stack([high.astype(jnp.bfloat16), (values - high).astype(jnp.bfloat16)])


def on_device(
    tokens,
    cotangent,
    norm_params,
    attention_weight,
    attention_bias,
    merge_weight,
    branch_bias,
    up_weight,
    up_bias,
    down_weight,
    prefix_ids,
    prefix_table,
    encoder_weight,
    encoder_bias,
    decoder_weight,
    decoder_bias,
    first_table,
    second_table,
    first_encoder,
    second_encoder,
    first_encoder_bias,
    second_encoder_bias,
    first_decoder,
    second_decoder,
    first_decoder_bias,
    second_decoder_bias,
):
    highest_prec = lax.Precision.HIGHEST
    dp_index = lax.axis_index("dp")
    here = lax.axis_index("tensor")
    core, side = here % 2, here // 2
    tok_rows, width = tokens.shape
    local_width = merge_weight.shape[1]
    local_heads = local_width // HD
    sequences = tok_rows // SEQ
    share = tok_rows // lax.axis_size("tensor")
    row_start = here * share
    in_rows = attention_weight.shape[0]
    encoder_rows = encoder_weight.shape[0]
    decoder_rows = decoder_weight.shape[0]
    hidden = encoder_weight.shape[1]

    onehot = (prefix_ids[:, None] == jnp.arange(PRE, dtype=jnp.int32)[None, :]).astype(jnp.float32)
    selected = jnp.dot(onehot, prefix_table, precision=highest_prec)
    selected_low = selected.astype(jnp.bfloat16)
    selected_own = lax.dynamic_slice_in_dim(
        selected_low, dp_index * encoder_rows, encoder_rows, 1
    )
    encoder_low = encoder_weight.astype(jnp.bfloat16)
    decoder_low = decoder_weight.astype(jnp.bfloat16)
    encoded_own = jnp.dot(selected_own, encoder_low, preferred_element_type=jnp.float32)
    sent = split_low(encoded_own).reshape(-1, local_width)
    sent_rows = sent.shape[0]
    sent = jnp.pad(sent, ((0, -sent_rows % 16), (0, 0)))
    first = jnp.concatenate(
        [attention_weight.transpose(1, 0, 2).reshape(3 * in_rows, local_width), sent]
    )
    second = jnp.concatenate([merge_weight, decoder_low.reshape(2 * decoder_rows, local_width)])
    first, second, down_all, up_all, encoder_all = gather_all(
        [first, second, down_weight, up_weight, encoder_low]
    )
    attend_full = first[:, : 3 * in_rows].reshape(-1, 3, in_rows, local_width)
    attend_full = attend_full.transpose(1, 0, 2, 3).reshape(3, width, local_width)
    encoded_all = first[:, 3 * in_rows : 3 * in_rows + sent_rows]
    encoded = (
        jnp.sum(encoded_all.astype(jnp.float32).reshape(-1, PRE, hidden), 0) + encoder_bias
    )
    merge_own = second[:, : merge_weight.shape[0]].reshape(width, local_width)
    decoder_full = second[:, merge_weight.shape[0] :].reshape(hidden, 2, local_width)
    down_full = down_all.reshape(width, -1)
    up_full = up_all.reshape(width, -1)
    encoder_full = encoder_all.reshape(width, hidden)

    hidden_prefix = jnp.tanh(encoded)
    hidden_low = hidden_prefix.astype(jnp.bfloat16)
    prefix_kv = (
        jnp.einsum("jp,pcm->jcm", hidden_low, decoder_full, preferred_element_type=jnp.float32)
        + decoder_bias[None]
    )
    prefix_kv = prefix_kv.astype(jnp.bfloat16).reshape(PRE, 2, local_heads, HD)
    prefix_keys = prefix_kv[:, 0]
    prefix_values = prefix_kv[:, 1]
    inputs = tokens.astype(jnp.float32)

    merge_side = swap(merge_own, "tensor", 2)
    merge_pair = swap(jnp.stack([merge_own, merge_side]), "tensor", 1)

    normed_one = layer_norm(inputs, norm_params[0], norm_params[1]).astype(jnp.bfloat16)
    projected = (
        jnp.einsum("td,cdm->tcm", normed_one, attend_full, preferred_element_type=jnp.float32)
        + attention_bias[None]
    )
    projected = projected.astype(jnp.bfloat16).reshape(tok_rows, 3, local_heads, HD)
    mixture, log_sums = attend_forward(
        projected[:, 0], projected[:, 1], projected[:, 2], prefix_keys, prefix_values
    )
    mixture = mixture.reshape(tok_rows, local_width).astype(jnp.bfloat16)
    mixture_side = swap(mixture, "tensor", 2)
    mixture_pair = swap(jnp.stack([mixture, mixture_side]), "tensor", 1)
    mixture_cat = jnp.concatenate(
        [mixture, mixture_side, mixture_pair[0], mixture_pair[1]], 1
    )
    merge_cat = jnp.concatenate([merge_own, merge_side, merge_pair[0], merge_pair[1]], 1)
    merged = jnp.einsum("tm,dm->td", mixture_cat, merge_cat, preferred_element_type=jnp.float32)
    resid = inputs + merged + branch_bias[0]
    normed_two = layer_norm(resid, norm_params[2], norm_params[3]).astype(jnp.bfloat16)
    hidden_pre = jnp.dot(normed_two, up_full, preferred_element_type=jnp.float32) + up_bias
    hidden_act = gelu_tanh(hidden_pre).astype(jnp.bfloat16)
    branch_part = jnp.einsum("tf,df->td", hidden_act, down_full, preferred_element_type=jnp.float32)
    resid_own = lax.dynamic_slice_in_dim(resid, row_start, share, 0)

    grad_hidden = jnp.dot(cotangent, down_full, preferred_element_type=jnp.float32)
    _, gelu_pull = jax.vjp(gelu_tanh, hidden_pre)
    grad_pre = gelu_pull(grad_hidden)[0].astype(jnp.bfloat16)
    up_part = jnp.einsum("tf,df->td", grad_pre, up_full, preferred_element_type=jnp.float32)
    up_own = scatter_rows(up_part)
    branch_own = scatter_rows(branch_part)
    output_rows = resid_own + branch_own + branch_bias[1]
    cotangent_own = lax.dynamic_slice_in_dim(cotangent, row_start, share, 0).astype(jnp.float32)
    grad_resid = cotangent_own + norm_back(resid_own, norm_params[2], norm_params[3], up_own)
    branch_grad = grad_resid.astype(jnp.bfloat16)
    grad_cat = jnp.dot(branch_grad, merge_cat, preferred_element_type=jnp.float32)
    grad_cat = grad_cat.astype(jnp.bfloat16)
    grad_blocks = [grad_cat[:, i * local_width : (i + 1) * local_width] for i in range(4)]
    from_side = swap(jnp.stack([grad_blocks[1], grad_blocks[3]]), "tensor", 2)
    from_pair = swap(jnp.stack([grad_blocks[2], from_side[1]]), "tensor", 1)
    by_offset = jnp.stack([grad_blocks[0], from_pair[0], from_side[0], from_pair[1]])
    order = lax.bitwise_xor(jnp.arange(4), here)
    grad_mixture = jnp.stack(
        [lax.dynamic_index_in_dim(by_offset, order[i], 0, keepdims=False) for i in range(4)]
    )
    grad_mixture = grad_mixture.reshape(tok_rows, local_heads, HD)

    grad_seq, grad_prefix = attend_backward(
        projected[:, 0],
        projected[:, 1],
        projected[:, 2],
        prefix_keys,
        prefix_values,
        grad_mixture,
        log_sums,
    )
    grad_projected = grad_seq.reshape(tok_rows, 3, local_width).astype(jnp.bfloat16)
    first_part = jnp.einsum(
        "tcm,cdm->td", grad_projected, attend_full, preferred_element_type=jnp.float32
    )
    first_own = scatter_rows(first_part)
    inputs_own = lax.dynamic_slice_in_dim(inputs, row_start, share, 0)
    input_grad = grad_resid + norm_back(inputs_own, norm_params[0], norm_params[1], first_own)

    prefix_total = sum_over(grad_prefix.reshape(PRE, 2, local_width), "dp")
    prefix_low = prefix_total.astype(jnp.bfloat16)
    grad_decoder = jnp.einsum(
        "jp,jcm->pcm", hidden_low, prefix_low, preferred_element_type=jnp.float32
    )
    grad_decoder_bias = jnp.sum(prefix_low.astype(jnp.float32), 0)
    encoded_part = jnp.einsum(
        "jcm,pcm->jp", prefix_low, decoder_full, preferred_element_type=jnp.float32
    )
    square_part = jnp.sum(grad_decoder * grad_decoder) + jnp.sum(
        grad_decoder_bias * grad_decoder_bias
    )
    joint = jnp.concatenate(
        [encoded_part, jnp.broadcast_to(square_part, (1, hidden))]
    )
    joint = sum_over(joint, "tensor")
    encoded_grad, square_decoder = joint[:PRE], joint[PRE, 0]
    grad_encoded = (encoded_grad * (1.0 - hidden_prefix * hidden_prefix)).astype(jnp.bfloat16)
    grad_encoder = jnp.dot(selected_low.T, grad_encoded, preferred_element_type=jnp.float32)
    grad_encoder_bias = jnp.sum(grad_encoded.astype(jnp.float32), 0)
    grad_selected = jnp.dot(grad_encoded, encoder_full.T, preferred_element_type=jnp.float32)
    grad_table = jnp.dot(onehot.T, grad_selected, precision=highest_prec)
    squares = (
        square_decoder
        + jnp.sum(grad_table * grad_table)
        + jnp.sum(grad_encoder * grad_encoder)
        + jnp.sum(grad_encoder_bias * grad_encoder_bias)
    )
    grad_norm = jnp.sqrt(squares)
    factor = CLIP_LIMIT / (grad_norm + 1e-06)
    encoder_own = lax.dynamic_slice_in_dim(grad_encoder, dp_index * encoder_rows, encoder_rows, 0)
    decoder_own = lax.dynamic_slice_in_dim(grad_decoder, dp_index * decoder_rows, decoder_rows, 0)
    table_new = adam_update(prefix_table, grad_table, first_table, second_table, factor)
    encoder_new = adam_update(encoder_weight, encoder_own, first_encoder, second_encoder, factor)
    enc_bias_new = adam_update(
        encoder_bias, grad_encoder_bias, first_encoder_bias, second_encoder_bias, factor
    )
    decoder_new = adam_update(decoder_weight, decoder_own, first_decoder, second_decoder, factor)
    dec_bias_new = adam_update(
        decoder_bias, grad_decoder_bias, first_decoder_bias, second_decoder_bias, factor
    )
    return (
        output_rows.astype(jnp.bfloat16),
        input_grad.astype(jnp.bfloat16),
        grad_norm,
        table_new[0],
        table_new[1],
        table_new[2],
        encoder_new[0],
        encoder_new[1],
        encoder_new[2],
        enc_bias_new[0],
        enc_bias_new[1],
        enc_bias_new[2],
        decoder_new[0],
        decoder_new[1],
        decoder_new[2],
        dec_bias_new[0],
        dec_bias_new[1],
        dec_bias_new[2],
    )


def solution(mesh):
    in_specs = (
        P("dp", None),
        P("dp", None),
        P(),
        P("dp", None, "tensor"),
        P(None, "tensor"),
        P("dp", "tensor"),
        P(),
        P("dp", "tensor"),
        P("tensor"),
        P("dp", "tensor"),
        P(),
        P(),
        P("dp", None),
        P(),
        P("dp", None, "tensor"),
        P(None, "tensor"),
        P(),
        P(),
        P("dp", None),
        P("dp", None),
        P(),
        P(),
        P("dp", None, "tensor"),
        P("dp", None, "tensor"),
        P(None, "tensor"),
        P(None, "tensor"),
    )
    out_specs = (
        P(("dp", "tensor"), None),
        P(("dp", "tensor"), None),
        P(),
        P(),
        P(),
        P(),
        P("dp", None),
        P("dp", None),
        P("dp", None),
        P(),
        P(),
        P(),
        P("dp", None, "tensor"),
        P("dp", None, "tensor"),
        P("dp", None, "tensor"),
        P(None, "tensor"),
        P(None, "tensor"),
        P(None, "tensor"),
    )
    return jax.shard_map(
        on_device, mesh=mesh, in_specs=in_specs, out_specs=out_specs, check_vma=False
    )
```

```python
import functools

import jax
import jax.numpy as jnp
from jax import lax
from jax.experimental import pallas as pl
from jax.experimental.pallas import tpu as pltpu
from jax.sharding import PartitionSpec as P

HD = 64
PRE = 10
PAD = 16
STEP = 10
TILE = 256


NORM_EPS = 1e-05
CLIP_LIMIT = 0.001
LEARN_RATE = 0.05
WEIGHT_DECAY = 0.01
BETA_FIRST = 0.9
BETA_SECOND = 0.999
ADAM_EPS = 1e-08
MASKED = -1e30
GELU_COEF = 0.7978845608028654

NN = ((1,), (0,))
NT = ((1,), (1,))
TN = ((0,), (0,))
OWN, CORE, SIDE, BOTH = 0, 1, 2, 3


def dot(left, right, dims, precision=None):
    return lax.dot_general(
        left, right, (dims, ((), ())), precision=precision, preferred_element_type=jnp.float32
    )


def shaped(shape, dtype):
    return jax.ShapeDtypeStruct(shape, dtype)


def cost(flops, *arrays):
    size = sum(a.size * a.dtype.itemsize for a in arrays)
    return pl.CostEstimate(flops=flops, transcendentals=0, bytes_accessed=size)


def norm_parts(rows):
    offsets = rows - jnp.mean(rows, axis=-1, keepdims=True)
    scale = lax.rsqrt(jnp.mean(offsets * offsets, axis=-1, keepdims=True) + NORM_EPS)
    return offsets * scale, scale


def norm_back(rows, gain, grad):
    unit, scale = norm_parts(rows)
    grad = grad * gain
    mean = jnp.mean(grad, axis=-1, keepdims=True)
    along = jnp.mean(grad * unit, axis=-1, keepdims=True)
    return scale * (grad - mean - unit * along)


def adam_update(weight, grad, first, second, factor):
    clipped = grad * factor
    new_first = BETA_FIRST * first + (1.0 - BETA_FIRST) * clipped
    new_second = BETA_SECOND * second + (1.0 - BETA_SECOND) * clipped * clipped
    fix_first = 1.0 - BETA_FIRST**STEP
    fix_second = 1.0 - BETA_SECOND**STEP
    new_weight = weight * (1.0 - LEARN_RATE * WEIGHT_DECAY) - LEARN_RATE * (
        new_first / fix_first
    ) / (jnp.sqrt(new_second / fix_second) + ADAM_EPS)
    return (new_weight, new_first, new_second)


def swap(values, axis, bits):
    size = lax.axis_size(axis)
    return lax.ppermute(values, axis, [(i, i ^ bits) for i in range(size)])


def gather_all(shards):
    if lax.axis_size("dp") != 8:
        return [lax.all_gather(shard, "dp", axis=0) for shard in shards]
    sides = [swap(shard, "dp", 1) for shard in shards]
    gathered = []
    far = near = None
    for shard, side in zip(shards, sides, strict=True):
        if far is not None:
            shard, far = lax.optimization_barrier((shard, far))
        far = swap(shard, "dp", 4)
        pair = jnp.stack([shard, far])
        if near is not None:
            pair, near = lax.optimization_barrier((pair, near))
        near = swap(pair, "dp", 2)
        rest = swap(jnp.concatenate([far[None], near]), "dp", 1)
        gathered.append((shard, far, near, side, rest))
    return gathered


def placed(pieces):
    if len(pieces) == 1:
        return [(pieces[0].at[i], i) for i in range(pieces[0].shape[0])]
    own, far, near, side, rest = pieces
    found = [(own, 0), (far, 4), (near.at[0], 2), (near.at[1], 6)]
    found += [(side, 1), (rest.at[0], 5), (rest.at[1], 3), (rest.at[2], 7)]
    here = lax.axis_index("dp")
    return [(piece, lax.bitwise_xor(here, bits)) for piece, bits in found]


def pieces_of(gathered):
    return list(gathered) if isinstance(gathered, tuple) else [gathered]


def sum_over(values, axis):
    bits = 1
    while bits < lax.axis_size(axis):
        values = values + swap(values, axis, bits)
        bits *= 2
    return values


def assemble_kernel(n_pieces, *refs):
    pieces, outs = refs[:n_pieces], refs[n_pieces:]
    for piece, place in placed(pieces):
        start = 0
        for out in outs:
            parts, rows = out.shape[0], out.shape[1] // lax.axis_size("dp")
            for part in range(parts):
                where = pl.ds(pl.multiple_of(place * rows, rows), rows)
                out[part, where, :] = piece[start : start + rows, :]
                start += rows


def assemble(gathered, shapes):
    pieces = pieces_of(gathered)
    outs = tuple(shaped(shape, pieces[0].dtype) for shape in shapes)
    return pl.pallas_call(
        functools.partial(assemble_kernel, len(pieces)),
        out_shape=outs,
        name="assemble",
        cost_estimate=cost(0, *pieces, *outs),
    )(*pieces)


def project_kernel(n_pieces, tokens, norms, bias, *refs):
    pieces, (projected, attend, encoded) = refs[:n_pieces], refs[n_pieces:]
    in_rows = attend.shape[1] // lax.axis_size("dp")
    half = attend.shape[2]
    sums = None
    for piece, place in placed(pieces):
        for part in range(3):
            where = pl.ds(pl.multiple_of(place * in_rows, in_rows), in_rows)
            attend[part, where, :] = piece[part * in_rows : (part + 1) * in_rows, :]
        sent = piece[3 * in_rows :, :].astype(jnp.float32)
        sums = sent if sums is None else sums + sent
    halves = encoded.shape[1] // half
    for i in range(halves):
        high = sums[i * PAD : (i + 1) * PAD]
        encoded[:, i * half : (i + 1) * half] = high + sums[(halves + i) * PAD : (halves + i + 1) * PAD]
    for start in range(0, tokens.shape[0], TILE):
        rows = slice(start, start + TILE)
        unit, _ = norm_parts(tokens[rows, :].astype(jnp.float32))
        normed = (unit * norms[0:1, :] + norms[1:2, :]).astype(jnp.bfloat16)
        for part in range(3):
            total = dot(normed, attend[part], NN) + bias[part : part + 1, :]
            projected[part, rows, :] = total.astype(jnp.bfloat16)


def project(tokens, norms, bias, gathered, hidden):
    pieces = pieces_of(gathered)
    rows, width = tokens.shape
    local = bias.shape[1]
    outs = (
        shaped((3, rows, local), jnp.bfloat16),
        shaped((3, width, local), jnp.bfloat16),
        shaped((PAD, hidden), jnp.float32),
    )
    return pl.pallas_call(
        functools.partial(project_kernel, len(pieces)),
        out_shape=outs,
        name="project",
        cost_estimate=cost(6 * rows * width * local, tokens, *pieces, *outs),
    )(tokens, norms, bias, *pieces)


def prefix_kernel(encoded, encoder_bias, decoder, decoder_bias, hidden, prefix):
    held = jnp.tanh(encoded[...] + encoder_bias[...])
    hidden[...] = held
    low = held.astype(jnp.bfloat16)
    for part in range(2):
        total = dot(low, decoder[part], NN) + decoder_bias[part : part + 1, :]
        prefix[part] = total.astype(jnp.bfloat16)


def attend_kernel(proj, prefix, mix, sums):
    rows, width = mix.shape
    lane = lax.broadcasted_iota(jnp.int32, (1, width), 1) // HD
    pre_col = lax.broadcasted_iota(jnp.int32, (TILE, PAD), 1)
    below = lax.broadcasted_iota(jnp.int32, (TILE, TILE), 0) >= lax.broadcasted_iota(
        jnp.int32, (TILE, TILE), 1
    )
    sum_col = lax.broadcasted_iota(jnp.int32, (TILE, 128), 1)
    for start in range(0, rows, TILE):
        here = slice(start, start + TILE)
        query = proj[0, here, :] * jnp.asarray(HD**-0.5, jnp.bfloat16)
        mixed = jnp.zeros((TILE, width), jnp.float32)
        log_sums = jnp.zeros((TILE, 128), jnp.float32)
        for head in range(width // HD):
            mine = lane == head
            one = jnp.where(mine, query, jnp.zeros_like(query))
            scores = [
                jnp.where(pre_col < PRE, dot(one, prefix[0], NT), MASKED),
                jnp.where(below, dot(one, proj[1, here, :], NT), MASKED),
            ]
            values = [prefix[1], proj[2, here, :]]
            if start:
                scores.append(dot(one, proj[1, :start, :], NT))
                values.append(proj[2, :start, :])
            top = functools.reduce(jnp.maximum, [jnp.max(s, 1, keepdims=True) for s in scores])
            exps = [jnp.exp(s - top) for s in scores]
            total = sum(jnp.sum(e, 1, keepdims=True) for e in exps)
            inverse = 1.0 / total
            part = sum(
                dot((e * inverse).astype(jnp.bfloat16), v, NN)
                for e, v in zip(exps, values, strict=True)
            )
            mixed = jnp.where(mine, part, mixed)
            log_sums = jnp.where(sum_col == head, top + jnp.log(total), log_sums)
        mix[here, :] = mixed.astype(jnp.bfloat16)
        sums[here, :] = log_sums


def attend(proj, prefix):
    _, rows, width = proj.shape
    outs = (shaped((rows, width), jnp.bfloat16), shaped((rows, 128), jnp.float32))
    return pl.pallas_call(
        attend_kernel,
        out_shape=outs,
        name="attend",
        cost_estimate=cost(5 * width // HD * rows * rows * width // 2, proj, *outs),
    )(proj, prefix)


def attend_back_kernel(proj, prefix, mix, sums, own, core, side, both, gproj, gprefix, gmix, gquery, gkey, gvalue):
    rows, width = mix.shape
    quarter = own.shape[0]
    me = lax.axis_index("tensor")
    for piece, bits in ((own, OWN), (core, CORE), (side, SIDE), (both, BOTH)):
        place = lax.bitwise_xor(me, bits) * quarter
        gmix[pl.ds(pl.multiple_of(place, quarter), quarter), :] = piece[...]
    lane = lax.broadcasted_iota(jnp.int32, (1, width), 1) // HD
    pre_row = lax.broadcasted_iota(jnp.int32, (PAD, TILE), 0)
    seen = lax.broadcasted_iota(jnp.int32, (TILE, TILE), 0) <= lax.broadcasted_iota(
        jnp.int32, (TILE, TILE), 1
    )
    scale = jnp.asarray(HD**-0.5, jnp.bfloat16)
    sums_row = sums[...].T
    head_of = lax.broadcasted_iota(jnp.int32, (8, width), 0) == lax.broadcasted_iota(
        jnp.int32, (8, width), 1
    ) // HD
    product = gmix[...].astype(jnp.float32) * mix[...].astype(jnp.float32)
    inner = dot(head_of.astype(jnp.float32), product, NT, lax.Precision.HIGHEST)
    keys_col = (proj[1] * scale).T
    pre_col = (prefix[0] * scale).T
    gkey[...] = jnp.zeros_like(gkey)
    gvalue[...] = jnp.zeros_like(gvalue)
    gpre_key = jnp.zeros((PAD, width), jnp.float32)
    gpre_value = jnp.zeros((PAD, width), jnp.float32)
    for start in range(0, rows, TILE):
        here = slice(start, start + TILE)
        query = proj[0, here, :] * scale
        grad = gmix[here, :]
        for head in range(width // HD):
            mine = lane == head
            cols = slice(head * HD, (head + 1) * HD)
            one = jnp.where(mine, query, jnp.zeros_like(query))
            one_grad = jnp.where(mine, grad, jnp.zeros_like(grad))
            log_sum = sums_row[head : head + 1, here]
            shared = inner[head : head + 1, here]

            def block(keys, values, shown):
                scores = dot(keys, one, NT)
                if shown is not None:
                    scores = jnp.where(shown, scores, MASKED)
                prob = jnp.exp(scores - log_sum)
                dscore = (prob * (dot(values, one_grad, NT) - shared)).astype(jnp.bfloat16)
                return dscore, dot(dscore, one, NN), dot(prob.astype(jnp.bfloat16), one_grad, NN)

            dscore, dkey, dvalue = block(prefix[0], prefix[1], pre_row < PRE)
            gpre_key = gpre_key + dkey
            gpre_value = gpre_value + dvalue
            dquery = dot(pre_col[cols, :], dscore, NN)
            for at in range(0, start + TILE, TILE):
                there = slice(at, at + TILE)
                dscore, dkey, dvalue = block(
                    proj[1, there, :], proj[2, there, :], seen if at == start else None
                )
                gkey[there, :] += dkey
                gvalue[there, :] += dvalue
                dquery = dquery + dot(keys_col[cols, there], dscore, NN)
            gquery[cols, here] = dquery
    gproj[0] = gquery[...].T.astype(jnp.bfloat16)
    gproj[1] = gkey[...].astype(jnp.bfloat16)
    gproj[2] = gvalue[...].astype(jnp.bfloat16)
    gprefix[0] = gpre_key
    gprefix[1] = gpre_value


def attend_back(proj, prefix, mix, sums, pieces):
    _, rows, width = proj.shape
    outs = (shaped(proj.shape, jnp.bfloat16), shaped(prefix.shape, jnp.float32))
    return pl.pallas_call(
        attend_back_kernel,
        out_shape=outs,
        scratch_shapes=[
            pltpu.VMEM((rows, width), jnp.bfloat16),
            pltpu.VMEM((width, rows), jnp.float32),
            pltpu.VMEM((rows, width), jnp.float32),
            pltpu.VMEM((rows, width), jnp.float32),
        ],
        name="attend_back",
        cost_estimate=cost(12 * width // HD * rows * rows * width // 2, proj, mix, sums, *outs),
    )(proj, prefix, mix, sums, *pieces)


def merge_kernel(tokens, norms, branch, *refs):
    mixes, merges, (normed, resid_own) = refs[:4], refs[4:8], refs[8:]
    i = pl.program_id(0)
    merged = sum(dot(m[...], w[...], NT) for m, w in zip(mixes, merges, strict=True))
    resid = tokens[...].astype(jnp.float32) + merged + branch[0:1, :]
    unit, _ = norm_parts(resid)
    normed[...] = (unit * norms[2:3, :] + norms[3:4, :]).astype(jnp.bfloat16)

    @pl.when(i == lax.axis_index("tensor"))
    def _():
        resid_own[...] = resid


def merge(tokens, norms, branch, mixes, merges):
    rows, width = tokens.shape
    share = rows // lax.axis_size("tensor")
    local = mixes[0].shape[1]
    whole = lambda a: pl.BlockSpec(a.shape, lambda i: (0,) * a.ndim)
    outs = (shaped((rows, width), jnp.bfloat16), shaped((share, width), jnp.float32))
    return pl.pallas_call(
        merge_kernel,
        grid=(rows // share,),
        in_specs=[pl.BlockSpec((share, width), lambda i: (i, 0)), whole(norms), whole(branch)]
        + [pl.BlockSpec((share, local), lambda i: (i, 0))] * 4
        + [whole(w) for w in merges],
        out_specs=(
            pl.BlockSpec((share, width), lambda i: (i, 0)),
            pl.BlockSpec((share, width), lambda i: (0, 0)),
        ),
        out_shape=outs,
        name="merge",
        cost_estimate=cost(8 * rows * width * local, tokens, *mixes, *merges, *outs),
    )(tokens, norms, branch, *mixes, *merges)


def feed_kernel(blocks, normed, ghidden, up, bias, act, part):
    value = dot(normed[...], up[...], NN) + bias[...]
    square = value * value
    tanh = jnp.tanh(GELU_COEF * value * (1.0 + 0.044715 * square))
    act[0] = (0.5 * value * (1.0 + tanh)).astype(jnp.bfloat16)
    slope = 0.5 * (1.0 + tanh) + 0.5 * GELU_COEF * value * (1.0 - tanh * tanh) * (
        1.0 + 3.0 * 0.044715 * square
    )
    gpre = (ghidden[...] * slope).astype(jnp.bfloat16)
    part[0] = dot(gpre, up[...], NT).astype(jnp.bfloat16)


def feed(bits, normed, ghidden, up, bias):
    rows, width = normed.shape
    share = rows // lax.axis_size("tensor")
    units = up.shape[1]
    blocks = lax.bitwise_xor(lax.axis_index("tensor"), jnp.array(bits, jnp.int32))
    outs = (
        shaped((len(bits), share, units), jnp.bfloat16),
        shaped((len(bits), share, width), jnp.bfloat16),
    )
    spec = pltpu.PrefetchScalarGridSpec(
        num_scalar_prefetch=1,
        grid=(len(bits),),
        in_specs=[
            pl.BlockSpec((share, width), lambda i, b: (b[i], 0)),
            pl.BlockSpec((share, units), lambda i, b: (b[i], 0)),
            pl.BlockSpec(up.shape, lambda i, b: (0, 0)),
            pl.BlockSpec(bias.shape, lambda i, b: (0, 0)),
        ],
        out_specs=(
            pl.BlockSpec((1, share, units), lambda i, b: (i, 0, 0)),
            pl.BlockSpec((1, share, width), lambda i, b: (i, 0, 0)),
        ),
    )
    return pl.pallas_call(
        feed_kernel,
        grid_spec=spec,
        out_shape=outs,
        name="feed",
        cost_estimate=cost(4 * len(bits) * share * width * units, up, *outs),
    )(blocks, normed, ghidden, up, bias)


def back_kernel(blocks, grad, weight, part):
    total = sum(dot(grad[i], weight[i], NT) for i in range(weight.shape[0]))
    part[0] = total.astype(jnp.bfloat16)


def project_back(bits, gproj, attend):
    _, rows, local = gproj.shape
    width = attend.shape[1]
    share = rows // lax.axis_size("tensor")
    blocks = lax.bitwise_xor(lax.axis_index("tensor"), jnp.array(bits, jnp.int32))
    out = shaped((len(bits), share, width), jnp.bfloat16)
    spec = pltpu.PrefetchScalarGridSpec(
        num_scalar_prefetch=1,
        grid=(len(bits),),
        in_specs=[
            pl.BlockSpec((3, share, local), lambda i, b: (0, b[i], 0)),
            pl.BlockSpec(attend.shape, lambda i, b: (0, 0, 0)),
        ],
        out_specs=pl.BlockSpec((1, share, width), lambda i, b: (i, 0, 0)),
    )
    return pl.pallas_call(
        back_kernel,
        grid_spec=spec,
        out_shape=out,
        name="project_back",
        cost_estimate=cost(6 * len(bits) * share * local * width, attend, out),
    )(blocks, gproj, attend)


def own_rows(values):
    share = values.shape[0] // lax.axis_size("tensor")
    return lax.dynamic_slice_in_dim(values, lax.axis_index("tensor") * share, share, 0)


def middle_kernel(own, core, side, cotangent, resid, norms, *refs):
    merges, (gresid, keep, send) = refs[:4], refs[4:]
    total = own[0].astype(jnp.float32) + core[1].astype(jnp.float32) + side[...].astype(jnp.float32)
    grad = cotangent[...].astype(jnp.float32) + norm_back(resid[...], norms[2:3, :], total)
    gresid[...] = grad
    low = grad.astype(jnp.bfloat16)
    keep[0] = dot(low, merges[OWN][...], NN).astype(jnp.bfloat16)
    keep[1] = dot(low, merges[CORE][...], NN).astype(jnp.bfloat16)
    send[0] = dot(low, merges[SIDE][...], NN).astype(jnp.bfloat16)
    send[1] = dot(low, merges[BOTH][...], NN).astype(jnp.bfloat16)


def middle(own, core, side, cotangent, resid, norms, merges):
    share, width = resid.shape
    local = merges[0].shape[1]
    outs = (
        shaped((share, width), jnp.float32),
        shaped((2, share, local), jnp.bfloat16),
        shaped((2, share, local), jnp.bfloat16),
    )
    return pl.pallas_call(
        middle_kernel,
        out_shape=outs,
        name="middle",
        cost_estimate=cost(8 * share * width * local, resid, *merges, *outs),
    )(own, core, side, cotangent, resid, norms, *merges)


def last_kernel(own, core, side, tokens, gresid, norms, out):
    total = own[0].astype(jnp.float32) + core[1].astype(jnp.float32) + side[...].astype(jnp.float32)
    rows = tokens[...].astype(jnp.float32)
    out[...] = (gresid[...] + norm_back(rows, norms[0:1, :], total)).astype(jnp.bfloat16)


def tail_kernel(total, hidden, decoder, joint):
    low = total[...].astype(jnp.bfloat16)
    held = hidden[...].astype(jnp.bfloat16)
    part = jnp.zeros(joint.shape, jnp.float32)
    square = jnp.zeros((1, 1), jnp.float32)
    for i in range(2):
        part = part + dot(low[i], decoder[i], NT)
        grad = dot(held, low[i], TN)
        square = square + jnp.sum(jnp.sum(grad * grad, 0, keepdims=True), 1, keepdims=True)
        bias = jnp.sum(low[i].astype(jnp.float32), 0, keepdims=True)
        square = square + jnp.sum(bias * bias, 1, keepdims=True)
    row = lax.broadcasted_iota(jnp.int32, joint.shape, 0)
    joint[...] = jnp.where(row == PAD - 1, square, part)


def update_kernel(joint, hidden, hidden_own, total, selected, selected_own, onehot, encoder, *refs):
    table, enc, enc_bias, dec, dec_bias = (refs[i : i + 3] for i in range(0, 15, 3))
    norm_out, outs = refs[15], refs[16:]
    held = hidden[...]
    row = lax.broadcasted_iota(jnp.int32, held.shape, 0)
    grad = jnp.where(row < PRE, joint[...], 0.0) * (1.0 - held * held)
    grad = grad.astype(jnp.bfloat16)
    square = joint[PAD - 1 : PAD, 0:1]

    def summed(values):
        return jnp.sum(jnp.sum(values * values, 0, keepdims=True), 1, keepdims=True)

    square = square + summed(dot(selected[...], grad, TN))
    grad_bias = jnp.sum(grad.astype(jnp.float32), 0, keepdims=True)
    square = square + summed(grad_bias)
    grad_selected = dot(grad, encoder[...], NT)
    grad_table = dot(onehot[...], grad_selected, TN, lax.Precision.HIGHEST)[:PRE]
    square = square + summed(grad_table)
    norm = jnp.sqrt(square)
    norm_out[...] = norm
    factor = CLIP_LIMIT / (norm + 1e-06)

    def update(old, grad_of, at, index):
        weight, first, second = (ref[index] for ref in old)
        for out, new in zip(
            outs[at : at + 3], adam_update(weight, grad_of, first, second, factor), strict=True
        ):
            out[index] = new

    update(table, grad_table, 0, ...)
    update(enc, dot(selected_own[...], grad, TN), 3, ...)
    update(enc_bias, grad_bias, 6, ...)
    low = total[...].astype(jnp.bfloat16)
    held_own = hidden_own[...].astype(jnp.bfloat16)
    for i in range(2):
        update(dec, dot(held_own, low[i], TN), 9, (slice(None), i, slice(None)))
        bias = jnp.sum(low[i].astype(jnp.float32), 0, keepdims=True)
        update(dec_bias, bias, 12, (slice(i, i + 1), slice(None)))


def on_device(
    tokens,
    cotangent,
    norm_params,
    attention_weight,
    attention_bias,
    merge_weight,
    branch_bias,
    up_weight,
    up_bias,
    down_weight,
    prefix_ids,
    prefix_table,
    encoder_weight,
    encoder_bias,
    decoder_weight,
    decoder_bias,
    first_table,
    second_table,
    first_encoder,
    second_encoder,
    first_encoder_bias,
    second_encoder_bias,
    first_decoder,
    second_decoder,
    first_decoder_bias,
    second_decoder_bias,
):
    highest = lax.Precision.HIGHEST
    dp_index = lax.axis_index("dp")
    dp_size = lax.axis_size("dp")
    rows, width = tokens.shape
    local = merge_weight.shape[1]
    units = up_weight.shape[1]
    in_rows = attention_weight.shape[0]
    hidden_size = encoder_weight.shape[1]
    dec_rows = decoder_weight.shape[0]
    halves = hidden_size // local

    onehot = (
        jnp.pad(prefix_ids, (0, PAD - PRE), constant_values=PAD)[:, None]
        == jnp.arange(PAD, dtype=jnp.int32)[None, :]
    ).astype(jnp.float32)
    selected = jnp.dot(onehot[:, :PRE], prefix_table, precision=highest).astype(jnp.bfloat16)
    selected_own = lax.dynamic_slice_in_dim(selected, dp_index * in_rows, in_rows, 1)
    encoder_low = encoder_weight.astype(jnp.bfloat16)
    decoder_low = decoder_weight.astype(jnp.bfloat16)
    encoded_own = jnp.dot(selected_own, encoder_low, preferred_element_type=jnp.float32)
    leading = lax.reduce_precision(encoded_own, 8, 7)
    sent = jnp.stack([leading, encoded_own - leading]).astype(jnp.bfloat16)
    sent = sent.reshape(2, PAD, halves, local).transpose(0, 2, 1, 3)
    first = jnp.concatenate(
        [
            attention_weight.transpose(1, 0, 2).reshape(3 * in_rows, local),
            sent.reshape(2 * halves * PAD, local),
        ]
    )
    second = jnp.concatenate(
        [merge_weight, decoder_low.transpose(1, 0, 2).reshape(2 * dec_rows, local)]
    )
    first, second, down, up, encoder = gather_all(
        [first, second, down_weight, up_weight, encoder_low]
    )

    projected, attend_full, encoded = project(
        tokens, norm_params, attention_bias, first, hidden_size
    )
    merge_own, decoder_full = assemble(second, [(1, width, local), (2, hidden_size, local)])
    merge_own = merge_own[0]
    hidden, prefix = pl.pallas_call(
        prefix_kernel,
        out_shape=(
            shaped((PAD, hidden_size), jnp.float32),
            shaped((2, PAD, local), jnp.bfloat16),
        ),
        name="prefix",
    )(encoded, encoder_bias[None], decoder_full, decoder_bias)
    mix, log_sums = attend(projected, prefix)

    def from_others(values):
        side = swap(values, "tensor", SIDE)
        return [values, swap(values, "tensor", CORE), side, swap(side, "tensor", CORE)]

    merges = from_others(merge_own)
    mixes = from_others(mix)
    normed, resid = merge(tokens, norm_params, branch_bias, mixes, merges)
    (down_full,) = assemble(down, [(1, width, units)])
    down_full = down_full[0]
    grad_hidden = jnp.dot(cotangent, down_full, preferred_element_type=jnp.float32)
    (up_full,) = assemble(up, [(1, width, units)])
    up_full = up_full[0]

    def feed_part(*bits):
        return feed(bits, normed, grad_hidden, up_full, up_bias[None])

    def branch(act):
        part = lax.dot_general(
            act, down_full, (((2,), (1,)), ((), ())), preferred_element_type=jnp.float32
        )
        return part.astype(jnp.bfloat16)

    def plus(one, two):
        return (one.astype(jnp.float32) + two.astype(jnp.float32)).astype(jnp.bfloat16)

    act_send, up_send = feed_part(BOTH, CORE)
    up_core = swap(up_send, "tensor", CORE)
    act_side, up_keep = feed_part(SIDE)
    up_side = swap(plus(up_keep[0], up_core[0]), "tensor", SIDE)
    act_own, up_own = feed_part(OWN)
    out_core = swap(branch(act_send), "tensor", CORE)
    out_side = swap(plus(branch(act_side)[0], out_core[0]), "tensor", SIDE)
    out_own = branch(act_own)[0]
    grad_resid, keep, send = middle(
        up_own, up_core, up_side, own_rows(cotangent), resid, norm_params, merges
    )
    output = (
        resid
        + (
            out_own.astype(jnp.float32)
            + out_core[1].astype(jnp.float32)
            + out_side.astype(jnp.float32)
        )
        + branch_bias[1]
    )
    from_side = swap(send, "tensor", SIDE)
    from_core = swap(jnp.stack([keep[1], from_side[1]]), "tensor", CORE)
    grad_projected, grad_prefix = attend_back(
        projected, prefix, mix, log_sums, [keep[0], from_core[0], from_side[0], from_core[1]]
    )
    back_send = project_back((BOTH, CORE), grad_projected, attend_full)
    back_core = swap(back_send, "tensor", CORE)
    back_keep = project_back((SIDE,), grad_projected, attend_full)
    back_side = swap(plus(back_keep[0], back_core[0]), "tensor", SIDE)
    back_own = project_back((OWN,), grad_projected, attend_full)
    input_grad = pl.pallas_call(
        last_kernel,
        out_shape=shaped(resid.shape, jnp.bfloat16),
        name="last",
    )(back_own, back_core, back_side, own_rows(tokens), grad_resid, norm_params)

    prefix_total = sum_over(grad_prefix, "dp")
    joint = pl.pallas_call(
        tail_kernel, out_shape=shaped((PAD, hidden_size), jnp.float32), name="tail"
    )(prefix_total, hidden, decoder_full)
    joint = sum_over(joint, "tensor")
    (encoder_full,) = assemble(encoder, [(1, width, hidden_size)])
    hidden_own = lax.dynamic_slice_in_dim(hidden, dp_index * dec_rows, dec_rows, 1)
    params = [
        (prefix_table, first_table, second_table),
        (encoder_weight, first_encoder, second_encoder),
        (encoder_bias[None], first_encoder_bias[None], second_encoder_bias[None]),
        (decoder_weight, first_decoder, second_decoder),
        (decoder_bias, first_decoder_bias, second_decoder_bias),
    ]
    params = [array for group in params for array in group]
    grad_norm, *new = pl.pallas_call(
        update_kernel,
        out_shape=[shaped((1, 1), jnp.float32)] + [shaped(p.shape, p.dtype) for p in params],
        name="update",
    )(
        joint,
        hidden,
        hidden_own,
        prefix_total,
        selected,
        selected_own,
        onehot,
        encoder_full[0],
        *params,
    )
    for i in range(6, 9):
        new[i] = new[i][0]
    return (output.astype(jnp.bfloat16), input_grad, grad_norm[0, 0], *new)


def solution(mesh):
    in_specs = (
        P("dp", None),
        P("dp", None),
        P(),
        P("dp", None, "tensor"),
        P(None, "tensor"),
        P("dp", "tensor"),
        P(),
        P("dp", "tensor"),
        P("tensor"),
        P("dp", "tensor"),
        P(),
        P(),
        P("dp", None),
        P(),
        P("dp", None, "tensor"),
        P(None, "tensor"),
        P(),
        P(),
        P("dp", None),
        P("dp", None),
        P(),
        P(),
        P("dp", None, "tensor"),
        P("dp", None, "tensor"),
        P(None, "tensor"),
        P(None, "tensor"),
    )
    out_specs = (
        P(("dp", "tensor"), None),
        P(("dp", "tensor"), None),
        P(),
        P(),
        P(),
        P(),
        P("dp", None),
        P("dp", None),
        P("dp", None),
        P(),
        P(),
        P(),
        P("dp", None, "tensor"),
        P("dp", None, "tensor"),
        P("dp", None, "tensor"),
        P(None, "tensor"),
        P(None, "tensor"),
        P(None, "tensor"),
    )
    return jax.shard_map(
        on_device, mesh=mesh, in_specs=in_specs, out_specs=out_specs, check_vma=False
    )
```

```python
import functools

import jax
import jax.numpy as jnp
from jax import lax
from jax.experimental import pallas as pl
from jax.experimental.pallas import tpu as pltpu
from jax.sharding import PartitionSpec as P

HD = 64
PRE = 10
PAD = 16
STEP = 10
TILE = 256


NORM_EPS = 1e-05
CLIP_LIMIT = 0.001
LEARN_RATE = 0.05
WEIGHT_DECAY = 0.01
BETA_FIRST = 0.9
BETA_SECOND = 0.999
ADAM_EPS = 1e-08
MASKED = -1e30
GELU_COEF = 0.7978845608028654

NN = ((1,), (0,))
NT = ((1,), (1,))
TN = ((0,), (0,))
OWN, CORE, SIDE, BOTH = 0, 1, 2, 3


def dot(left, right, dims, precision=None):
    return lax.dot_general(
        left, right, (dims, ((), ())), precision=precision, preferred_element_type=jnp.float32
    )


def shaped(shape, dtype):
    return jax.ShapeDtypeStruct(shape, dtype)


def cost(flops, *arrays):
    size = sum(a.size * a.dtype.itemsize for a in arrays)
    return pl.CostEstimate(flops=flops, transcendentals=0, bytes_accessed=size)


def norm_parts(rows):
    offsets = rows - jnp.mean(rows, axis=-1, keepdims=True)
    scale = lax.rsqrt(jnp.mean(offsets * offsets, axis=-1, keepdims=True) + NORM_EPS)
    return offsets * scale, scale


def norm_back(rows, gain, grad):
    unit, scale = norm_parts(rows)
    grad = grad * gain
    mean = jnp.mean(grad, axis=-1, keepdims=True)
    along = jnp.mean(grad * unit, axis=-1, keepdims=True)
    return scale * (grad - mean - unit * along)


def adam_update(weight, grad, first, second, factor):
    clipped = grad * factor
    new_first = BETA_FIRST * first + (1.0 - BETA_FIRST) * clipped
    new_second = BETA_SECOND * second + (1.0 - BETA_SECOND) * clipped * clipped
    fix_first = 1.0 - BETA_FIRST**STEP
    fix_second = 1.0 - BETA_SECOND**STEP
    new_weight = weight * (1.0 - LEARN_RATE * WEIGHT_DECAY) - LEARN_RATE * (
        new_first / fix_first
    ) / (jnp.sqrt(new_second / fix_second) + ADAM_EPS)
    return (new_weight, new_first, new_second)


def swap(values, axis, bits):
    size = lax.axis_size(axis)
    return lax.ppermute(values, axis, [(i, i ^ bits) for i in range(size)])


def after(values, *others):
    return lax.optimization_barrier((values, *others))[0]


def placed(found):
    refs, bits = found
    if bits is None:
        return [(refs[0].at[i], i) for i in range(refs[0].shape[0])]
    here = lax.axis_index("dp")
    return [
        (ref.at[i], lax.bitwise_xor(here, differ))
        for ref, group in zip(refs, bits, strict=True)
        for i, differ in enumerate(group)
    ]


def joined(*pieces):
    return jnp.concatenate(pieces)


def sum_over(values, axis):
    bits = 1
    while bits < lax.axis_size(axis):
        values = values + swap(values, axis, bits)
        bits *= 2
    return values


def assemble_into(outs, found):
    for piece, place in placed(found):
        start = 0
        for out in outs:
            parts, rows = out.shape[0], out.shape[1] // lax.axis_size("dp")
            for part in range(parts):
                where = pl.ds(pl.multiple_of(place * rows, rows), rows)
                out[part, where, :] = piece[start : start + rows, :]
                start += rows


def assemble_kernel(bits, *refs):
    assemble_into(refs[-1:], (refs[:-1], bits))


def assemble(gathered, shape):
    pieces, bits = gathered
    out = shaped(shape, pieces[0].dtype)
    return pl.pallas_call(
        functools.partial(assemble_kernel, bits),
        out_shape=out,
        name="assemble",
        cost_estimate=cost(0, *pieces, out),
    )(*pieces)


def merge_weight_kernel(bits, *refs):
    pieces, (weight, encoded) = refs[:-2], refs[-2:]
    rows = weight.shape[0] // lax.axis_size("dp")
    sums = None
    for piece, place in placed((pieces, bits)):
        weight[pl.ds(pl.multiple_of(place * rows, rows), rows), :] = piece[:rows, :]
        sent = piece[rows:, :].astype(jnp.float32)
        sums = sent if sums is None else sums + sent
    width = weight.shape[1]
    for i in range(encoded.shape[1] // width):
        encoded[:, i * width : (i + 1) * width] = sums[i * PAD : (i + 1) * PAD]


def gather_merge(pieces, bits, rows, hidden):
    outs = (shaped((rows, pieces[0].shape[-1]), jnp.bfloat16), shaped((PAD, hidden), jnp.float32))
    return pl.pallas_call(
        functools.partial(merge_weight_kernel, bits),
        out_shape=outs,
        name="gather_merge",
        cost_estimate=cost(0, *pieces, *outs),
    )(*pieces)


def project_kernel(bits, tokens, norms, bias, *refs):
    pieces, (projected, attend, decoder) = refs[:-3], refs[-3:]
    assemble_into((attend, decoder), (pieces, bits))
    for start in range(0, tokens.shape[0], TILE):
        rows = slice(start, start + TILE)
        unit, _ = norm_parts(tokens[rows, :].astype(jnp.float32))
        normed = (unit * norms[0:1, :] + norms[1:2, :]).astype(jnp.bfloat16)
        for part in range(3):
            total = dot(normed, attend[part], NN) + bias[part : part + 1, :]
            projected[part, rows, :] = total.astype(jnp.bfloat16)


def project(tokens, norms, bias, gathered, hidden):
    pieces, bits = gathered
    rows, width = tokens.shape
    local = bias.shape[1]
    outs = (
        shaped((3, rows, local), jnp.bfloat16),
        shaped((3, width, local), jnp.bfloat16),
        shaped((2, hidden, local), jnp.bfloat16),
    )
    return pl.pallas_call(
        functools.partial(project_kernel, bits),
        out_shape=outs,
        name="project",
        cost_estimate=cost(6 * rows * width * local, tokens, *pieces, *outs),
    )(tokens, norms, bias, *pieces)


def down_kernel(bits, cotangent, *refs):
    pieces, (down, grad) = refs[:-2], refs[-2:]
    assemble_into((down,), (pieces, bits))
    for start in range(0, cotangent.shape[0], TILE):
        rows = slice(start, start + TILE)
        grad[rows, :] = dot(cotangent[rows, :], down[0], NN).astype(jnp.bfloat16)


def down_back(cotangent, gathered):
    pieces, bits = gathered
    rows, width = cotangent.shape
    units = pieces[0].shape[-1]
    outs = (shaped((1, width, units), jnp.bfloat16), shaped((rows, units), jnp.bfloat16))
    return pl.pallas_call(
        functools.partial(down_kernel, bits),
        out_shape=outs,
        name="down_back",
        cost_estimate=cost(2 * rows * width * units, cotangent, *pieces, *outs),
    )(cotangent, *pieces)


def prefix_kernel(encoded, encoder_bias, decoder, decoder_bias, hidden, prefix):
    held = jnp.tanh(encoded[...] + encoder_bias[...])
    hidden[...] = held
    low = held.astype(jnp.bfloat16)
    for part in range(2):
        total = dot(low, decoder[part], NN) + decoder_bias[part : part + 1, :]
        prefix[part] = total.astype(jnp.bfloat16)


def attend_kernel(first, proj, prefix, mix, sums, mixed):
    rows, width = mix.shape
    lane = lax.broadcasted_iota(jnp.int32, (1, width), 1) // HD
    pre_col = lax.broadcasted_iota(jnp.int32, (TILE, PAD), 1)
    below = lax.broadcasted_iota(jnp.int32, (TILE, TILE), 0) >= lax.broadcasted_iota(
        jnp.int32, (TILE, TILE), 1
    )
    sum_col = lax.broadcasted_iota(jnp.int32, (TILE, 128), 1)
    sums[...] = jnp.zeros_like(sums)
    mixed[...] = jnp.zeros_like(mixed)

    def one_head(head, carry):
        mine = lane == head
        for start in range(first, first + rows, TILE):
            here = slice(start, start + TILE)
            there = slice(start - first, start - first + TILE)
            query = proj[0, here, :] * jnp.asarray(HD**-0.5, jnp.bfloat16)
            one = jnp.where(mine, query, jnp.zeros_like(query))
            scores = [
                jnp.where(pre_col < PRE, dot(one, prefix[0], NT), MASKED),
                jnp.where(below, dot(one, proj[1, here, :], NT), MASKED),
            ]
            values = [prefix[1], proj[2, here, :]]
            if start:
                scores.append(dot(one, proj[1, :start, :], NT))
                values.append(proj[2, :start, :])
            top = functools.reduce(jnp.maximum, [jnp.max(s, 1, keepdims=True) for s in scores])
            exps = [jnp.exp(s - top) for s in scores]
            total = sum(jnp.sum(e, 1, keepdims=True) for e in exps)
            inverse = 1.0 / total
            part = sum(
                dot((e * inverse).astype(jnp.bfloat16), v, NN)
                for e, v in zip(exps, values, strict=True)
            )
            mixed[there, :] = jnp.where(mine, part, mixed[there, :])
            sums[there, :] = jnp.where(sum_col == head, top + jnp.log(total), sums[there, :])
        return carry

    lax.fori_loop(0, width // HD, one_head, 0)
    mix[...] = mixed[...].astype(jnp.bfloat16)


def attend_first_kernel(proj, encoded, encoder_bias, decoder, decoder_bias, mix, sums, hidden, prefix, mixed):
    prefix_kernel(encoded, encoder_bias, decoder, decoder_bias, hidden, prefix)
    attend_kernel(0, proj, prefix, mix, sums, mixed)


def attend_shapes(proj):
    _, rows, width = proj.shape
    return shaped((rows // 2, width), jnp.bfloat16), shaped((rows // 2, 128), jnp.float32)


def attend_first(proj, encoded, encoder_bias, decoder, decoder_bias):
    _, rows, width = proj.shape
    outs = (
        *attend_shapes(proj),
        shaped(encoded.shape, jnp.float32),
        shaped((2, PAD, width), jnp.bfloat16),
    )
    return pl.pallas_call(
        attend_first_kernel,
        out_shape=outs,
        scratch_shapes=[pltpu.VMEM((rows // 2, width), jnp.float32)],
        name="attend_first",
        cost_estimate=cost(5 * width // HD * rows * rows * width // 6, proj, *outs),
    )(proj, encoded, encoder_bias, decoder, decoder_bias)


def attend_second(proj, prefix):
    _, rows, width = proj.shape
    outs = attend_shapes(proj)
    return pl.pallas_call(
        functools.partial(attend_kernel, rows // 2),
        out_shape=outs,
        scratch_shapes=[pltpu.VMEM((rows // 2, width), jnp.float32)],
        name="attend_second",
        cost_estimate=cost(5 * width // HD * rows * rows * width // 3, proj, *outs),
    )(proj, prefix)


def attend_back_kernel(
    proj, prefix, mix_first, mix_second, sums_first, sums_second, own, core, side, both, gproj, gprefix, *scratch
):
    gmix, gquery, gkey, gvalue, log_sums, inner, keys_col, pre_col = scratch
    rows, width = gmix.shape
    half = rows // 2
    quarter = own.shape[0]
    me = lax.axis_index("tensor")
    for piece, bits in ((own, OWN), (core, CORE), (side, SIDE), (both, BOTH)):
        place = lax.bitwise_xor(me, bits) * quarter
        gmix[pl.ds(pl.multiple_of(place, quarter), quarter), :] = piece[...]
    lane = lax.broadcasted_iota(jnp.int32, (1, width), 1) // HD
    pre_row = lax.broadcasted_iota(jnp.int32, (PAD, TILE), 0)
    seen = lax.broadcasted_iota(jnp.int32, (TILE, TILE), 0) <= lax.broadcasted_iota(
        jnp.int32, (TILE, TILE), 1
    )
    scale = jnp.asarray(HD**-0.5, jnp.bfloat16)
    head_of = lax.broadcasted_iota(jnp.int32, (8, width), 0) == lax.broadcasted_iota(
        jnp.int32, (8, width), 1
    ) // HD
    for i, (mix, sums) in enumerate(((mix_first, sums_first), (mix_second, sums_second))):
        part = slice(i * half, (i + 1) * half)
        log_sums[:, part] = sums[...].T[:8]
        product = gmix[part, :].astype(jnp.float32) * mix[...].astype(jnp.float32)
        inner[:, part] = dot(head_of.astype(jnp.float32), product, NT, lax.Precision.HIGHEST)
    keys_col[...] = (proj[1] * scale).T
    pre_col[...] = (prefix[0] * scale).T
    gkey[...] = jnp.zeros_like(gkey)
    gvalue[...] = jnp.zeros_like(gvalue)
    gprefix[...] = jnp.zeros_like(gprefix)

    def one_head(head, carry):
        mine = lane == head
        cols = pl.ds(pl.multiple_of(head * HD, HD), HD)
        for start in range(0, rows, TILE):
            here = slice(start, start + TILE)
            query = proj[0, here, :] * scale
            grad = gmix[here, :]
            one = jnp.where(mine, query, jnp.zeros_like(query))
            one_grad = jnp.where(mine, grad, jnp.zeros_like(grad))
            log_sum = log_sums[pl.ds(head, 1), here]
            shared = inner[pl.ds(head, 1), here]

            def block(keys, values, shown):
                scores = dot(keys, one, NT)
                if shown is not None:
                    scores = jnp.where(shown, scores, MASKED)
                prob = jnp.exp(scores - log_sum)
                dscore = (prob * (dot(values, one_grad, NT) - shared)).astype(jnp.bfloat16)
                return dscore, dot(dscore, one, NN), dot(prob.astype(jnp.bfloat16), one_grad, NN)

            dscore, dkey, dvalue = block(prefix[0], prefix[1], pre_row < PRE)
            gprefix[0] += dkey
            gprefix[1] += dvalue
            dquery = dot(pre_col[cols, :], dscore, NN)
            for at in range(0, start + TILE, TILE):
                there = slice(at, at + TILE)
                dscore, dkey, dvalue = block(
                    proj[1, there, :], proj[2, there, :], seen if at == start else None
                )
                gkey[there, :] += dkey
                gvalue[there, :] += dvalue
                dquery = dquery + dot(keys_col[cols, there], dscore, NN)
            gquery[cols, here] = dquery
        return carry

    lax.fori_loop(0, width // HD, one_head, 0)
    gproj[0] = gquery[...].T.astype(jnp.bfloat16)
    gproj[1] = gkey[...].astype(jnp.bfloat16)
    gproj[2] = gvalue[...].astype(jnp.bfloat16)


def attend_back(proj, prefix, mixes, sums, pieces):
    _, rows, width = proj.shape
    outs = (shaped(proj.shape, jnp.bfloat16), shaped(prefix.shape, jnp.float32))
    return pl.pallas_call(
        attend_back_kernel,
        out_shape=outs,
        scratch_shapes=[
            pltpu.VMEM((rows, width), jnp.bfloat16),
            pltpu.VMEM((width, rows), jnp.float32),
            pltpu.VMEM((rows, width), jnp.float32),
            pltpu.VMEM((rows, width), jnp.float32),
            pltpu.VMEM((8, rows), jnp.float32),
            pltpu.VMEM((8, rows), jnp.float32),
            pltpu.VMEM((width, rows), jnp.bfloat16),
            pltpu.VMEM((width, PAD), jnp.bfloat16),
        ],
        name="attend_back",
        cost_estimate=cost(12 * width // HD * rows * rows * width // 2, proj, *mixes, *sums, *outs),
    )(proj, prefix, *mixes, *sums, *pieces)


def merge_kernel(first, tokens, norms, branch, *refs):
    mixes, merges, earlier, (normed, resid_own) = refs[:4], refs[4:8], refs[8:-2], refs[-2:]
    i = pl.program_id(0)
    merged = sum(dot(m[...], w[...], NT) for m, w in zip(mixes, merges, strict=True))
    resid = tokens[...].astype(jnp.float32) + merged + branch[0:1, :]
    unit, _ = norm_parts(resid)
    normed[...] = (unit * norms[2:3, :] + norms[3:4, :]).astype(jnp.bfloat16)
    if earlier:

        @pl.when(i == 0)
        def _():
            resid_own[...] = earlier[1][...]

    @pl.when(i + first == lax.axis_index("tensor"))
    def _():
        resid_own[...] = resid


def merge_half(tokens, norms, branch, mixes, merges, earlier=()):
    rows, width = tokens.shape
    share = rows // lax.axis_size("tensor")
    local = mixes[0].shape[1]
    steps = mixes[0].shape[0] // share
    first = steps if earlier else 0
    whole = lambda a: pl.BlockSpec(a.shape, lambda i: (0,) * a.ndim)
    outs = (shaped((rows, width), jnp.bfloat16), shaped((share, width), jnp.float32))
    return pl.pallas_call(
        functools.partial(merge_kernel, first),
        grid=(steps,),
        in_specs=[pl.BlockSpec((share, width), lambda i: (i + first, 0)), whole(norms), whole(branch)]
        + [pl.BlockSpec((share, local), lambda i: (i, 0))] * 4
        + [whole(w) for w in merges]
        + ([pl.BlockSpec(memory_space=pl.ANY), whole(earlier[1])] if earlier else []),
        out_specs=(
            pl.BlockSpec((share, width), lambda i: (i + first, 0)),
            pl.BlockSpec((share, width), lambda i: (0, 0)),
        ),
        out_shape=outs,
        input_output_aliases={11: 0} if earlier else {},
        name="merge_second" if earlier else "merge_first",
        cost_estimate=cost(4 * rows * width * local, *mixes, *merges, *outs),
    )(tokens, norms, branch, *mixes, *merges, *earlier)


def feed_rows(normed, ghidden, up, bias, act, part, plus=None):
    value = dot(normed[...], up, NN) + bias[...]
    square = value * value
    tanh = jnp.tanh(GELU_COEF * value * (1.0 + 0.044715 * square))
    act[...] = (0.5 * value * (1.0 + tanh)).astype(jnp.bfloat16)
    slope = 0.5 * (1.0 + tanh) + 0.5 * GELU_COEF * value * (1.0 - tanh * tanh) * (
        1.0 + 3.0 * 0.044715 * square
    )
    gpre = (ghidden[...].astype(jnp.float32) * slope).astype(jnp.bfloat16)
    total = dot(gpre, up, NT)
    if plus is not None:
        total = total + plus[...].astype(jnp.float32)
    part[...] = total.astype(jnp.bfloat16)


def feed_first_kernel(bits, normed, ghidden, bias, *refs):
    pieces, (act, part, up) = refs[:-3], refs[-3:]
    assemble_into((up,), (pieces, bits))
    feed_rows(normed, ghidden, up[0], bias, act, part)


def feed_kernel(count, up, bias, *refs):
    rows, plus, outs = refs[: 2 * count], refs[2 * count : -2 * count], refs[-2 * count :]
    for i in range(count):
        feed_rows(rows[2 * i], rows[2 * i + 1], up[0], bias, outs[2 * i], outs[2 * i + 1], *plus)


def block_of(differ):
    return lambda i: (lax.bitwise_xor(lax.axis_index("tensor"), differ), 0)


def whole_spec(a):
    return pl.BlockSpec(a.shape, lambda i: (0,) * a.ndim)


def feed_first(bits, normed, ghidden, gathered, bias):
    pieces, places = gathered
    rows, width = normed.shape
    share = rows // lax.axis_size("tensor")
    units = pieces[0].shape[-1]
    outs = (
        shaped((share, units), jnp.bfloat16),
        shaped((share, width), jnp.bfloat16),
        shaped((1, width, units), jnp.bfloat16),
    )
    return pl.pallas_call(
        functools.partial(feed_first_kernel, places),
        grid=(1,),
        in_specs=[
            pl.BlockSpec((share, width), block_of(bits)),
            pl.BlockSpec((share, units), block_of(bits)),
            whole_spec(bias),
        ]
        + [whole_spec(p) for p in pieces],
        out_specs=[whole_spec(o) for o in outs],
        out_shape=outs,
        name="feed_first",
        cost_estimate=cost(4 * share * width * units, *pieces, *outs),
    )(normed, ghidden, bias, *pieces)


def feed(bits, normed, ghidden, up, bias, *plus):
    rows, width = normed.shape
    share = rows // lax.axis_size("tensor")
    units = up.shape[-1]
    outs = [shaped((share, units), jnp.bfloat16), shaped((share, width), jnp.bfloat16)] * len(bits)
    specs = []
    for differ in bits:
        specs.append(pl.BlockSpec((share, width), block_of(differ)))
        specs.append(pl.BlockSpec((share, units), block_of(differ)))
    return pl.pallas_call(
        functools.partial(feed_kernel, len(bits)),
        grid=(1,),
        in_specs=[whole_spec(up), whole_spec(bias), *specs] + [whole_spec(p) for p in plus],
        out_specs=[whole_spec(o) for o in outs],
        out_shape=outs,
        name="feed",
        cost_estimate=cost(4 * len(bits) * share * width * units, up, *outs),
    )(up, bias, *[normed, ghidden] * len(bits), *plus)


def back_kernel(count, weight, *refs):
    rows, plus, outs = refs[:count], refs[count:-count], refs[-count:]
    for grad, out in zip(rows, outs, strict=True):
        total = sum(dot(grad[i], weight[i], NT) for i in range(weight.shape[0]))
        for one in plus:
            total = total + one[...].astype(jnp.float32)
        out[...] = total.astype(jnp.bfloat16)


def project_back(bits, gproj, attend, *plus):
    _, rows, local = gproj.shape
    width = attend.shape[1]
    share = rows // lax.axis_size("tensor")
    outs = [shaped((share, width), jnp.bfloat16)] * len(bits)
    specs = [
        pl.BlockSpec((3, share, local), lambda i, block=block_of(differ): (0, *block(i)))
        for differ in bits
    ]
    return pl.pallas_call(
        functools.partial(back_kernel, len(bits)),
        grid=(1,),
        in_specs=[whole_spec(attend), *specs] + [whole_spec(p) for p in plus],
        out_specs=[whole_spec(o) for o in outs],
        out_shape=outs,
        name="project_back",
        cost_estimate=cost(6 * len(bits) * share * local * width, attend, *outs),
    )(attend, *[gproj] * len(bits), *plus)


def three(own, core, side):
    return own[...].astype(jnp.float32) + core[...].astype(jnp.float32) + side[...].astype(jnp.float32)


def middle_kernel(own, core, side, cotangent, resid, norms, *refs):
    merges, (gresid, keep, send) = refs[:4], refs[4:]
    total = three(own, core, side)
    grad = cotangent[...].astype(jnp.float32) + norm_back(resid[...], norms[2:3, :], total)
    gresid[...] = grad
    low = grad.astype(jnp.bfloat16)
    keep[0] = dot(low, merges[OWN][...], NN).astype(jnp.bfloat16)
    keep[1] = dot(low, merges[CORE][...], NN).astype(jnp.bfloat16)
    send[0] = dot(low, merges[SIDE][...], NN).astype(jnp.bfloat16)
    send[1] = dot(low, merges[BOTH][...], NN).astype(jnp.bfloat16)


def middle(own, core, side, cotangent, resid, norms, merges):
    share, width = resid.shape
    local = merges[0].shape[1]
    outs = (
        shaped((share, width), jnp.float32),
        shaped((2, share, local), jnp.bfloat16),
        shaped((2, share, local), jnp.bfloat16),
    )
    mine = pl.BlockSpec((share, width), block_of(OWN))
    return pl.pallas_call(
        middle_kernel,
        grid=(1,),
        in_specs=[whole_spec(own), whole_spec(core), whole_spec(side), mine]
        + [whole_spec(a) for a in (resid, norms, *merges)],
        out_specs=[whole_spec(o) for o in outs],
        out_shape=outs,
        name="middle",
        cost_estimate=cost(8 * share * width * local, resid, *merges, *outs),
    )(own, core, side, cotangent, resid, norms, *merges)


def last_kernel(own, core, side, tokens, gresid, norms, out):
    total = three(own, core, side)
    rows = tokens[...].astype(jnp.float32)
    out[...] = (gresid[...] + norm_back(rows, norms[0:1, :], total)).astype(jnp.bfloat16)


def last(own, core, side, tokens, gresid, norms):
    share, width = gresid.shape
    out = shaped((share, width), jnp.bfloat16)
    return pl.pallas_call(
        last_kernel,
        grid=(1,),
        in_specs=[
            whole_spec(own),
            whole_spec(core),
            whole_spec(side),
            pl.BlockSpec((share, width), block_of(OWN)),
            whole_spec(gresid),
            whole_spec(norms),
        ],
        out_specs=whole_spec(out),
        out_shape=out,
        name="last",
        cost_estimate=cost(0, core, side, gresid, out),
    )(own, core, side, tokens, gresid, norms)


def tail_kernel(total, hidden, decoder, joint):
    low = total[...].astype(jnp.bfloat16)
    held = hidden[...].astype(jnp.bfloat16)
    part = jnp.zeros(joint.shape, jnp.float32)
    square = jnp.zeros((1, 1), jnp.float32)
    for i in range(2):
        part = part + dot(low[i], decoder[i], NT)
        grad = dot(held, low[i], TN)
        square = square + jnp.sum(jnp.sum(grad * grad, 0, keepdims=True), 1, keepdims=True)
        bias = jnp.sum(low[i].astype(jnp.float32), 0, keepdims=True)
        square = square + jnp.sum(bias * bias, 1, keepdims=True)
    row = lax.broadcasted_iota(jnp.int32, joint.shape, 0)
    joint[...] = jnp.where(row == PAD - 1, square, part)


def update_kernel(joint, hidden, hidden_own, total, selected, selected_own, onehot, encoder, *refs):
    table, enc, enc_bias, dec, dec_bias = (refs[i : i + 3] for i in range(0, 15, 3))
    norm_out, outs = refs[15], refs[16:]
    held = hidden[...]
    row = lax.broadcasted_iota(jnp.int32, held.shape, 0)
    grad = jnp.where(row < PRE, joint[...], 0.0) * (1.0 - held * held)
    grad = grad.astype(jnp.bfloat16)
    square = joint[PAD - 1 : PAD, 0:1]

    def summed(values):
        return jnp.sum(jnp.sum(values * values, 0, keepdims=True), 1, keepdims=True)

    square = square + summed(dot(selected[...], grad, TN))
    grad_bias = jnp.sum(grad.astype(jnp.float32), 0, keepdims=True)
    square = square + summed(grad_bias)
    grad_selected = dot(grad, encoder[...], NT)
    grad_table = dot(onehot[...], grad_selected, TN, lax.Precision.HIGHEST)[:PRE]
    square = square + summed(grad_table)
    norm = jnp.sqrt(square)
    norm_out[...] = norm
    factor = CLIP_LIMIT / (norm + 1e-06)

    def update(old, grad_of, at, index):
        weight, first, second = (ref[index] for ref in old)
        for out, new in zip(
            outs[at : at + 3], adam_update(weight, grad_of, first, second, factor), strict=True
        ):
            out[index] = new

    update(table, grad_table, 0, ...)
    update(enc, dot(selected_own[...], grad, TN), 3, ...)
    update(enc_bias, grad_bias, 6, ...)
    low = total[...].astype(jnp.bfloat16)
    held_own = hidden_own[...].astype(jnp.bfloat16)
    for i in range(2):
        update(dec, dot(held_own, low[i], TN), 9, (slice(None), i, slice(None)))
        bias = jnp.sum(low[i].astype(jnp.float32), 0, keepdims=True)
        update(dec_bias, bias, 12, (slice(i, i + 1), slice(None)))


def on_device(
    tokens,
    cotangent,
    norm_params,
    attention_weight,
    attention_bias,
    merge_weight,
    branch_bias,
    up_weight,
    up_bias,
    down_weight,
    prefix_ids,
    prefix_table,
    encoder_weight,
    encoder_bias,
    decoder_weight,
    decoder_bias,
    first_table,
    second_table,
    first_encoder,
    second_encoder,
    first_encoder_bias,
    second_encoder_bias,
    first_decoder,
    second_decoder,
    first_decoder_bias,
    second_decoder_bias,
):
    highest = lax.Precision.HIGHEST
    dp_index = lax.axis_index("dp")
    rows, width = tokens.shape
    share = rows // lax.axis_size("tensor")
    local = merge_weight.shape[1]
    units = up_weight.shape[1]
    in_rows = attention_weight.shape[0]
    hidden_size = encoder_weight.shape[1]
    dec_rows = decoder_weight.shape[0]
    halves = hidden_size // local

    decoder_low = decoder_weight.astype(jnp.bfloat16)
    attention = jnp.concatenate(
        [
            attention_weight.transpose(1, 0, 2).reshape(3 * in_rows, local),
            decoder_low.transpose(1, 0, 2).reshape(2 * dec_rows, local),
        ]
    )
    onehot = (
        jnp.pad(prefix_ids, (0, PAD - PRE), constant_values=PAD)[:, None]
        == jnp.arange(PAD, dtype=jnp.int32)[None, :]
    ).astype(jnp.float32)
    selected = jnp.dot(onehot[:, :PRE], prefix_table, precision=highest).astype(jnp.bfloat16)
    selected_own = lax.dynamic_slice_in_dim(selected, dp_index * in_rows, in_rows, 1)
    encoder_low = encoder_weight.astype(jnp.bfloat16)
    encoded_own = jnp.dot(selected_own, encoder_low, preferred_element_type=jnp.float32)
    sent = encoded_own.astype(jnp.bfloat16).reshape(PAD, halves, local).transpose(1, 0, 2)
    merging = jnp.concatenate([merge_weight, sent.reshape(halves * PAD, local)])

    small = lax.axis_size("dp") == 8
    if small:
        y, z, far = 1, 2, 4
        attention_far = swap(attention, "dp", far)
        merging_side = swap(merging, "dp", y)[None]
        down_side = swap(down_weight, "dp", y)[None]
        up_side = swap(up_weight, "dp", y)[None]
        pair = jnp.stack([attention, attention_far])
        near = swap(pair, "dp", z)
        pair_side = swap(pair, "dp", y)
        merging_pair = joined(merging[None], merging_side)
        merging_far = swap(after(merging_pair, attention_far), "dp", far)
        near_side = swap(after(near, merging_far), "dp", y)
        attention = ((pair, near, pair_side, near_side), ((0, 4), (2, 6), (1, 5), (3, 7)))
        merging_quad = joined(merging_pair, merging_far)
        merging_near = swap(merging_quad, "dp", z)
        merging = ((merging_quad, merging_near), ((0, 1, 4, 5), (2, 3, 6, 7)))
        down_far = swap(after(down_weight, near), "dp", far)[None]
    else:
        gathered = lambda shard: ((lax.all_gather(shard, "dp", axis=0),), None)
        attention, merging, down, up, encoder = map(
            gathered, (attention, merging, down_weight, up_weight, encoder_low)
        )

    projected, attend_full, decoder_full = project(
        tokens, norm_params, attention_bias, attention, hidden_size
    )
    if small:
        down_far = after(down_far, projected)
        down_near = swap(joined(down_weight[None], down_far), "dp", z)
        down_far_side = swap(down_far, "dp", y)
        up_far = swap(after(up_weight, down_far), "dp", far)[None]
    merge_own, encoded = gather_merge(after(merging[0], projected), merging[1], width, hidden_size)
    mix_first, sums_first, hidden, prefix = attend_first(
        projected, encoded, encoder_bias[None], decoder_full, decoder_bias
    )

    def from_others(values):
        side = swap(values, "tensor", SIDE)
        return [values, swap(values, "tensor", CORE), side, swap(side, "tensor", CORE)]

    merges = from_others(merge_own)
    mixes_first = from_others(mix_first)
    mix_second, sums_second = attend_second(projected, prefix)
    mixes_second = from_others(mix_second)
    if small:
        down_near = after(down_near, mix_second)
        down_near_side = swap(down_near, "dp", y)
        down = (
            (down_weight[None], down_side, down_far, down_far_side, down_near, down_near_side),
            ((0,), (1,), (4,), (5,), (2, 6), (3, 7)),
        )
        up_far = after(up_far, mix_second)
        up_near = swap(joined(up_weight[None], up_far), "dp", z)
        up_far_side = swap(up_far, "dp", y)
    first_half = merge_half(tokens, norm_params, branch_bias, mixes_first, merges)
    down_full, grad_hidden = down_back(after(cotangent, first_half), down)
    if small:
        up_near_side = swap(up_near, "dp", y)
        up = (
            (up_weight[None], up_side, up_far, up_far_side, up_near, up_near_side),
            ((0,), (1,), (4,), (5,), (2, 6), (3, 7)),
        )
        encoder_far = swap(after(encoder_low, up_near), "dp", far)
        encoder_pair = jnp.stack([encoder_low, encoder_far])
    normed, resid = merge_half(
        tokens, norm_params, branch_bias, mixes_second, merges, after(first_half, grad_hidden)
    )

    def branch(act, *plus):
        part = lax.dot_general(
            act, down_full[0], (((1,), (1,)), ((), ())), preferred_element_type=jnp.float32
        )
        for one in plus:
            part = part + one.astype(jnp.float32)
        return part.astype(jnp.bfloat16)

    bias = up_bias[None]
    act_both, up_both, up_full = feed_first(BOTH, normed, grad_hidden, up, bias)
    up_both = swap(up_both, "tensor", CORE)
    out_both = branch(act_both)
    if small:
        encoder_near = swap(after(encoder_pair, normed), "dp", z)
        up_both = after(up_both, encoder_near)
    act_side, up_send = feed(
        (SIDE,), normed, grad_hidden, up_full, bias, after(up_both, out_both)
    )
    up_from = swap(up_send, "tensor", SIDE)
    out_both = swap(out_both, "tensor", CORE)
    if small:
        encoder_quad = joined(encoder_pair, encoder_near)
        encoder_side = swap(after(encoder_quad, up_send), "dp", y)
        encoder = ((encoder_quad, encoder_side), ((0, 4, 2, 6), (1, 5, 3, 7)))
    act_core, up_core, act_own, up_own = feed(
        (CORE, OWN), after(normed, up_send), grad_hidden, up_full, bias
    )
    up_core = swap(up_core, "tensor", CORE)
    out_core = branch(act_core)
    up_from, up_core = after((up_from, up_core), out_core)
    grad_resid, keep, send = middle(up_own, up_core, up_from, cotangent, resid, norm_params, merges)
    from_side = swap(send, "tensor", SIDE)
    out_core = swap(out_core, "tensor", CORE)
    out_send = branch(after(act_side, send), out_both)
    out_from = swap(out_send, "tensor", SIDE)
    out_own = branch(after(act_own, send))
    from_side = after(from_side, out_own, out_send)
    from_core = swap(jnp.stack([keep[1], from_side[1]]), "tensor", CORE)
    if small:
        from_core = after(from_core, encoder_side)
    grad_projected, grad_prefix = attend_back(
        projected,
        prefix,
        (mix_first, mix_second),
        (sums_first, sums_second),
        [keep[0], from_core[0], from_side[0], from_core[1]],
    )
    (back_both,) = project_back((BOTH,), grad_projected, attend_full)
    back_both = swap(back_both, "tensor", CORE)
    (back_send,) = project_back((SIDE,), grad_projected, attend_full, back_both)
    back_from = swap(back_send, "tensor", SIDE)
    back_core, back_own = project_back(
        (CORE, OWN), after(grad_projected, back_send), attend_full
    )
    back_core = swap(back_core, "tensor", CORE)
    output = (
        resid
        + (
            out_own.astype(jnp.float32)
            + out_core.astype(jnp.float32)
            + out_from.astype(jnp.float32)
        )
        + branch_bias[1]
    )
    input_grad = last(back_own, back_core, back_from, tokens, grad_resid, norm_params)

    prefix_total = sum_over(grad_prefix, "dp")
    joint = pl.pallas_call(
        tail_kernel, out_shape=shaped((PAD, hidden_size), jnp.float32), name="tail"
    )(prefix_total, hidden, decoder_full)
    joint = sum_over(joint, "tensor")
    encoder_full = assemble(encoder, (1, width, hidden_size))
    hidden_own = lax.dynamic_slice_in_dim(hidden, dp_index * dec_rows, dec_rows, 1)
    params = [
        (prefix_table, first_table, second_table),
        (encoder_weight, first_encoder, second_encoder),
        (encoder_bias[None], first_encoder_bias[None], second_encoder_bias[None]),
        (decoder_weight, first_decoder, second_decoder),
        (decoder_bias, first_decoder_bias, second_decoder_bias),
    ]
    params = [array for group in params for array in group]
    grad_norm, *new = pl.pallas_call(
        update_kernel,
        out_shape=[shaped((1, 1), jnp.float32)] + [shaped(p.shape, p.dtype) for p in params],
        name="update",
    )(
        joint,
        hidden,
        hidden_own,
        prefix_total,
        selected,
        selected_own,
        onehot,
        encoder_full[0],
        *params,
    )
    for i in range(6, 9):
        new[i] = new[i][0]
    return (output.astype(jnp.bfloat16), input_grad, grad_norm[0, 0], *new)


def solution(mesh):
    in_specs = (
        P("dp", None),
        P("dp", None),
        P(),
        P("dp", None, "tensor"),
        P(None, "tensor"),
        P("dp", "tensor"),
        P(),
        P("dp", "tensor"),
        P("tensor"),
        P("dp", "tensor"),
        P(),
        P(),
        P("dp", None),
        P(),
        P("dp", None, "tensor"),
        P(None, "tensor"),
        P(),
        P(),
        P("dp", None),
        P("dp", None),
        P(),
        P(),
        P("dp", None, "tensor"),
        P("dp", None, "tensor"),
        P(None, "tensor"),
        P(None, "tensor"),
    )
    out_specs = (
        P(("dp", "tensor"), None),
        P(("dp", "tensor"), None),
        P(),
        P(),
        P(),
        P(),
        P("dp", None),
        P("dp", None),
        P("dp", None),
        P(),
        P(),
        P(),
        P("dp", None, "tensor"),
        P("dp", None, "tensor"),
        P("dp", None, "tensor"),
        P(None, "tensor"),
        P(None, "tensor"),
        P(None, "tensor"),
    )
    return jax.shard_map(
        on_device, mesh=mesh, in_specs=in_specs, out_specs=out_specs, check_vma=False
    )
```

```python
import functools

import jax
import jax.numpy as jnp
from jax import lax
from jax.experimental import pallas as pl
from jax.experimental.pallas import tpu as pltpu
from jax.sharding import PartitionSpec as P

HD = 64
PRE = 10
PAD = 16
STEP = 10
TILE = 256


NORM_EPS = 1e-05
CLIP_LIMIT = 0.001
LEARN_RATE = 0.05
WEIGHT_DECAY = 0.01
BETA_FIRST = 0.9
BETA_SECOND = 0.999
ADAM_EPS = 1e-08
MASKED = -1e30
GELU_COEF = 0.7978845608028654

NN = ((1,), (0,))
NT = ((1,), (1,))
TN = ((0,), (0,))
OWN, CORE, SIDE, BOTH = 0, 1, 2, 3


def dot(left, right, dims, precision=None):
    return lax.dot_general(
        left, right, (dims, ((), ())), precision=precision, preferred_element_type=jnp.float32
    )


def shaped(shape, dtype):
    return jax.ShapeDtypeStruct(shape, dtype)


def limited():
    return pltpu.CompilerParams(vmem_limit_bytes=24 * 2**20)


def cost(flops, *arrays):
    size = sum(a.size * a.dtype.itemsize for a in arrays)
    return pl.CostEstimate(flops=flops, transcendentals=0, bytes_accessed=size)


def brief():
    return pl.CostEstimate(flops=0, transcendentals=0, bytes_accessed=0)


def norm_parts(rows):
    offsets = rows - jnp.mean(rows, axis=-1, keepdims=True)
    scale = lax.rsqrt(jnp.mean(offsets * offsets, axis=-1, keepdims=True) + NORM_EPS)
    return offsets * scale, scale


def norm_back(rows, gain, grad):
    unit, scale = norm_parts(rows)
    grad = grad * gain
    mean = jnp.mean(grad, axis=-1, keepdims=True)
    along = jnp.mean(grad * unit, axis=-1, keepdims=True)
    return scale * (grad - mean - unit * along)


def adam_update(weight, grad, first, second, factor):
    clipped = grad * factor
    new_first = BETA_FIRST * first + (1.0 - BETA_FIRST) * clipped
    new_second = BETA_SECOND * second + (1.0 - BETA_SECOND) * clipped * clipped
    fix_first = 1.0 - BETA_FIRST**STEP
    fix_second = 1.0 - BETA_SECOND**STEP
    new_weight = weight * (1.0 - LEARN_RATE * WEIGHT_DECAY) - LEARN_RATE * (
        new_first / fix_first
    ) / (jnp.sqrt(new_second / fix_second) + ADAM_EPS)
    return (new_weight, new_first, new_second)


def swap(values, axis, bits):
    size = lax.axis_size(axis)
    return lax.ppermute(values, axis, [(i, i ^ bits) for i in range(size)])


def after(values, *others):
    return lax.optimization_barrier((values, *others))[0]


def placed(found):
    refs, bits = found
    if bits is None:
        return [(refs[0].at[i], i) for i in range(refs[0].shape[0])]
    here = lax.axis_index("dp")
    return [
        (ref.at[i], lax.bitwise_xor(here, differ))
        for ref, group in zip(refs, bits, strict=True)
        for i, differ in enumerate(group)
    ]


def joined(*pieces):
    return jnp.concatenate(pieces)


def sum_over(values, axis):
    bits = 1
    while bits < lax.axis_size(axis):
        values = values + swap(values, axis, bits)
        bits *= 2
    return values


def assemble_into(outs, found):
    for piece, place in placed(found):
        start = 0
        for out in outs:
            parts, rows = out.shape[0], out.shape[1] // lax.axis_size("dp")
            for part in range(parts):
                where = pl.ds(pl.multiple_of(place * rows, rows), rows)
                out[part, where, :] = piece[start : start + rows, :]
                start += rows


def assemble_kernel(bits, *refs):
    assemble_into(refs[-1:], (refs[:-1], bits))


def assemble(gathered, shape):
    pieces, bits = gathered
    out = shaped(shape, pieces[0].dtype)
    return pl.pallas_call(
        functools.partial(assemble_kernel, bits),
        out_shape=out,
        compiler_params=limited(),
        name="assemble",
        cost_estimate=brief(),
    )(*pieces)


def merge_weight_kernel(bits, *refs):
    pieces, (weight, encoded) = refs[:-2], refs[-2:]
    rows = weight.shape[0] // lax.axis_size("dp")
    sums = None
    for piece, place in placed((pieces, bits)):
        weight[pl.ds(pl.multiple_of(place * rows, rows), rows), :] = piece[:rows, :]
        sent = piece[rows:, :].astype(jnp.float32)
        sums = sent if sums is None else sums + sent
    width = weight.shape[1]
    for i in range(encoded.shape[1] // width):
        encoded[:, i * width : (i + 1) * width] = sums[i * PAD : (i + 1) * PAD]


def gather_merge(pieces, bits, rows, hidden):
    outs = (shaped((rows, pieces[0].shape[-1]), jnp.bfloat16), shaped((PAD, hidden), jnp.float32))
    return pl.pallas_call(
        functools.partial(merge_weight_kernel, bits),
        out_shape=outs,
        compiler_params=limited(),
        name="gather_merge",
        cost_estimate=brief(),
    )(*pieces)


def project_kernel(bits, tokens, norms, bias, *refs):
    pieces, (projected, attend, decoder) = refs[:-3], refs[-3:]
    assemble_into((attend, decoder), (pieces, bits))
    for start in range(0, tokens.shape[0], TILE):
        rows = slice(start, start + TILE)
        unit, _ = norm_parts(tokens[rows, :].astype(jnp.float32))
        normed = (unit * norms[0:1, :] + norms[1:2, :]).astype(jnp.bfloat16)
        for part in range(3):
            total = dot(normed, attend[part], NN) + bias[part : part + 1, :]
            projected[part, rows, :] = total.astype(jnp.bfloat16)


def project(tokens, norms, bias, gathered, hidden):
    pieces, bits = gathered
    rows, width = tokens.shape
    local = bias.shape[1]
    outs = (
        shaped((3, rows, local), jnp.bfloat16),
        shaped((3, width, local), jnp.bfloat16),
        shaped((2, hidden, local), jnp.bfloat16),
    )
    return pl.pallas_call(
        functools.partial(project_kernel, bits),
        out_shape=outs,
        compiler_params=limited(),
        name="project",
        cost_estimate=brief(),
    )(tokens, norms, bias, *pieces)


def down_kernel(bits, cotangent, *refs):
    pieces, (down, grad) = refs[:-2], refs[-2:]
    assemble_into((down,), (pieces, bits))
    for start in range(0, cotangent.shape[0], TILE):
        rows = slice(start, start + TILE)
        grad[rows, :] = dot(cotangent[rows, :], down[0], NN).astype(jnp.bfloat16)


def down_back(cotangent, gathered):
    pieces, bits = gathered
    rows, width = cotangent.shape
    units = pieces[0].shape[-1]
    outs = (shaped((1, width, units), jnp.bfloat16), shaped((rows, units), jnp.bfloat16))
    return pl.pallas_call(
        functools.partial(down_kernel, bits),
        out_shape=outs,
        compiler_params=limited(),
        name="down_back",
        cost_estimate=brief(),
    )(cotangent, *pieces)


def prefix_kernel(encoded, encoder_bias, decoder, decoder_bias, hidden, prefix):
    held = jnp.tanh(encoded[...] + encoder_bias[...])
    hidden[...] = held
    low = held.astype(jnp.bfloat16)
    for part in range(2):
        total = dot(low, decoder[part], NN) + decoder_bias[part : part + 1, :]
        prefix[part] = total.astype(jnp.bfloat16)


def attend_kernel(first, proj, prefix, mix, sums, mixed):
    rows, width = mix.shape
    lane = lax.broadcasted_iota(jnp.int32, (1, width), 1) // HD
    pre_col = lax.broadcasted_iota(jnp.int32, (TILE, PAD), 1)
    below = lax.broadcasted_iota(jnp.int32, (TILE, TILE), 0) >= lax.broadcasted_iota(
        jnp.int32, (TILE, TILE), 1
    )
    sum_col = lax.broadcasted_iota(jnp.int32, (TILE, 128), 1)
    sums[...] = jnp.zeros_like(sums)
    mixed[...] = jnp.zeros_like(mixed)

    def one_head(head, carry):
        mine = lane == head
        for start in range(first, first + rows, TILE):
            here = slice(start, start + TILE)
            there = slice(start - first, start - first + TILE)
            query = proj[0, here, :] * jnp.asarray(HD**-0.5, jnp.bfloat16)
            one = jnp.where(mine, query, jnp.zeros_like(query))
            scores = [
                jnp.where(pre_col < PRE, dot(one, prefix[0], NT), MASKED),
                jnp.where(below, dot(one, proj[1, here, :], NT), MASKED),
            ]
            values = [prefix[1], proj[2, here, :]]
            if start:
                scores.append(dot(one, proj[1, :start, :], NT))
                values.append(proj[2, :start, :])
            top = functools.reduce(jnp.maximum, [jnp.max(s, 1, keepdims=True) for s in scores])
            exps = [jnp.exp(s - top) for s in scores]
            total = sum(jnp.sum(e, 1, keepdims=True) for e in exps)
            inverse = 1.0 / total
            part = sum(
                dot((e * inverse).astype(jnp.bfloat16), v, NN)
                for e, v in zip(exps, values, strict=True)
            )
            mixed[there, :] = jnp.where(mine, part, mixed[there, :])
            sums[there, :] = jnp.where(sum_col == head, top + jnp.log(total), sums[there, :])
        return carry

    lax.fori_loop(0, width // HD, one_head, 0)
    mix[...] = mixed[...].astype(jnp.bfloat16)


def attend_first_kernel(proj, encoded, encoder_bias, decoder, decoder_bias, mix, sums, hidden, prefix, mixed):
    prefix_kernel(encoded, encoder_bias, decoder, decoder_bias, hidden, prefix)
    attend_kernel(0, proj, prefix, mix, sums, mixed)


def attend_shapes(proj):
    _, rows, width = proj.shape
    return shaped((rows // 2, width), jnp.bfloat16), shaped((rows // 2, 128), jnp.float32)


def attend_first(proj, encoded, encoder_bias, decoder, decoder_bias):
    _, rows, width = proj.shape
    outs = (
        *attend_shapes(proj),
        shaped(encoded.shape, jnp.float32),
        shaped((2, PAD, width), jnp.bfloat16),
    )
    return pl.pallas_call(
        attend_first_kernel,
        out_shape=outs,
        scratch_shapes=[pltpu.VMEM((rows // 2, width), jnp.float32)],
        compiler_params=limited(),
        name="attend_first",
        cost_estimate=brief(),
    )(proj, encoded, encoder_bias, decoder, decoder_bias)


def attend_second(proj, prefix):
    _, rows, width = proj.shape
    outs = attend_shapes(proj)
    return pl.pallas_call(
        functools.partial(attend_kernel, rows // 2),
        out_shape=outs,
        scratch_shapes=[pltpu.VMEM((rows // 2, width), jnp.float32)],
        compiler_params=limited(),
        name="attend_second",
        cost_estimate=brief(),
    )(proj, prefix)


def prefix_back_kernel(
    query, prefix, mix_first, mix_second, sums_first, sums_second, keep, side, core_keep, core_side, *refs
):
    gprefix, gmix, log_sums, inner, gquery = refs
    rows, width = gmix.shape
    half = rows // 2
    quarter = keep.shape[1]
    heads = width // HD
    me = lax.axis_index("tensor")
    for piece, bits in ((keep.at[0], OWN), (core_keep.at[1], CORE), (side.at[0], SIDE), (core_side.at[1], BOTH)):
        place = lax.bitwise_xor(me, bits) * quarter
        gmix[pl.ds(pl.multiple_of(place, quarter), quarter), :] = piece[...]
    head_of = lax.broadcasted_iota(jnp.int32, (8, width), 0) == lax.broadcasted_iota(
        jnp.int32, (8, width), 1
    ) // HD
    for i, (mix, sums) in enumerate(((mix_first, sums_first), (mix_second, sums_second))):
        part = slice(i * half, (i + 1) * half)
        log_sums[:, part] = sums[...].T[:8]
        product = gmix[part, :].astype(jnp.float32) * mix[...].astype(jnp.float32)
        inner[:, part] = dot(head_of.astype(jnp.float32), product, NT, lax.Precision.HIGHEST)
    lane = lax.broadcasted_iota(jnp.int32, (PAD, width), 1) // HD
    zero = jnp.zeros((PAD, width), jnp.bfloat16)
    keys, values = (
        jnp.concatenate([jnp.where(lane == head, prefix[i], zero) for head in range(heads)])
        for i in range(2)
    )
    scale = jnp.asarray(HD**-0.5, jnp.bfloat16)

    def spread(of_heads):
        return jnp.concatenate(
            [jnp.broadcast_to(of_heads[head : head + 1, :], (PAD, rows)) for head in range(heads)]
        )

    scaled = query[0] * scale
    grad = gmix[...]
    position = lax.broadcasted_iota(jnp.int32, (heads * PAD, rows), 0) % PAD
    scores = jnp.where(position < PRE, dot(keys, scaled, NT), MASKED)
    prob = jnp.exp(scores - spread(log_sums))
    dscore = (prob * (dot(values, grad, NT) - spread(inner))).astype(jnp.bfloat16)
    dkeys = dot(dscore, scaled, NN)
    dvalues = dot(prob.astype(jnp.bfloat16), grad, NN)
    for i, found in enumerate((dkeys, dvalues)):
        gprefix[i] = sum(
            jnp.where(lane == head, found[head * PAD : (head + 1) * PAD], 0.0)
            for head in range(heads)
        )
    gquery[...] = dot(keys * scale, dscore, TN)


def prefix_back(proj, prefix, mixes, sums, pieces):
    _, rows, width = proj.shape
    outs = (
        shaped(prefix.shape, jnp.float32),
        shaped((rows, width), jnp.bfloat16),
        shaped((8, rows), jnp.float32),
        shaped((8, rows), jnp.float32),
        shaped((width, rows), jnp.float32),
    )
    return pl.pallas_call(
        prefix_back_kernel,
        grid=(1,),
        in_specs=[pl.BlockSpec((1, rows, width), lambda i: (0, 0, 0))]
        + [whole_spec(a) for a in (prefix, *mixes, *sums, *pieces)],
        out_specs=[whole_spec(o) for o in outs],
        out_shape=outs,
        compiler_params=limited(),
        name="prefix_back",
        cost_estimate=brief(),
    )(proj, prefix, *mixes, *sums, *pieces)


def attend_back_kernel(pair, proj, gmix, log_sums, inner, gquery_prefix, gproj, gquery, gkey, gvalue, keys_col):
    rows, width = gmix.shape
    lane = lax.broadcasted_iota(jnp.int32, (1, width), 1) // HD
    seen = lax.broadcasted_iota(jnp.int32, (TILE, TILE), 0) <= lax.broadcasted_iota(
        jnp.int32, (TILE, TILE), 1
    )
    scale = jnp.asarray(HD**-0.5, jnp.bfloat16)
    keys_col[...] = (proj[1] * scale).T
    gkey[...] = jnp.zeros_like(gkey)
    gvalue[...] = jnp.zeros_like(gvalue)

    def one_head(head, carry):
        mine = lane == head
        cols = pl.ds(pl.multiple_of(head * HD, HD), HD)
        row = pl.ds(pair * (width // HD) + head, 1)
        for start in range(0, rows, TILE):
            here = slice(start, start + TILE)
            query = proj[0, here, :] * scale
            grad = gmix[here, :]
            one = jnp.where(mine, query, jnp.zeros_like(query))
            one_grad = jnp.where(mine, grad, jnp.zeros_like(grad))
            log_sum = log_sums[row, here]
            shared = inner[row, here]
            dquery = gquery_prefix[cols, here]
            for at in range(0, start + TILE, TILE):
                there = slice(at, at + TILE)
                scores = dot(proj[1, there, :], one, NT)
                if at == start:
                    scores = jnp.where(seen, scores, MASKED)
                prob = jnp.exp(scores - log_sum)
                dscore = prob * (dot(proj[2, there, :], one_grad, NT) - shared)
                dscore = dscore.astype(jnp.bfloat16)
                gkey[there, :] += dot(dscore, one, NN)
                gvalue[there, :] += dot(prob.astype(jnp.bfloat16), one_grad, NN)
                dquery = dquery + dot(keys_col[cols, there], dscore, NN)
            gquery[cols, here] = dquery
        return carry

    lax.fori_loop(0, width // HD, one_head, 0)
    gproj[0] = gquery[...].T.astype(jnp.bfloat16)
    gproj[1] = gkey[...].astype(jnp.bfloat16)
    gproj[2] = gvalue[...].astype(jnp.bfloat16)


def attend_back(pair, proj, gmix, log_sums, inner, gquery):
    _, rows, local = proj.shape
    width = 2 * HD
    out = shaped((3, rows, width), jnp.bfloat16)
    return pl.pallas_call(
        functools.partial(attend_back_kernel, pair),
        grid=(1,),
        in_specs=[
            pl.BlockSpec((3, rows, width), lambda i: (0, 0, pair)),
            pl.BlockSpec((rows, width), lambda i: (0, pair)),
            whole_spec(log_sums),
            whole_spec(inner),
            pl.BlockSpec((width, rows), lambda i: (pair, 0)),
        ],
        out_specs=whole_spec(out),
        out_shape=out,
        scratch_shapes=[
            pltpu.VMEM((width, rows), jnp.float32),
            pltpu.VMEM((rows, width), jnp.float32),
            pltpu.VMEM((rows, width), jnp.float32),
            pltpu.VMEM((width, rows), jnp.bfloat16),
        ],
        compiler_params=limited(),
        name="attend_back",
        cost_estimate=cost(12 * rows * rows * width, proj, gmix, gquery, out),
    )(proj, gmix, log_sums, inner, gquery)


def four(refs):
    own, side, other = refs
    return own, other.at[0], side, other.at[1]


def merge_kernel(first, tokens, norms, branch, *refs):
    mixes, merges, earlier, (normed, resid_own) = refs[:3], refs[3:6], refs[6:-2], refs[-2:]
    i = pl.program_id(0)
    merged = sum(dot(m[...], w[...], NT) for m, w in zip(four(mixes), four(merges), strict=True))
    resid = tokens[...].astype(jnp.float32) + merged + branch[0:1, :]
    unit, _ = norm_parts(resid)
    normed[...] = (unit * norms[2:3, :] + norms[3:4, :]).astype(jnp.bfloat16)
    if earlier:

        @pl.when(i == 0)
        def _():
            resid_own[...] = earlier[1][...]

    @pl.when(i + first == lax.axis_index("tensor"))
    def _():
        resid_own[...] = resid


def merge_half(tokens, norms, branch, mixes, merges, earlier=()):
    rows, width = tokens.shape
    share = rows // lax.axis_size("tensor")
    local = mixes[0].shape[1]
    steps = mixes[0].shape[0] // share
    first = steps if earlier else 0
    whole = lambda a: pl.BlockSpec(a.shape, lambda i: (0,) * a.ndim)
    outs = (shaped((rows, width), jnp.bfloat16), shaped((share, width), jnp.float32))
    return pl.pallas_call(
        functools.partial(merge_kernel, first),
        grid=(steps,),
        in_specs=[pl.BlockSpec((share, width), lambda i: (i + first, 0)), whole(norms), whole(branch)]
        + [pl.BlockSpec((share, local), lambda i: (i, 0))] * 2
        + [pl.BlockSpec((2, share, local), lambda i: (0, i, 0))]
        + [whole(w) for w in merges]
        + ([pl.BlockSpec(memory_space=pl.ANY), whole(earlier[1])] if earlier else []),
        out_specs=(
            pl.BlockSpec((share, width), lambda i: (i + first, 0)),
            pl.BlockSpec((share, width), lambda i: (0, 0)),
        ),
        out_shape=outs,
        input_output_aliases={9: 0} if earlier else {},
        compiler_params=limited(),
        name="merge_second" if earlier else "merge_first",
        cost_estimate=brief(),
    )(tokens, norms, branch, *mixes, *merges, *earlier)


def feed_rows(normed, ghidden, up, bias, act, part, plus=None):
    value = dot(normed[...], up, NN) + bias[...]
    square = value * value
    tanh = jnp.tanh(GELU_COEF * value * (1.0 + 0.044715 * square))
    act[...] = (0.5 * value * (1.0 + tanh)).astype(jnp.bfloat16)
    slope = 0.5 * (1.0 + tanh) + 0.5 * GELU_COEF * value * (1.0 - tanh * tanh) * (
        1.0 + 3.0 * 0.044715 * square
    )
    gpre = (ghidden[...].astype(jnp.float32) * slope).astype(jnp.bfloat16)
    total = dot(gpre, up, NT)
    if plus is not None:
        total = total + plus[...].astype(jnp.float32)
    part[...] = total.astype(jnp.bfloat16)


def feed_first_kernel(bits, normed, ghidden, bias, *refs):
    pieces, (act, part, up) = refs[:-3], refs[-3:]
    assemble_into((up,), (pieces, bits))
    feed_rows(normed, ghidden, up[0], bias, act, part)


def feed_kernel(up, bias, normed, ghidden, *refs):
    feed_rows(normed, ghidden, up[0], bias, *refs[-2:], *refs[:-2])


def block_of(*bits):
    last = len(bits) - 1
    return lambda i: (lax.bitwise_xor(lax.axis_index("tensor"), bits[0] if not last else last - i), 0)


def whole_spec(a):
    return pl.BlockSpec(a.shape, lambda i: (0,) * a.ndim)


def feed_first(bits, normed, ghidden, gathered, bias):
    pieces, places = gathered
    rows, width = normed.shape
    share = rows // lax.axis_size("tensor")
    units = pieces[0].shape[-1]
    outs = (
        shaped((share, units), jnp.bfloat16),
        shaped((share, width), jnp.bfloat16),
        shaped((1, width, units), jnp.bfloat16),
    )
    return pl.pallas_call(
        functools.partial(feed_first_kernel, places),
        grid=(1,),
        in_specs=[
            pl.BlockSpec((share, width), block_of(bits)),
            pl.BlockSpec((share, units), block_of(bits)),
            whole_spec(bias),
        ]
        + [whole_spec(p) for p in pieces],
        out_specs=[whole_spec(o) for o in outs],
        out_shape=outs,
        compiler_params=limited(),
        name="feed_first",
        cost_estimate=brief(),
    )(normed, ghidden, bias, *pieces)


def feed(bits, normed, ghidden, up, bias, *plus):
    rows, width = normed.shape
    share = rows // lax.axis_size("tensor")
    units = up.shape[-1]
    steps = len(bits)
    outs = (
        shaped((steps * share, units), jnp.bfloat16),
        shaped((steps * share, width), jnp.bfloat16),
    )
    return pl.pallas_call(
        feed_kernel,
        grid=(steps,),
        in_specs=[
            whole_spec(up),
            whole_spec(bias),
            pl.BlockSpec((share, width), block_of(*bits)),
            pl.BlockSpec((share, units), block_of(*bits)),
        ]
        + [whole_spec(p) for p in plus],
        out_specs=[
            pl.BlockSpec((share, units), lambda i: (i, 0)),
            pl.BlockSpec((share, width), lambda i: (i, 0)),
        ],
        out_shape=outs,
        compiler_params=limited(),
        name="feed",
        cost_estimate=brief(),
    )(up, bias, normed, ghidden, *plus)


def back_kernel(weight, one, two, *refs):
    total = sum(
        dot(jnp.concatenate([one[i], two[i]], axis=1), weight[i], NT) for i in range(weight.shape[0])
    )
    for plus in refs[:-1]:
        total = total + plus[...].astype(jnp.float32)
    refs[-1][...] = total.astype(jnp.bfloat16)


def project_back(bits, gprojs, attend, *plus):
    _, rows, local = gprojs[0].shape
    width = attend.shape[1]
    share = rows // lax.axis_size("tensor")
    steps = len(bits)
    block = block_of(*bits)
    out = shaped((steps * share, width), jnp.bfloat16)
    return pl.pallas_call(
        back_kernel,
        grid=(steps,),
        in_specs=[whole_spec(attend)]
        + [pl.BlockSpec((3, share, local), lambda i: (0, *block(i)))] * 2
        + [whole_spec(p) for p in plus],
        out_specs=pl.BlockSpec((share, width), lambda i: (i, 0)),
        out_shape=out,
        compiler_params=limited(),
        name="project_back",
        cost_estimate=brief(),
    )(attend, *gprojs, *plus)


def three(own, core, side):
    return own[...].astype(jnp.float32) + core[...].astype(jnp.float32) + side[...].astype(jnp.float32)


def middle_kernel(own, core, side, cotangent, resid, norms, *refs):
    merges, (gresid, keep, send) = four(refs[:3]), refs[3:]
    total = three(own, core, side)
    grad = cotangent[...].astype(jnp.float32) + norm_back(resid[...], norms[2:3, :], total)
    gresid[...] = grad
    low = grad.astype(jnp.bfloat16)
    keep[0] = dot(low, merges[OWN][...], NN).astype(jnp.bfloat16)
    keep[1] = dot(low, merges[CORE][...], NN).astype(jnp.bfloat16)
    send[0] = dot(low, merges[SIDE][...], NN).astype(jnp.bfloat16)
    send[1] = dot(low, merges[BOTH][...], NN).astype(jnp.bfloat16)


def row_of(share, width, step):
    return pl.BlockSpec((share, width), lambda i: (step, 0))


def middle(own, core, side, cotangent, resid, norms, merges):
    share, width = resid.shape
    local = merges[0].shape[1]
    outs = (
        shaped((share, width), jnp.float32),
        shaped((2, share, local), jnp.bfloat16),
        shaped((2, share, local), jnp.bfloat16),
    )
    mine = pl.BlockSpec((share, width), block_of(OWN))
    return pl.pallas_call(
        middle_kernel,
        grid=(1,),
        in_specs=[row_of(share, width, 1), row_of(share, width, 0), whole_spec(side), mine]
        + [whole_spec(a) for a in (resid, norms, *merges)],
        out_specs=[whole_spec(o) for o in outs],
        out_shape=outs,
        compiler_params=limited(),
        name="middle",
        cost_estimate=brief(),
    )(own, core, side, cotangent, resid, norms, *merges)


def last_kernel(own, core, side, tokens, gresid, norms, out):
    total = three(own, core, side)
    rows = tokens[...].astype(jnp.float32)
    out[...] = (gresid[...] + norm_back(rows, norms[0:1, :], total)).astype(jnp.bfloat16)


def last(own, core, side, tokens, gresid, norms):
    share, width = gresid.shape
    out = shaped((share, width), jnp.bfloat16)
    return pl.pallas_call(
        last_kernel,
        grid=(1,),
        in_specs=[
            row_of(share, width, 1),
            row_of(share, width, 0),
            whole_spec(side),
            pl.BlockSpec((share, width), block_of(OWN)),
            whole_spec(gresid),
            whole_spec(norms),
        ],
        out_specs=whole_spec(out),
        out_shape=out,
        compiler_params=limited(),
        name="last",
        cost_estimate=brief(),
    )(own, core, side, tokens, gresid, norms)


def tail_kernel(total, hidden, decoder, joint):
    low = total[...].astype(jnp.bfloat16)
    held = hidden[...].astype(jnp.bfloat16)
    part = jnp.zeros(joint.shape, jnp.float32)
    square = jnp.zeros((1, 1), jnp.float32)
    for i in range(2):
        part = part + dot(low[i], decoder[i], NT)
        grad = dot(held, low[i], TN)
        square = square + jnp.sum(jnp.sum(grad * grad, 0, keepdims=True), 1, keepdims=True)
        bias = jnp.sum(low[i].astype(jnp.float32), 0, keepdims=True)
        square = square + jnp.sum(bias * bias, 1, keepdims=True)
    row = lax.broadcasted_iota(jnp.int32, joint.shape, 0)
    joint[...] = jnp.where(row == PAD - 1, square, part)


def update_kernel(joint, hidden, hidden_own, total, selected, selected_own, onehot, encoder, *refs):
    table, enc, enc_bias, dec, dec_bias = (refs[i : i + 3] for i in range(0, 15, 3))
    norm_out, outs = refs[15], refs[16:]
    held = hidden[...]
    row = lax.broadcasted_iota(jnp.int32, held.shape, 0)
    grad = jnp.where(row < PRE, joint[...], 0.0) * (1.0 - held * held)
    grad = grad.astype(jnp.bfloat16)
    square = joint[PAD - 1 : PAD, 0:1]

    def summed(values):
        return jnp.sum(jnp.sum(values * values, 0, keepdims=True), 1, keepdims=True)

    square = square + summed(dot(selected[...], grad, TN))
    grad_bias = jnp.sum(grad.astype(jnp.float32), 0, keepdims=True)
    square = square + summed(grad_bias)
    grad_selected = dot(grad, encoder[...], NT)
    grad_table = dot(onehot[...], grad_selected, TN, lax.Precision.HIGHEST)[:PRE]
    square = square + summed(grad_table)
    norm = jnp.sqrt(square)
    norm_out[...] = norm
    factor = CLIP_LIMIT / (norm + 1e-06)

    def update(old, grad_of, at, index):
        weight, first, second = (ref[index] for ref in old)
        for out, new in zip(
            outs[at : at + 3], adam_update(weight, grad_of, first, second, factor), strict=True
        ):
            out[index] = new

    update(table, grad_table, 0, ...)
    update(enc, dot(selected_own[...], grad, TN), 3, ...)
    update(enc_bias, grad_bias, 6, ...)
    low = total[...].astype(jnp.bfloat16)
    held_own = hidden_own[...].astype(jnp.bfloat16)
    for i in range(2):
        update(dec, dot(held_own, low[i], TN), 9, (slice(None), i, slice(None)))
        bias = jnp.sum(low[i].astype(jnp.float32), 0, keepdims=True)
        update(dec_bias, bias, 12, (slice(i, i + 1), slice(None)))


def on_device(
    tokens,
    cotangent,
    norm_params,
    attention_weight,
    attention_bias,
    merge_weight,
    branch_bias,
    up_weight,
    up_bias,
    down_weight,
    prefix_ids,
    prefix_table,
    encoder_weight,
    encoder_bias,
    decoder_weight,
    decoder_bias,
    first_table,
    second_table,
    first_encoder,
    second_encoder,
    first_encoder_bias,
    second_encoder_bias,
    first_decoder,
    second_decoder,
    first_decoder_bias,
    second_decoder_bias,
):
    highest = lax.Precision.HIGHEST
    dp_index = lax.axis_index("dp")
    rows, width = tokens.shape
    share = rows // lax.axis_size("tensor")
    local = merge_weight.shape[1]
    units = up_weight.shape[1]
    in_rows = attention_weight.shape[0]
    hidden_size = encoder_weight.shape[1]
    dec_rows = decoder_weight.shape[0]
    halves = hidden_size // local

    decoder_low = decoder_weight.astype(jnp.bfloat16)
    attention = jnp.concatenate(
        [
            attention_weight.transpose(1, 0, 2).reshape(3 * in_rows, local),
            decoder_low.transpose(1, 0, 2).reshape(2 * dec_rows, local),
        ]
    )
    onehot = (
        jnp.pad(prefix_ids, (0, PAD - PRE), constant_values=PAD)[:, None]
        == jnp.arange(PAD, dtype=jnp.int32)[None, :]
    ).astype(jnp.float32)
    selected = jnp.dot(onehot[:, :PRE], prefix_table, precision=highest).astype(jnp.bfloat16)
    selected_own = lax.dynamic_slice_in_dim(selected, dp_index * in_rows, in_rows, 1)
    encoder_low = encoder_weight.astype(jnp.bfloat16)
    encoded_own = jnp.dot(selected_own, encoder_low, preferred_element_type=jnp.float32)
    sent = encoded_own.astype(jnp.bfloat16).reshape(PAD, halves, local).transpose(1, 0, 2)
    merging = jnp.concatenate([merge_weight, sent.reshape(halves * PAD, local)])

    small = lax.axis_size("dp") == 8
    if small:
        y, z, far = 1, 2, 4
        attention_far = swap(attention, "dp", far)
        merging_side = swap(merging, "dp", y)[None]
        up_side = swap(up_weight, "dp", y)[None]
        pair = jnp.stack([attention, after(attention_far, merging_side)])
        near = swap(pair, "dp", z)
        pair_side = swap(pair, "dp", y)
        merging_pair = joined(merging[None], merging_side)
        merging_far = swap(after(merging_pair, attention_far), "dp", far)
        near_side = swap(near, "dp", y)
        attention = ((pair, near, pair_side, near_side), ((0, 4), (2, 6), (1, 5), (3, 7)))
        merging_quad = joined(merging_pair, merging_far)
        merging_near = swap(merging_quad, "dp", z)
        merging = ((merging_quad, merging_near), ((0, 1, 4, 5), (2, 3, 6, 7)))
        down_far = swap(after(down_weight, near), "dp", far)[None]
    else:
        gathered = lambda shard: ((lax.all_gather(shard, "dp", axis=0),), None)
        attention, merging, down, up, encoder = map(
            gathered, (attention, merging, down_weight, up_weight, encoder_low)
        )

    projected, attend_full, decoder_full = project(
        tokens, norm_params, attention_bias, attention, hidden_size
    )
    if small:
        down_far = after(down_far, projected, up_side)
        down_pair = joined(down_weight[None], down_far)
        down_near = swap(down_pair, "dp", z)
        down_pair_side = swap(down_pair, "dp", y)
        up_far = swap(after(up_weight, down_far), "dp", far)[None]
    pieces, places = merging
    pieces = after(pieces, projected)
    if small:
        pieces = after(pieces, down_far, up_side)
    merge_own, encoded = gather_merge(pieces, places, width, hidden_size)
    mix_first, sums_first, hidden, prefix = attend_first(
        projected, encoded, encoder_bias[None], decoder_full, decoder_bias
    )

    def from_others(values, side):
        return values, side, swap(jnp.stack([values, side]), "tensor", CORE)

    merges = from_others(merge_own, after(swap(merge_own, "tensor", SIDE), mix_first))
    mixes_first = from_others(mix_first, swap(mix_first, "tensor", SIDE))
    mix_second, sums_second = attend_second(projected, prefix)
    mix_side = swap(mix_second, "tensor", SIDE)
    if small:
        down_near, down_pair_side, up_far = after((down_near, down_pair_side, up_far), mix_second)
        down_near_side = swap(down_near, "dp", y)
        down = (
            (down_pair, down_pair_side, down_near, down_near_side),
            ((0, 4), (1, 5), (2, 6), (3, 7)),
        )
        up_far = after(up_far, mixes_first[1])
        up_near = swap(joined(up_weight[None], up_far), "dp", z)
        up_far_side = swap(up_far, "dp", y)
    first_half = merge_half(tokens, norm_params, branch_bias, mixes_first, merges)
    mixes_second = from_others(mix_second, after(mix_side, first_half))
    cotangent_late = after(cotangent, first_half)
    if small:
        up_near = after(up_near, first_half)
        cotangent_late = after(cotangent_late, up_near)
        up_near_side = swap(up_near, "dp", y)
        up = (
            (up_weight[None], up_side, up_far, up_far_side, up_near, up_near_side),
            ((0,), (1,), (4,), (5,), (2, 6), (3, 7)),
        )
    down_full, grad_hidden = down_back(cotangent_late, down)
    if small:
        encoder_far = swap(after(encoder_low, grad_hidden), "dp", far)
    normed, resid = merge_half(
        tokens, norm_params, branch_bias, mixes_second, merges, after(first_half, grad_hidden)
    )

    def branch(act, *plus):
        part = lax.dot_general(
            act, down_full[0], (((1,), (1,)), ((), ())), preferred_element_type=jnp.float32
        )
        for one in plus:
            part = part + one.astype(jnp.float32)
        return part.astype(jnp.bfloat16)

    bias = up_bias[None]
    if small:
        normed = after(normed, encoder_far)
    act_both, up_both, up_full = feed_first(BOTH, normed, grad_hidden, up, bias)
    up_both = swap(up_both, "tensor", CORE)
    if small:
        encoder_pair = jnp.stack([encoder_low, encoder_far])
        encoder_near = swap(encoder_pair, "dp", z)
    act_side, up_send = feed((SIDE,), normed, grad_hidden, up_full, bias, up_both)
    up_from = swap(up_send, "tensor", SIDE)
    normed = after(normed, up_send)
    if small:
        normed = after(normed, encoder_near)
        encoder_quad = joined(encoder_pair, encoder_near)
        encoder_side = swap(encoder_quad, "dp", y)
        encoder = ((encoder_quad, encoder_side), ((0, 4, 2, 6), (1, 5, 3, 7)))
    act_rest, up_rest = feed((CORE, OWN), normed, grad_hidden, up_full, bias)
    up_core = swap(up_rest, "tensor", CORE)
    out_both = branch(after(act_both, act_rest))
    out_core = branch(act_rest[:share])
    up_from = after(up_from, out_both, out_core)
    out_own = branch(after(act_rest, up_from)[share:])
    up_core = after(up_core, out_own)
    grad_resid, keep, send = middle(up_rest, up_core, up_from, cotangent, resid, norm_params, merges)
    out_both = swap(out_both, "tensor", CORE)
    from_side = swap(send, "tensor", SIDE)
    core_keep = swap(keep, "tensor", CORE)
    out_core = swap(out_core, "tensor", CORE)
    out_send = branch(after(act_side, send), out_both)
    out_from = swap(out_send, "tensor", SIDE)
    encoder_full = assemble((after(encoder[0], send), encoder[1]), (1, width, hidden_size))
    hidden_own = lax.dynamic_slice_in_dim(after(hidden, send), dp_index * dec_rows, dec_rows, 1)
    from_side = after(from_side, out_send, encoder_full, hidden_own)
    core_side = swap(from_side, "tensor", CORE)
    grad_prefix, grad_mix, log_sums, inner, grad_query = prefix_back(
        projected,
        prefix,
        (mix_first, mix_second),
        (sums_first, sums_second),
        (keep, from_side, core_keep, core_side),
    )
    grad_first = attend_back(0, projected, grad_mix, log_sums, inner, grad_query)
    prefix_total = grad_prefix + swap(grad_prefix, "dp", 1)
    grad_second = attend_back(
        1, projected, after(grad_mix, prefix_total), log_sums, inner, grad_query
    )
    prefix_total = prefix_total + swap(prefix_total, "dp", 2)
    gprojs = after((grad_first, grad_second), prefix_total, out_from, out_core)
    bits = 4
    while bits < lax.axis_size("dp"):
        prefix_total = prefix_total + swap(prefix_total, "dp", bits)
        bits *= 2
    back_both = swap(project_back((BOTH,), gprojs, attend_full), "tensor", CORE)
    back_send = project_back((SIDE,), gprojs, attend_full, after(back_both, prefix_total))
    back_from = swap(back_send, "tensor", SIDE)
    joint = pl.pallas_call(
        tail_kernel,
        out_shape=shaped((PAD, hidden_size), jnp.float32),
        compiler_params=limited(),
        name="tail",
        cost_estimate=brief(),
    )(prefix_total, hidden, decoder_full)
    joint = joint + swap(joint, "tensor", CORE)
    back_rest = project_back((CORE, OWN), after(gprojs, back_send), attend_full)
    joint = joint + swap(joint, "tensor", SIDE)
    back_core = swap(back_rest, "tensor", CORE)
    output = (
        resid
        + (
            out_own.astype(jnp.float32)
            + out_core.astype(jnp.float32)
            + out_from.astype(jnp.float32)
        )
        + branch_bias[1]
    )
    input_grad = last(back_rest, back_core, back_from, tokens, grad_resid, norm_params)

    params = [
        (prefix_table, first_table, second_table),
        (encoder_weight, first_encoder, second_encoder),
        (encoder_bias[None], first_encoder_bias[None], second_encoder_bias[None]),
        (decoder_weight, first_decoder, second_decoder),
        (decoder_bias, first_decoder_bias, second_decoder_bias),
    ]
    params = [array for group in params for array in group]
    grad_norm, *new = pl.pallas_call(
        update_kernel,
        out_shape=[shaped((1, 1), jnp.float32)] + [shaped(p.shape, p.dtype) for p in params],
        compiler_params=limited(),
        name="update",
    )(
        joint,
        hidden,
        hidden_own,
        prefix_total,
        selected,
        selected_own,
        onehot,
        encoder_full[0],
        *params,
    )
    for i in range(6, 9):
        new[i] = new[i][0]
    return (output.astype(jnp.bfloat16), input_grad, grad_norm[0, 0], *new)


def solution(mesh):
    in_specs = (
        P("dp", None),
        P("dp", None),
        P(),
        P("dp", None, "tensor"),
        P(None, "tensor"),
        P("dp", "tensor"),
        P(),
        P("dp", "tensor"),
        P("tensor"),
        P("dp", "tensor"),
        P(),
        P(),
        P("dp", None),
        P(),
        P("dp", None, "tensor"),
        P(None, "tensor"),
        P(),
        P(),
        P("dp", None),
        P("dp", None),
        P(),
        P(),
        P("dp", None, "tensor"),
        P("dp", None, "tensor"),
        P(None, "tensor"),
        P(None, "tensor"),
    )
    out_specs = (
        P(("dp", "tensor"), None),
        P(("dp", "tensor"), None),
        P(),
        P(),
        P(),
        P(),
        P("dp", None),
        P("dp", None),
        P("dp", None),
        P(),
        P(),
        P(),
        P("dp", None, "tensor"),
        P("dp", None, "tensor"),
        P("dp", None, "tensor"),
        P(None, "tensor"),
        P(None, "tensor"),
        P(None, "tensor"),
    )
    return jax.shard_map(
        on_device, mesh=mesh, in_specs=in_specs, out_specs=out_specs, check_vma=False
    )
```

```python
import functools

import jax
import jax.numpy as jnp
from jax import lax
from jax.experimental import pallas as pl
from jax.experimental.pallas import tpu as pltpu
from jax.sharding import PartitionSpec as P

HD = 64
PRE = 10
PAD = 16
STEP = 10
TILE = 256


NORM_EPS = 1e-05
CLIP_LIMIT = 0.001
LEARN_RATE = 0.05
WEIGHT_DECAY = 0.01
BETA_FIRST = 0.9
BETA_SECOND = 0.999
ADAM_EPS = 1e-08
MASKED = -1e30
GELU_COEF = 0.7978845608028654

NN = ((1,), (0,))
NT = ((1,), (1,))
TN = ((0,), (0,))
OWN, CORE, SIDE, BOTH = 0, 1, 2, 3


def dot(left, right, dims, precision=None):
    return lax.dot_general(
        left, right, (dims, ((), ())), precision=precision, preferred_element_type=jnp.float32
    )


def shaped(shape, dtype):
    return jax.ShapeDtypeStruct(shape, dtype)


def limited():
    return pltpu.CompilerParams(vmem_limit_bytes=24 * 2**20)


def cost(flops, *arrays):
    size = sum(a.size * a.dtype.itemsize for a in arrays)
    return pl.CostEstimate(flops=flops, transcendentals=0, bytes_accessed=size)


def brief():
    return pl.CostEstimate(flops=0, transcendentals=0, bytes_accessed=0)


def norm_parts(rows):
    offsets = rows - jnp.mean(rows, axis=-1, keepdims=True)
    scale = lax.rsqrt(jnp.mean(offsets * offsets, axis=-1, keepdims=True) + NORM_EPS)
    return offsets * scale, scale


def norm_back(rows, gain, grad):
    unit, scale = norm_parts(rows)
    grad = grad * gain
    mean = jnp.mean(grad, axis=-1, keepdims=True)
    along = jnp.mean(grad * unit, axis=-1, keepdims=True)
    return scale * (grad - mean - unit * along)


def adam_update(weight, grad, first, second, factor):
    clipped = grad * factor
    new_first = BETA_FIRST * first + (1.0 - BETA_FIRST) * clipped
    new_second = BETA_SECOND * second + (1.0 - BETA_SECOND) * clipped * clipped
    fix_first = 1.0 - BETA_FIRST**STEP
    fix_second = 1.0 - BETA_SECOND**STEP
    new_weight = weight * (1.0 - LEARN_RATE * WEIGHT_DECAY) - LEARN_RATE * (
        new_first / fix_first
    ) / (jnp.sqrt(new_second / fix_second) + ADAM_EPS)
    return (new_weight, new_first, new_second)


def swap(values, axis, bits):
    size = lax.axis_size(axis)
    return lax.ppermute(values, axis, [(i, i ^ bits) for i in range(size)])


def after(values, *others):
    return lax.optimization_barrier((values, *others))[0]


def placed(found):
    refs, bits = found
    if bits is None:
        return [(refs[0].at[i], i) for i in range(refs[0].shape[0])]
    here = lax.axis_index("dp")
    return [
        (ref.at[i], lax.bitwise_xor(here, differ))
        for ref, group in zip(refs, bits, strict=True)
        for i, differ in enumerate(group)
    ]


def joined(*pieces):
    return jnp.concatenate(pieces)


def sum_over(values, axis):
    bits = 1
    while bits < lax.axis_size(axis):
        values = values + swap(values, axis, bits)
        bits *= 2
    return values


def assemble_into(outs, found):
    for piece, place in placed(found):
        start = 0
        for out in outs:
            parts, rows = out.shape[0], out.shape[1] // lax.axis_size("dp")
            for part in range(parts):
                where = pl.ds(pl.multiple_of(place * rows, rows), rows)
                out[part, where, :] = piece[start : start + rows, :]
                start += rows


def assemble_kernel(bits, *refs):
    assemble_into(refs[-1:], (refs[:-1], bits))


def assemble(gathered, shape):
    pieces, bits = gathered
    out = shaped(shape, pieces[0].dtype)
    return pl.pallas_call(
        functools.partial(assemble_kernel, bits),
        out_shape=out,
        compiler_params=limited(),
        name="assemble",
        cost_estimate=brief(),
    )(*pieces)


def merge_weight_kernel(bits, *refs):
    pieces, (weight, encoded) = refs[:-2], refs[-2:]
    rows = weight.shape[0] // lax.axis_size("dp")
    sums = None
    for piece, place in placed((pieces, bits)):
        weight[pl.ds(pl.multiple_of(place * rows, rows), rows), :] = piece[:rows, :]
        sent = piece[rows:, :].astype(jnp.float32)
        sums = sent if sums is None else sums + sent
    width = weight.shape[1]
    for i in range(encoded.shape[1] // width):
        encoded[:, i * width : (i + 1) * width] = sums[i * PAD : (i + 1) * PAD]


def gather_merge(pieces, bits, rows, hidden):
    outs = (shaped((rows, pieces[0].shape[-1]), jnp.bfloat16), shaped((PAD, hidden), jnp.float32))
    return pl.pallas_call(
        functools.partial(merge_weight_kernel, bits),
        out_shape=outs,
        compiler_params=limited(),
        name="gather_merge",
        cost_estimate=brief(),
    )(*pieces)


def project_kernel(bits, tokens, norms, bias, *refs):
    pieces, (projected, attend, decoder) = refs[:-3], refs[-3:]
    assemble_into((attend, decoder), (pieces, bits))
    for start in range(0, tokens.shape[0], TILE):
        rows = slice(start, start + TILE)
        unit, _ = norm_parts(tokens[rows, :].astype(jnp.float32))
        normed = (unit * norms[0:1, :] + norms[1:2, :]).astype(jnp.bfloat16)
        for part in range(3):
            total = dot(normed, attend[part], NN) + bias[part : part + 1, :]
            projected[part, rows, :] = total.astype(jnp.bfloat16)


def project(tokens, norms, bias, gathered, hidden):
    pieces, bits = gathered
    rows, width = tokens.shape
    local = bias.shape[1]
    outs = (
        shaped((3, rows, local), jnp.bfloat16),
        shaped((3, width, local), jnp.bfloat16),
        shaped((2, hidden, local), jnp.bfloat16),
    )
    return pl.pallas_call(
        functools.partial(project_kernel, bits),
        out_shape=outs,
        compiler_params=limited(),
        name="project",
        cost_estimate=brief(),
    )(tokens, norms, bias, *pieces)


def down_kernel(bits, cotangent, *refs):
    pieces, (down, grad) = refs[:-2], refs[-2:]
    assemble_into((down,), (pieces, bits))
    for start in range(0, cotangent.shape[0], TILE):
        rows = slice(start, start + TILE)
        grad[rows, :] = dot(cotangent[rows, :], down[0], NN).astype(jnp.bfloat16)


def down_back(cotangent, gathered):
    pieces, bits = gathered
    rows, width = cotangent.shape
    units = pieces[0].shape[-1]
    outs = (shaped((1, width, units), jnp.bfloat16), shaped((rows, units), jnp.bfloat16))
    return pl.pallas_call(
        functools.partial(down_kernel, bits),
        out_shape=outs,
        compiler_params=limited(),
        name="down_back",
        cost_estimate=brief(),
    )(cotangent, *pieces)


def prefix_kernel(encoded, encoder_bias, decoder, decoder_bias, hidden, prefix):
    held = jnp.tanh(encoded[...] + encoder_bias[...])
    hidden[...] = held
    low = held.astype(jnp.bfloat16)
    for part in range(2):
        total = dot(low, decoder[part], NN) + decoder_bias[part : part + 1, :]
        prefix[part] = total.astype(jnp.bfloat16)


def attend_kernel(first, proj, prefix, mix, sums, mixed):
    rows, width = mix.shape
    lane = lax.broadcasted_iota(jnp.int32, (1, width), 1) // HD
    pre_col = lax.broadcasted_iota(jnp.int32, (TILE, PAD), 1)
    below = lax.broadcasted_iota(jnp.int32, (TILE, TILE), 0) >= lax.broadcasted_iota(
        jnp.int32, (TILE, TILE), 1
    )
    sum_col = lax.broadcasted_iota(jnp.int32, (TILE, 128), 1)
    sums[...] = jnp.zeros_like(sums)
    mixed[...] = jnp.zeros_like(mixed)

    def one_head(head, carry):
        mine = lane == head
        for start in range(first, first + rows, TILE):
            here = slice(start, start + TILE)
            there = slice(start - first, start - first + TILE)
            query = proj[0, here, :] * jnp.asarray(HD**-0.5, jnp.bfloat16)
            one = jnp.where(mine, query, jnp.zeros_like(query))
            scores = [
                jnp.where(pre_col < PRE, dot(one, prefix[0], NT), MASKED),
                jnp.where(below, dot(one, proj[1, here, :], NT), MASKED),
            ]
            values = [prefix[1], proj[2, here, :]]
            if start:
                scores.append(dot(one, proj[1, :start, :], NT))
                values.append(proj[2, :start, :])
            top = functools.reduce(jnp.maximum, [jnp.max(s, 1, keepdims=True) for s in scores])
            exps = [jnp.exp(s - top) for s in scores]
            total = sum(jnp.sum(e, 1, keepdims=True) for e in exps)
            inverse = 1.0 / total
            part = sum(
                dot((e * inverse).astype(jnp.bfloat16), v, NN)
                for e, v in zip(exps, values, strict=True)
            )
            mixed[there, :] = jnp.where(mine, part, mixed[there, :])
            sums[there, :] = jnp.where(sum_col == head, top + jnp.log(total), sums[there, :])
        return carry

    lax.fori_loop(0, width // HD, one_head, 0)
    mix[...] = mixed[...].astype(jnp.bfloat16)


def attend_first_kernel(proj, encoded, encoder_bias, decoder, decoder_bias, mix, sums, hidden, prefix, mixed):
    prefix_kernel(encoded, encoder_bias, decoder, decoder_bias, hidden, prefix)
    attend_kernel(0, proj, prefix, mix, sums, mixed)


def attend_shapes(proj):
    _, rows, width = proj.shape
    return shaped((rows // 2, width), jnp.bfloat16), shaped((rows // 2, 128), jnp.float32)


def attend_first(proj, encoded, encoder_bias, decoder, decoder_bias):
    _, rows, width = proj.shape
    outs = (
        *attend_shapes(proj),
        shaped(encoded.shape, jnp.float32),
        shaped((2, PAD, width), jnp.bfloat16),
    )
    return pl.pallas_call(
        attend_first_kernel,
        out_shape=outs,
        scratch_shapes=[pltpu.VMEM((rows // 2, width), jnp.float32)],
        compiler_params=limited(),
        name="attend_first",
        cost_estimate=brief(),
    )(proj, encoded, encoder_bias, decoder, decoder_bias)


def attend_second(proj, prefix):
    _, rows, width = proj.shape
    outs = attend_shapes(proj)
    return pl.pallas_call(
        functools.partial(attend_kernel, rows // 2),
        out_shape=outs,
        scratch_shapes=[pltpu.VMEM((rows // 2, width), jnp.float32)],
        compiler_params=limited(),
        name="attend_second",
        cost_estimate=brief(),
    )(proj, prefix)


def prefix_back_kernel(
    query, prefix, mix_first, mix_second, sums_first, sums_second, keep, side, core_keep, core_side, *refs
):
    gprefix, gmix, log_sums, inner, gquery = refs
    rows, width = gmix.shape
    half = rows // 2
    quarter = keep.shape[1]
    heads = width // HD
    me = lax.axis_index("tensor")
    for piece, bits in ((keep.at[0], OWN), (core_keep.at[1], CORE), (side.at[0], SIDE), (core_side.at[1], BOTH)):
        place = lax.bitwise_xor(me, bits) * quarter
        gmix[pl.ds(pl.multiple_of(place, quarter), quarter), :] = piece[...]
    head_of = lax.broadcasted_iota(jnp.int32, (8, width), 0) == lax.broadcasted_iota(
        jnp.int32, (8, width), 1
    ) // HD
    for i, (mix, sums) in enumerate(((mix_first, sums_first), (mix_second, sums_second))):
        part = slice(i * half, (i + 1) * half)
        log_sums[:, part] = sums[...].T[:8]
        product = gmix[part, :].astype(jnp.float32) * mix[...].astype(jnp.float32)
        inner[:, part] = dot(head_of.astype(jnp.float32), product, NT, lax.Precision.HIGHEST)
    lane = lax.broadcasted_iota(jnp.int32, (PAD, width), 1) // HD
    zero = jnp.zeros((PAD, width), jnp.bfloat16)
    keys, values = (
        jnp.concatenate([jnp.where(lane == head, prefix[i], zero) for head in range(heads)])
        for i in range(2)
    )
    scale = jnp.asarray(HD**-0.5, jnp.bfloat16)

    def spread(of_heads):
        return jnp.concatenate(
            [jnp.broadcast_to(of_heads[head : head + 1, :], (PAD, rows)) for head in range(heads)]
        )

    scaled = query[0] * scale
    grad = gmix[...]
    position = lax.broadcasted_iota(jnp.int32, (heads * PAD, rows), 0) % PAD
    scores = jnp.where(position < PRE, dot(keys, scaled, NT), MASKED)
    prob = jnp.exp(scores - spread(log_sums))
    dscore = (prob * (dot(values, grad, NT) - spread(inner))).astype(jnp.bfloat16)
    dkeys = dot(dscore, scaled, NN)
    dvalues = dot(prob.astype(jnp.bfloat16), grad, NN)
    for i, found in enumerate((dkeys, dvalues)):
        gprefix[i] = sum(
            jnp.where(lane == head, found[head * PAD : (head + 1) * PAD], 0.0)
            for head in range(heads)
        )
    gquery[...] = dot(keys * scale, dscore, TN)


def prefix_back(proj, prefix, mixes, sums, pieces):
    _, rows, width = proj.shape
    outs = (
        shaped(prefix.shape, jnp.float32),
        shaped((rows, width), jnp.bfloat16),
        shaped((8, rows), jnp.float32),
        shaped((8, rows), jnp.float32),
        shaped((width, rows), jnp.float32),
    )
    return pl.pallas_call(
        prefix_back_kernel,
        grid=(1,),
        in_specs=[pl.BlockSpec((1, rows, width), lambda i: (0, 0, 0))]
        + [whole_spec(a) for a in (prefix, *mixes, *sums, *pieces)],
        out_specs=[whole_spec(o) for o in outs],
        out_shape=outs,
        compiler_params=limited(),
        name="prefix_back",
        cost_estimate=brief(),
    )(proj, prefix, *mixes, *sums, *pieces)


def attend_back_kernel(pair, proj, gmix, log_sums, inner, gquery_prefix, gproj, gquery, gkey, gvalue, keys_col):
    rows, width = gmix.shape
    lane = lax.broadcasted_iota(jnp.int32, (1, width), 1) // HD
    seen = lax.broadcasted_iota(jnp.int32, (TILE, TILE), 0) <= lax.broadcasted_iota(
        jnp.int32, (TILE, TILE), 1
    )
    scale = jnp.asarray(HD**-0.5, jnp.bfloat16)
    keys_col[...] = (proj[1] * scale).T
    gkey[...] = jnp.zeros_like(gkey)
    gvalue[...] = jnp.zeros_like(gvalue)

    def one_head(head, carry):
        mine = lane == head
        cols = pl.ds(pl.multiple_of(head * HD, HD), HD)
        row = pl.ds(pair * (width // HD) + head, 1)
        for start in range(0, rows, TILE):
            here = slice(start, start + TILE)
            query = proj[0, here, :] * scale
            grad = gmix[here, :]
            one = jnp.where(mine, query, jnp.zeros_like(query))
            one_grad = jnp.where(mine, grad, jnp.zeros_like(grad))
            log_sum = log_sums[row, here]
            shared = inner[row, here]
            dquery = gquery_prefix[cols, here]
            for at in range(0, start + TILE, TILE):
                there = slice(at, at + TILE)
                scores = dot(proj[1, there, :], one, NT)
                if at == start:
                    scores = jnp.where(seen, scores, MASKED)
                prob = jnp.exp(scores - log_sum)
                dscore = prob * (dot(proj[2, there, :], one_grad, NT) - shared)
                dscore = dscore.astype(jnp.bfloat16)
                gkey[there, :] += dot(dscore, one, NN)
                gvalue[there, :] += dot(prob.astype(jnp.bfloat16), one_grad, NN)
                dquery = dquery + dot(keys_col[cols, there], dscore, NN)
            gquery[cols, here] = dquery
        return carry

    lax.fori_loop(0, width // HD, one_head, 0)
    gproj[0] = gquery[...].T.astype(jnp.bfloat16)
    gproj[1] = gkey[...].astype(jnp.bfloat16)
    gproj[2] = gvalue[...].astype(jnp.bfloat16)


def attend_back(pair, proj, gmix, log_sums, inner, gquery):
    _, rows, local = proj.shape
    width = 2 * HD
    out = shaped((3, rows, width), jnp.bfloat16)
    return pl.pallas_call(
        functools.partial(attend_back_kernel, pair),
        grid=(1,),
        in_specs=[
            pl.BlockSpec((3, rows, width), lambda i: (0, 0, pair)),
            pl.BlockSpec((rows, width), lambda i: (0, pair)),
            whole_spec(log_sums),
            whole_spec(inner),
            pl.BlockSpec((width, rows), lambda i: (pair, 0)),
        ],
        out_specs=whole_spec(out),
        out_shape=out,
        scratch_shapes=[
            pltpu.VMEM((width, rows), jnp.float32),
            pltpu.VMEM((rows, width), jnp.float32),
            pltpu.VMEM((rows, width), jnp.float32),
            pltpu.VMEM((width, rows), jnp.bfloat16),
        ],
        compiler_params=limited(),
        name="attend_back",
        cost_estimate=cost(12 * rows * rows * width, proj, gmix, gquery, out),
    )(proj, gmix, log_sums, inner, gquery)


def four(refs):
    own, side, other = refs
    return own, other.at[0], side, other.at[1]


def merge_kernel(first, tokens, norms, branch, *refs):
    mixes, merges, earlier, (normed, resid_own) = refs[:3], refs[3:6], refs[6:-2], refs[-2:]
    i = pl.program_id(0)
    merged = sum(dot(m[...], w[...], NT) for m, w in zip(four(mixes), four(merges), strict=True))
    resid = tokens[...].astype(jnp.float32) + merged + branch[0:1, :]
    unit, _ = norm_parts(resid)
    normed[...] = (unit * norms[2:3, :] + norms[3:4, :]).astype(jnp.bfloat16)
    if earlier:

        @pl.when(i == 0)
        def _():
            resid_own[...] = earlier[1][...]

    @pl.when(i + first == lax.axis_index("tensor"))
    def _():
        resid_own[...] = resid


def merge_half(tokens, norms, branch, mixes, merges, earlier=()):
    rows, width = tokens.shape
    share = rows // lax.axis_size("tensor")
    local = mixes[0].shape[1]
    steps = mixes[0].shape[0] // share
    first = steps if earlier else 0
    whole = lambda a: pl.BlockSpec(a.shape, lambda i: (0,) * a.ndim)
    outs = (shaped((rows, width), jnp.bfloat16), shaped((share, width), jnp.float32))
    return pl.pallas_call(
        functools.partial(merge_kernel, first),
        grid=(steps,),
        in_specs=[pl.BlockSpec((share, width), lambda i: (i + first, 0)), whole(norms), whole(branch)]
        + [pl.BlockSpec((share, local), lambda i: (i, 0))] * 2
        + [pl.BlockSpec((2, share, local), lambda i: (0, i, 0))]
        + [whole(w) for w in merges]
        + ([pl.BlockSpec(memory_space=pl.ANY), whole(earlier[1])] if earlier else []),
        out_specs=(
            pl.BlockSpec((share, width), lambda i: (i + first, 0)),
            pl.BlockSpec((share, width), lambda i: (0, 0)),
        ),
        out_shape=outs,
        input_output_aliases={9: 0} if earlier else {},
        compiler_params=limited(),
        name="merge_second" if earlier else "merge_first",
        cost_estimate=brief(),
    )(tokens, norms, branch, *mixes, *merges, *earlier)


def feed_rows(normed, ghidden, up, bias, act, part, plus=None):
    value = dot(normed[...], up, NN) + bias[...]
    square = value * value
    tanh = jnp.tanh(GELU_COEF * value * (1.0 + 0.044715 * square))
    act[...] = (0.5 * value * (1.0 + tanh)).astype(jnp.bfloat16)
    slope = 0.5 * (1.0 + tanh) + 0.5 * GELU_COEF * value * (1.0 - tanh * tanh) * (
        1.0 + 3.0 * 0.044715 * square
    )
    gpre = (ghidden[...].astype(jnp.float32) * slope).astype(jnp.bfloat16)
    total = dot(gpre, up, NT)
    if plus is not None:
        total = total + plus[...].astype(jnp.float32)
    part[...] = total.astype(jnp.bfloat16)


def feed_first_kernel(bits, normed, ghidden, bias, *refs):
    pieces, (act, part, up) = refs[:-3], refs[-3:]
    assemble_into((up,), (pieces, bits))
    feed_rows(normed, ghidden, up[0], bias, act, part)


def feed_kernel(up, bias, normed, ghidden, *refs):
    feed_rows(normed, ghidden, up[0], bias, *refs[-2:], *refs[:-2])


def block_of(*bits):
    last = len(bits) - 1
    return lambda i: (lax.bitwise_xor(lax.axis_index("tensor"), bits[0] if not last else last - i), 0)


def whole_spec(a):
    return pl.BlockSpec(a.shape, lambda i: (0,) * a.ndim)


def feed_first(bits, normed, ghidden, gathered, bias):
    pieces, places = gathered
    rows, width = normed.shape
    share = rows // lax.axis_size("tensor")
    units = pieces[0].shape[-1]
    outs = (
        shaped((share, units), jnp.bfloat16),
        shaped((share, width), jnp.bfloat16),
        shaped((1, width, units), jnp.bfloat16),
    )
    return pl.pallas_call(
        functools.partial(feed_first_kernel, places),
        grid=(1,),
        in_specs=[
            pl.BlockSpec((share, width), block_of(bits)),
            pl.BlockSpec((share, units), block_of(bits)),
            whole_spec(bias),
        ]
        + [whole_spec(p) for p in pieces],
        out_specs=[whole_spec(o) for o in outs],
        out_shape=outs,
        compiler_params=limited(),
        name="feed_first",
        cost_estimate=brief(),
    )(normed, ghidden, bias, *pieces)


def feed(differ, normed, ghidden, up, bias, *plus):
    rows, width = normed.shape
    share = rows // lax.axis_size("tensor")
    units = up.shape[-1]
    outs = (shaped((share, units), jnp.bfloat16), shaped((share, width), jnp.bfloat16))
    return pl.pallas_call(
        feed_kernel,
        grid=(1,),
        in_specs=[
            whole_spec(up),
            whole_spec(bias),
            pl.BlockSpec((share, width), block_of(differ)),
            pl.BlockSpec((share, units), block_of(differ)),
        ]
        + [whole_spec(p) for p in plus],
        out_specs=[whole_spec(o) for o in outs],
        out_shape=outs,
        compiler_params=limited(),
        name="feed",
        cost_estimate=brief(),
    )(up, bias, normed, ghidden, *plus)


def back_kernel(weight, one, two, *refs):
    total = sum(
        dot(jnp.concatenate([one[i], two[i]], axis=1), weight[i], NT) for i in range(weight.shape[0])
    )
    for plus in refs[:-1]:
        total = total + plus[...].astype(jnp.float32)
    refs[-1][...] = total.astype(jnp.bfloat16)


def project_back(bits, gprojs, attend, *plus):
    _, rows, local = gprojs[0].shape
    width = attend.shape[1]
    share = rows // lax.axis_size("tensor")
    steps = len(bits)
    block = block_of(*bits)
    out = shaped((steps * share, width), jnp.bfloat16)
    return pl.pallas_call(
        back_kernel,
        grid=(steps,),
        in_specs=[whole_spec(attend)]
        + [pl.BlockSpec((3, share, local), lambda i: (0, *block(i)))] * 2
        + [whole_spec(p) for p in plus],
        out_specs=pl.BlockSpec((share, width), lambda i: (i, 0)),
        out_shape=out,
        compiler_params=limited(),
        name="project_back",
        cost_estimate=brief(),
    )(attend, *gprojs, *plus)


def three(own, core, side):
    return own[...].astype(jnp.float32) + core[...].astype(jnp.float32) + side[...].astype(jnp.float32)


def middle_kernel(own, core, side, cotangent, resid, norms, *refs):
    merges, (gresid, keep, send) = four(refs[:3]), refs[3:]
    total = three(own, core, side)
    grad = cotangent[...].astype(jnp.float32) + norm_back(resid[...], norms[2:3, :], total)
    gresid[...] = grad
    low = grad.astype(jnp.bfloat16)
    keep[0] = dot(low, merges[OWN][...], NN).astype(jnp.bfloat16)
    keep[1] = dot(low, merges[CORE][...], NN).astype(jnp.bfloat16)
    send[0] = dot(low, merges[SIDE][...], NN).astype(jnp.bfloat16)
    send[1] = dot(low, merges[BOTH][...], NN).astype(jnp.bfloat16)


def row_of(share, width, step):
    return pl.BlockSpec((share, width), lambda i: (step, 0))


def middle(own, core, side, cotangent, resid, norms, merges):
    share, width = resid.shape
    local = merges[0].shape[1]
    outs = (
        shaped((share, width), jnp.float32),
        shaped((2, share, local), jnp.bfloat16),
        shaped((2, share, local), jnp.bfloat16),
    )
    mine = pl.BlockSpec((share, width), block_of(OWN))
    return pl.pallas_call(
        middle_kernel,
        grid=(1,),
        in_specs=[whole_spec(own), whole_spec(core), whole_spec(side), mine]
        + [whole_spec(a) for a in (resid, norms, *merges)],
        out_specs=[whole_spec(o) for o in outs],
        out_shape=outs,
        compiler_params=limited(),
        name="middle",
        cost_estimate=brief(),
    )(own, core, side, cotangent, resid, norms, *merges)


def last_kernel(own, core, side, tokens, gresid, norms, out):
    total = three(own, core, side)
    rows = tokens[...].astype(jnp.float32)
    out[...] = (gresid[...] + norm_back(rows, norms[0:1, :], total)).astype(jnp.bfloat16)


def last(own, core, side, tokens, gresid, norms):
    share, width = gresid.shape
    out = shaped((share, width), jnp.bfloat16)
    return pl.pallas_call(
        last_kernel,
        grid=(1,),
        in_specs=[
            row_of(share, width, 1),
            row_of(share, width, 0),
            whole_spec(side),
            pl.BlockSpec((share, width), block_of(OWN)),
            whole_spec(gresid),
            whole_spec(norms),
        ],
        out_specs=whole_spec(out),
        out_shape=out,
        compiler_params=limited(),
        name="last",
        cost_estimate=brief(),
    )(own, core, side, tokens, gresid, norms)


def tail_kernel(total, hidden, decoder, joint):
    low = total[...].astype(jnp.bfloat16)
    held = hidden[...].astype(jnp.bfloat16)
    part = jnp.zeros(joint.shape, jnp.float32)
    square = jnp.zeros((1, 1), jnp.float32)
    for i in range(2):
        part = part + dot(low[i], decoder[i], NT)
        grad = dot(held, low[i], TN)
        square = square + jnp.sum(jnp.sum(grad * grad, 0, keepdims=True), 1, keepdims=True)
        bias = jnp.sum(low[i].astype(jnp.float32), 0, keepdims=True)
        square = square + jnp.sum(bias * bias, 1, keepdims=True)
    row = lax.broadcasted_iota(jnp.int32, joint.shape, 0)
    joint[...] = jnp.where(row == PAD - 1, square, part)


def update_kernel(joint, hidden, hidden_own, total, selected, selected_own, onehot, encoder, *refs):
    table, enc, enc_bias, dec, dec_bias = (refs[i : i + 3] for i in range(0, 15, 3))
    norm_out, outs = refs[15], refs[16:]
    held = hidden[...]
    row = lax.broadcasted_iota(jnp.int32, held.shape, 0)
    grad = jnp.where(row < PRE, joint[...], 0.0) * (1.0 - held * held)
    grad = grad.astype(jnp.bfloat16)
    square = joint[PAD - 1 : PAD, 0:1]

    def summed(values):
        return jnp.sum(jnp.sum(values * values, 0, keepdims=True), 1, keepdims=True)

    square = square + summed(dot(selected[...], grad, TN))
    grad_bias = jnp.sum(grad.astype(jnp.float32), 0, keepdims=True)
    square = square + summed(grad_bias)
    grad_selected = dot(grad, encoder[...], NT)
    grad_table = dot(onehot[...], grad_selected, TN, lax.Precision.HIGHEST)[:PRE]
    square = square + summed(grad_table)
    norm = jnp.sqrt(square)
    norm_out[...] = norm
    factor = CLIP_LIMIT / (norm + 1e-06)

    def update(old, grad_of, at, index):
        weight, first, second = (ref[index] for ref in old)
        for out, new in zip(
            outs[at : at + 3], adam_update(weight, grad_of, first, second, factor), strict=True
        ):
            out[index] = new

    update(table, grad_table, 0, ...)
    update(enc, dot(selected_own[...], grad, TN), 3, ...)
    update(enc_bias, grad_bias, 6, ...)
    low = total[...].astype(jnp.bfloat16)
    held_own = hidden_own[...].astype(jnp.bfloat16)
    for i in range(2):
        update(dec, dot(held_own, low[i], TN), 9, (slice(None), i, slice(None)))
        bias = jnp.sum(low[i].astype(jnp.float32), 0, keepdims=True)
        update(dec_bias, bias, 12, (slice(i, i + 1), slice(None)))


def on_device(
    tokens,
    cotangent,
    norm_params,
    attention_weight,
    attention_bias,
    merge_weight,
    branch_bias,
    up_weight,
    up_bias,
    down_weight,
    prefix_ids,
    prefix_table,
    encoder_weight,
    encoder_bias,
    decoder_weight,
    decoder_bias,
    first_table,
    second_table,
    first_encoder,
    second_encoder,
    first_encoder_bias,
    second_encoder_bias,
    first_decoder,
    second_decoder,
    first_decoder_bias,
    second_decoder_bias,
):
    highest = lax.Precision.HIGHEST
    dp_index = lax.axis_index("dp")
    rows, width = tokens.shape
    share = rows // lax.axis_size("tensor")
    local = merge_weight.shape[1]
    units = up_weight.shape[1]
    in_rows = attention_weight.shape[0]
    hidden_size = encoder_weight.shape[1]
    dec_rows = decoder_weight.shape[0]
    halves = hidden_size // local

    decoder_low = decoder_weight.astype(jnp.bfloat16)
    attention = jnp.concatenate(
        [
            attention_weight.transpose(1, 0, 2).reshape(3 * in_rows, local),
            decoder_low.transpose(1, 0, 2).reshape(2 * dec_rows, local),
        ]
    )
    onehot = (
        jnp.pad(prefix_ids, (0, PAD - PRE), constant_values=PAD)[:, None]
        == jnp.arange(PAD, dtype=jnp.int32)[None, :]
    ).astype(jnp.float32)
    selected = jnp.dot(onehot[:, :PRE], prefix_table, precision=highest).astype(jnp.bfloat16)
    selected_own = lax.dynamic_slice_in_dim(selected, dp_index * in_rows, in_rows, 1)
    encoder_low = encoder_weight.astype(jnp.bfloat16)
    encoded_own = jnp.dot(selected_own, encoder_low, preferred_element_type=jnp.float32)
    sent = encoded_own.astype(jnp.bfloat16).reshape(PAD, halves, local).transpose(1, 0, 2)
    merging = jnp.concatenate([merge_weight, sent.reshape(halves * PAD, local)])

    own_start = dp_index.astype(jnp.uint32) * dec_rows
    small = lax.axis_size("dp") == 8
    if small:
        y, z, far = 1, 2, 4
        attention_far = swap(attention, "dp", far)
        merging_side = swap(merging, "dp", y)[None]
        up_side = swap(up_weight, "dp", y)[None]
        attention_far, own_start = after((attention_far, own_start), merging_side, up_side)
        pair = jnp.stack([attention, attention_far])
        near = swap(pair, "dp", z)
        pair_side = swap(pair, "dp", y)
        merging_pair = joined(merging[None], merging_side)
        merging_far = swap(after(merging_pair, attention_far), "dp", far)
        near_side = swap(near, "dp", y)
        attention = ((pair, near, pair_side, near_side), ((0, 4), (2, 6), (1, 5), (3, 7)))
        merging_quad = joined(merging_pair, merging_far)
        merging_near = swap(merging_quad, "dp", z)
        merging = ((merging_quad, merging_near), ((0, 1, 4, 5), (2, 3, 6, 7)))
        down_far = swap(after(down_weight, near), "dp", far)[None]
    else:
        gathered = lambda shard: ((lax.all_gather(shard, "dp", axis=0),), None)
        attention, merging, down, up, encoder = map(
            gathered, (attention, merging, down_weight, up_weight, encoder_low)
        )

    projected, attend_full, decoder_full = project(
        tokens, norm_params, attention_bias, attention, hidden_size
    )
    if small:
        down_far = after(down_far, projected)
        down_pair = joined(down_weight[None], down_far)
        down_near = swap(down_pair, "dp", z)
        down_pair_side = swap(down_pair, "dp", y)
        up_far = swap(after(up_weight, down_far), "dp", far)[None]
    pieces, places = merging
    pieces = after(pieces, projected)
    if small:
        pieces = after(pieces, down_far)
    merge_own, encoded = gather_merge(pieces, places, width, hidden_size)
    mix_first, sums_first, hidden, prefix = attend_first(
        projected, encoded, encoder_bias[None], decoder_full, decoder_bias
    )

    def from_others(values, side):
        return values, side, swap(jnp.stack([values, side]), "tensor", CORE)

    merge_side = after(swap(merge_own, "tensor", SIDE), mix_first)
    if small:
        merge_side, up_far = after((merge_side, up_far))
    merges = from_others(merge_own, merge_side)
    mixes_first = from_others(mix_first, swap(mix_first, "tensor", SIDE))
    proj_late = after(projected, mixes_first[1])
    if small:
        proj_late, down_near, down_pair_side, up_far = after(
            (proj_late, down_near, down_pair_side, up_far)
        )
        down_near_side = swap(down_near, "dp", y)
        up_near = swap(joined(up_weight[None], up_far), "dp", z)
        up_far_side = swap(up_far, "dp", y)
    mix_second, sums_second = attend_second(proj_late, prefix)
    mix_side = swap(mix_second, "tensor", SIDE)
    branch_late = branch_bias
    if small:
        branch_late, down_near_side, up_near = after((branch_bias, down_near_side, up_near), mix_second)
        down = (
            (down_pair, down_pair_side, down_near, down_near_side),
            ((0, 4), (1, 5), (2, 6), (3, 7)),
        )
        up_near_side = swap(up_near, "dp", y)
    first_half = merge_half(tokens, norm_params, branch_late, mixes_first, merges)
    mixes_second = from_others(mix_second, after(mix_side, first_half))
    down_full, grad_hidden = down_back(after(cotangent, first_half), down)
    branch_late = after(branch_bias, grad_hidden)
    if small:
        encoder_far = swap(after(encoder_low, first_half), "dp", far)
        branch_late, up_far_side = after((branch_late, up_far_side))
        up = (
            (up_weight[None], up_side, up_far, up_far_side, up_near, up_near_side),
            ((0,), (1,), (4,), (5,), (2, 6), (3, 7)),
        )
    normed, resid = merge_half(
        tokens, norm_params, branch_late, mixes_second, merges, after(first_half, grad_hidden)
    )
    if small:
        normed = after(normed, encoder_far)

    def branch(act, *plus):
        part = lax.dot_general(
            act, down_full[0], (((1,), (1,)), ((), ())), preferred_element_type=jnp.float32
        )
        for one in plus:
            part = part + one.astype(jnp.float32)
        return part.astype(jnp.bfloat16)

    bias = up_bias[None]
    if small:
        normed = after(normed, encoder_far)
    act_both, up_both, up_full = feed_first(BOTH, normed, grad_hidden, up, bias)
    up_both = swap(up_both, "tensor", CORE)
    if small:
        encoder_pair = jnp.stack([encoder_low, after(encoder_far, act_both)])
        encoder_near = swap(encoder_pair, "dp", z)
    act_side, up_send = feed(SIDE, normed, grad_hidden, up_full, bias, up_both)
    up_from = swap(up_send, "tensor", SIDE)
    act_core, up_core = feed(CORE, after(normed, up_send), grad_hidden, up_full, bias)
    up_core = swap(up_core, "tensor", CORE)
    act_own, up_own = feed(OWN, after(normed, act_core), grad_hidden, up_full, bias)
    out_both = branch(after(act_both, act_own))
    up_from = after(up_from, out_both)
    if small:
        encoder_near = after(encoder_near, act_own)
        encoder_quad = joined(encoder_pair, encoder_near)
        encoder_side = swap(encoder_quad, "dp", y)
        encoder = ((encoder_quad, encoder_side), ((0, 4, 2, 6), (1, 5, 3, 7)))
        up_from = after(up_from, encoder_near)
    out_core = branch(after(act_core, up_from))
    out_own = branch(after(act_own, up_from))
    up_core = after(up_core, out_own, out_core)
    grad_resid, keep, send = middle(up_own, up_core, up_from, cotangent, resid, norm_params, merges)
    out_both = swap(out_both, "tensor", CORE)
    from_side = swap(send, "tensor", SIDE)
    core_keep = swap(keep, "tensor", CORE)
    out_core = swap(out_core, "tensor", CORE)
    out_send = branch(after(act_side, send), out_both)
    out_from = swap(out_send, "tensor", SIDE)
    encoder_full = assemble((after(encoder[0], send), encoder[1]), (1, width, hidden_size))
    hidden_own = lax.dynamic_slice(
        after(hidden, send), (jnp.uint32(0), own_start), (hidden.shape[0], dec_rows)
    )
    from_side = after(from_side, out_send, encoder_full, hidden_own)
    core_side = swap(from_side, "tensor", CORE)
    grad_prefix, grad_mix, log_sums, inner, grad_query = prefix_back(
        projected,
        prefix,
        (mix_first, mix_second),
        (sums_first, sums_second),
        (keep, from_side, core_keep, core_side),
    )
    grad_first = attend_back(0, projected, grad_mix, log_sums, inner, grad_query)
    prefix_total = grad_prefix + swap(grad_prefix, "dp", 1)
    grad_second = attend_back(
        1, projected, after(grad_mix, prefix_total), log_sums, inner, grad_query
    )
    prefix_total = prefix_total + swap(prefix_total, "dp", 2)
    gprojs = after((grad_first, grad_second), prefix_total, out_from, out_core)
    back_both = swap(project_back((BOTH,), gprojs, attend_full), "tensor", CORE)
    back_send = project_back((SIDE,), gprojs, attend_full, back_both)
    back_from = swap(back_send, "tensor", SIDE)
    bits = 4
    while bits < lax.axis_size("dp"):
        prefix_total = prefix_total + after(swap(prefix_total, "dp", bits), back_send)
        bits *= 2
    joint = pl.pallas_call(
        tail_kernel,
        out_shape=shaped((PAD, hidden_size), jnp.float32),
        compiler_params=limited(),
        name="tail",
        cost_estimate=brief(),
    )(prefix_total, hidden, decoder_full)
    joint = joint + swap(joint, "tensor", CORE)
    back_rest = project_back((CORE, OWN), after(gprojs, back_send, prefix_total), attend_full)
    joint_side = swap(joint, "tensor", SIDE)
    back_core = swap(back_rest, "tensor", CORE)
    output = (
        resid
        + (
            out_own.astype(jnp.float32)
            + out_core.astype(jnp.float32)
            + out_from.astype(jnp.float32)
        )
        + branch_bias[1]
    )
    input_grad = last(back_rest, back_core, back_from, tokens, grad_resid, norm_params)
    joint = joint + after(joint_side, input_grad)

    params = [
        (prefix_table, first_table, second_table),
        (encoder_weight, first_encoder, second_encoder),
        (encoder_bias[None], first_encoder_bias[None], second_encoder_bias[None]),
        (decoder_weight, first_decoder, second_decoder),
        (decoder_bias, first_decoder_bias, second_decoder_bias),
    ]
    params = [array for group in params for array in group]
    grad_norm, *new = pl.pallas_call(
        update_kernel,
        out_shape=[shaped((1, 1), jnp.float32)] + [shaped(p.shape, p.dtype) for p in params],
        compiler_params=limited(),
        name="update",
    )(
        joint,
        hidden,
        hidden_own,
        prefix_total,
        selected,
        selected_own,
        onehot,
        encoder_full[0],
        *params,
    )
    for i in range(6, 9):
        new[i] = new[i][0]
    return (output.astype(jnp.bfloat16), input_grad, grad_norm[0, 0], *new)


def solution(mesh):
    in_specs = (
        P("dp", None),
        P("dp", None),
        P(),
        P("dp", None, "tensor"),
        P(None, "tensor"),
        P("dp", "tensor"),
        P(),
        P("dp", "tensor"),
        P("tensor"),
        P("dp", "tensor"),
        P(),
        P(),
        P("dp", None),
        P(),
        P("dp", None, "tensor"),
        P(None, "tensor"),
        P(),
        P(),
        P("dp", None),
        P("dp", None),
        P(),
        P(),
        P("dp", None, "tensor"),
        P("dp", None, "tensor"),
        P(None, "tensor"),
        P(None, "tensor"),
    )
    out_specs = (
        P(("dp", "tensor"), None),
        P(("dp", "tensor"), None),
        P(),
        P(),
        P(),
        P(),
        P("dp", None),
        P("dp", None),
        P("dp", None),
        P(),
        P(),
        P(),
        P("dp", None, "tensor"),
        P("dp", None, "tensor"),
        P("dp", None, "tensor"),
        P(None, "tensor"),
        P(None, "tensor"),
        P(None, "tensor"),
    )
    return jax.shard_map(
        on_device, mesh=mesh, in_specs=in_specs, out_specs=out_specs, check_vma=False
    )
```

```python
import functools

import jax
import jax.numpy as jnp
from jax import lax
from jax.experimental import pallas as pl
from jax.experimental.pallas import tpu as pltpu
from jax.sharding import PartitionSpec as P

HD = 64
PRE = 10
PAD = 16
STEP = 10
TILE = 256


NORM_EPS = 1e-05
CLIP_LIMIT = 0.001
LEARN_RATE = 0.05
WEIGHT_DECAY = 0.01
BETA_FIRST = 0.9
BETA_SECOND = 0.999
ADAM_EPS = 1e-08
MASKED = -1e30
GELU_COEF = 0.7978845608028654

NN = ((1,), (0,))
NT = ((1,), (1,))
TN = ((0,), (0,))
OWN, CORE, SIDE, BOTH = 0, 1, 2, 3


def dot(left, right, dims, precision=None):
    return lax.dot_general(
        left, right, (dims, ((), ())), precision=precision, preferred_element_type=jnp.float32
    )


def shaped(shape, dtype):
    return jax.ShapeDtypeStruct(shape, dtype)


def limited():
    return pltpu.CompilerParams(vmem_limit_bytes=24 * 2**20)


def cost(flops, *arrays):
    size = sum(a.size * a.dtype.itemsize for a in arrays)
    return pl.CostEstimate(flops=flops, transcendentals=0, bytes_accessed=size)


def brief():
    return pl.CostEstimate(flops=0, transcendentals=0, bytes_accessed=0)


def norm_parts(rows):
    offsets = rows - jnp.mean(rows, axis=-1, keepdims=True)
    scale = lax.rsqrt(jnp.mean(offsets * offsets, axis=-1, keepdims=True) + NORM_EPS)
    return offsets * scale, scale


def norm_back(rows, gain, grad):
    unit, scale = norm_parts(rows)
    grad = grad * gain
    mean = jnp.mean(grad, axis=-1, keepdims=True)
    along = jnp.mean(grad * unit, axis=-1, keepdims=True)
    return scale * (grad - mean - unit * along)


def adam_update(weight, grad, first, second, factor):
    clipped = grad * factor
    new_first = BETA_FIRST * first + (1.0 - BETA_FIRST) * clipped
    new_second = BETA_SECOND * second + (1.0 - BETA_SECOND) * clipped * clipped
    fix_first = 1.0 - BETA_FIRST**STEP
    fix_second = 1.0 - BETA_SECOND**STEP
    new_weight = weight * (1.0 - LEARN_RATE * WEIGHT_DECAY) - LEARN_RATE * (
        new_first / fix_first
    ) / (jnp.sqrt(new_second / fix_second) + ADAM_EPS)
    return (new_weight, new_first, new_second)


def swap(values, axis, bits):
    size = lax.axis_size(axis)
    return lax.ppermute(values, axis, [(i, i ^ bits) for i in range(size)])


def after(values, *others):
    return lax.optimization_barrier((values, *others))[0]


def placed(found):
    refs, bits = found
    if bits is None:
        return [(refs[0].at[i], i) for i in range(refs[0].shape[0])]
    here = lax.axis_index("dp")
    return [
        (ref.at[i], lax.bitwise_xor(here, differ))
        for ref, group in zip(refs, bits, strict=True)
        for i, differ in enumerate(group)
    ]


def joined(*pieces):
    return jnp.concatenate(pieces)


def sum_over(values, axis):
    bits = 1
    while bits < lax.axis_size(axis):
        values = values + swap(values, axis, bits)
        bits *= 2
    return values


def assemble_into(outs, found):
    for piece, place in placed(found):
        start = 0
        for out in outs:
            parts, rows = out.shape[0], out.shape[1] // lax.axis_size("dp")
            for part in range(parts):
                where = pl.ds(pl.multiple_of(place * rows, rows), rows)
                out[part, where, :] = piece[start : start + rows, :]
                start += rows


def assemble_kernel(bits, *refs):
    assemble_into(refs[-1:], (refs[:-1], bits))


def assemble(gathered, shape):
    pieces, bits = gathered
    out = shaped(shape, pieces[0].dtype)
    return pl.pallas_call(
        functools.partial(assemble_kernel, bits),
        out_shape=out,
        compiler_params=limited(),
        name="assemble",
        cost_estimate=brief(),
    )(*pieces)


def merge_weight_kernel(bits, *refs):
    pieces, (weight, encoded) = refs[:-2], refs[-2:]
    rows = weight.shape[0] // lax.axis_size("dp")
    sums = None
    for piece, place in placed((pieces, bits)):
        weight[pl.ds(pl.multiple_of(place * rows, rows), rows), :] = piece[:rows, :]
        sent = piece[rows:, :].astype(jnp.float32)
        sums = sent if sums is None else sums + sent
    width = weight.shape[1]
    for i in range(encoded.shape[1] // width):
        encoded[:, i * width : (i + 1) * width] = sums[i * PAD : (i + 1) * PAD]


def gather_merge(pieces, bits, rows, hidden):
    outs = (shaped((rows, pieces[0].shape[-1]), jnp.bfloat16), shaped((PAD, hidden), jnp.float32))
    return pl.pallas_call(
        functools.partial(merge_weight_kernel, bits),
        out_shape=outs,
        compiler_params=limited(),
        name="gather_merge",
        cost_estimate=brief(),
    )(*pieces)


def project_kernel(bits, tokens, norms, bias, *refs):
    pieces, (projected, attend, decoder) = refs[:-3], refs[-3:]
    assemble_into((attend, decoder), (pieces, bits))
    for start in range(0, tokens.shape[0], TILE):
        rows = slice(start, start + TILE)
        unit, _ = norm_parts(tokens[rows, :].astype(jnp.float32))
        normed = (unit * norms[0:1, :] + norms[1:2, :]).astype(jnp.bfloat16)
        for part in range(3):
            total = dot(normed, attend[part], NN) + bias[part : part + 1, :]
            projected[part, rows, :] = total.astype(jnp.bfloat16)


def project(tokens, norms, bias, gathered, hidden):
    pieces, bits = gathered
    rows, width = tokens.shape
    local = bias.shape[1]
    outs = (
        shaped((3, rows, local), jnp.bfloat16),
        shaped((3, width, local), jnp.bfloat16),
        shaped((2, hidden, local), jnp.bfloat16),
    )
    return pl.pallas_call(
        functools.partial(project_kernel, bits),
        out_shape=outs,
        compiler_params=limited(),
        name="project",
        cost_estimate=brief(),
    )(tokens, norms, bias, *pieces)


def down_kernel(bits, cotangent, *refs):
    pieces, (down, grad) = refs[:-2], refs[-2:]
    assemble_into((down,), (pieces, bits))
    for start in range(0, cotangent.shape[0], TILE):
        rows = slice(start, start + TILE)
        grad[rows, :] = dot(cotangent[rows, :], down[0], NN).astype(jnp.bfloat16)


def down_back(cotangent, gathered):
    pieces, bits = gathered
    rows, width = cotangent.shape
    units = pieces[0].shape[-1]
    outs = (shaped((1, width, units), jnp.bfloat16), shaped((rows, units), jnp.bfloat16))
    return pl.pallas_call(
        functools.partial(down_kernel, bits),
        out_shape=outs,
        compiler_params=limited(),
        name="down_back",
        cost_estimate=brief(),
    )(cotangent, *pieces)


def prefix_kernel(encoded, encoder_bias, decoder, decoder_bias, hidden, prefix):
    held = jnp.tanh(encoded[...] + encoder_bias[...])
    hidden[...] = held
    low = held.astype(jnp.bfloat16)
    for part in range(2):
        total = dot(low, decoder[part], NN) + decoder_bias[part : part + 1, :]
        prefix[part] = total.astype(jnp.bfloat16)


def attend_kernel(first, proj, prefix, mix, sums, mixed):
    rows, width = mix.shape
    lane = lax.broadcasted_iota(jnp.int32, (1, width), 1) // HD
    pre_col = lax.broadcasted_iota(jnp.int32, (TILE, PAD), 1)
    below = lax.broadcasted_iota(jnp.int32, (TILE, TILE), 0) >= lax.broadcasted_iota(
        jnp.int32, (TILE, TILE), 1
    )
    sum_col = lax.broadcasted_iota(jnp.int32, (TILE, 128), 1)
    sums[...] = jnp.zeros_like(sums)
    mixed[...] = jnp.zeros_like(mixed)

    def one_head(head, carry):
        mine = lane == head
        for start in range(first, first + rows, TILE):
            here = slice(start, start + TILE)
            there = slice(start - first, start - first + TILE)
            query = proj[0, here, :] * jnp.asarray(HD**-0.5, jnp.bfloat16)
            one = jnp.where(mine, query, jnp.zeros_like(query))
            scores = [
                jnp.where(pre_col < PRE, dot(one, prefix[0], NT), MASKED),
                jnp.where(below, dot(one, proj[1, here, :], NT), MASKED),
            ]
            values = [prefix[1], proj[2, here, :]]
            if start:
                scores.append(dot(one, proj[1, :start, :], NT))
                values.append(proj[2, :start, :])
            top = functools.reduce(jnp.maximum, [jnp.max(s, 1, keepdims=True) for s in scores])
            exps = [jnp.exp(s - top) for s in scores]
            total = sum(jnp.sum(e, 1, keepdims=True) for e in exps)
            inverse = 1.0 / total
            part = sum(
                dot((e * inverse).astype(jnp.bfloat16), v, NN)
                for e, v in zip(exps, values, strict=True)
            )
            mixed[there, :] = jnp.where(mine, part, mixed[there, :])
            sums[there, :] = jnp.where(sum_col == head, top + jnp.log(total), sums[there, :])
        return carry

    lax.fori_loop(0, width // HD, one_head, 0, unroll=2 if first else 1)
    mix[...] = mixed[...].astype(jnp.bfloat16)


def attend_first_kernel(proj, encoded, encoder_bias, decoder, decoder_bias, mix, sums, hidden, prefix, mixed):
    prefix_kernel(encoded, encoder_bias, decoder, decoder_bias, hidden, prefix)
    attend_kernel(0, proj, prefix, mix, sums, mixed)


def attend_shapes(proj):
    _, rows, width = proj.shape
    return shaped((rows // 2, width), jnp.bfloat16), shaped((rows // 2, 128), jnp.float32)


def attend_first(proj, encoded, encoder_bias, decoder, decoder_bias):
    _, rows, width = proj.shape
    outs = (
        *attend_shapes(proj),
        shaped(encoded.shape, jnp.float32),
        shaped((2, PAD, width), jnp.bfloat16),
    )
    return pl.pallas_call(
        attend_first_kernel,
        out_shape=outs,
        scratch_shapes=[pltpu.VMEM((rows // 2, width), jnp.float32)],
        compiler_params=limited(),
        name="attend_first",
        cost_estimate=brief(),
    )(proj, encoded, encoder_bias, decoder, decoder_bias)


def attend_second(proj, prefix):
    _, rows, width = proj.shape
    outs = attend_shapes(proj)
    return pl.pallas_call(
        functools.partial(attend_kernel, rows // 2),
        out_shape=outs,
        scratch_shapes=[pltpu.VMEM((rows // 2, width), jnp.float32)],
        compiler_params=limited(),
        name="attend_second",
        cost_estimate=brief(),
    )(proj, prefix)


def prefix_back_kernel(
    query, prefix, mix_first, mix_second, sums_first, sums_second, keep, side, core_keep, core_side, *refs
):
    gprefix, gmix, log_sums, inner, gquery = refs
    rows, width = gmix.shape
    half = rows // 2
    quarter = keep.shape[1]
    heads = width // HD
    me = lax.axis_index("tensor")
    for piece, bits in ((keep.at[0], OWN), (core_keep.at[1], CORE), (side.at[0], SIDE), (core_side.at[1], BOTH)):
        place = lax.bitwise_xor(me, bits) * quarter
        gmix[pl.ds(pl.multiple_of(place, quarter), quarter), :] = piece[...]
    head_of = lax.broadcasted_iota(jnp.int32, (8, width), 0) == lax.broadcasted_iota(
        jnp.int32, (8, width), 1
    ) // HD
    for i, (mix, sums) in enumerate(((mix_first, sums_first), (mix_second, sums_second))):
        part = slice(i * half, (i + 1) * half)
        log_sums[:, part] = sums[...].T[:8]
        product = gmix[part, :].astype(jnp.float32) * mix[...].astype(jnp.float32)
        inner[:, part] = dot(head_of.astype(jnp.float32), product, NT, lax.Precision.HIGHEST)
    lane = lax.broadcasted_iota(jnp.int32, (PAD, width), 1) // HD
    zero = jnp.zeros((PAD, width), jnp.bfloat16)
    keys, values = (
        jnp.concatenate([jnp.where(lane == head, prefix[i], zero) for head in range(heads)])
        for i in range(2)
    )
    scale = jnp.asarray(HD**-0.5, jnp.bfloat16)

    def spread(of_heads):
        return jnp.concatenate(
            [jnp.broadcast_to(of_heads[head : head + 1, :], (PAD, rows)) for head in range(heads)]
        )

    scaled = query[0] * scale
    grad = gmix[...]
    position = lax.broadcasted_iota(jnp.int32, (heads * PAD, rows), 0) % PAD
    scores = jnp.where(position < PRE, dot(keys, scaled, NT), MASKED)
    prob = jnp.exp(scores - spread(log_sums))
    dscore = (prob * (dot(values, grad, NT) - spread(inner))).astype(jnp.bfloat16)
    dkeys = dot(dscore, scaled, NN)
    dvalues = dot(prob.astype(jnp.bfloat16), grad, NN)
    for i, found in enumerate((dkeys, dvalues)):
        gprefix[i] = sum(
            jnp.where(lane == head, found[head * PAD : (head + 1) * PAD], 0.0)
            for head in range(heads)
        )
    gquery[...] = dot(keys * scale, dscore, TN)


def prefix_back(proj, prefix, mixes, sums, pieces):
    _, rows, width = proj.shape
    outs = (
        shaped(prefix.shape, jnp.float32),
        shaped((rows, width), jnp.bfloat16),
        shaped((8, rows), jnp.float32),
        shaped((8, rows), jnp.float32),
        shaped((width, rows), jnp.float32),
    )
    return pl.pallas_call(
        prefix_back_kernel,
        grid=(1,),
        in_specs=[pl.BlockSpec((1, rows, width), lambda i: (0, 0, 0))]
        + [whole_spec(a) for a in (prefix, *mixes, *sums, *pieces)],
        out_specs=[whole_spec(o) for o in outs],
        out_shape=outs,
        compiler_params=limited(),
        name="prefix_back",
        cost_estimate=brief(),
    )(proj, prefix, *mixes, *sums, *pieces)


def attend_back_kernel(pair, proj, gmix, log_sums, inner, gquery_prefix, gproj, gquery, gkey, gvalue, keys_col):
    rows, width = gmix.shape
    lane = lax.broadcasted_iota(jnp.int32, (1, width), 1) // HD
    seen = lax.broadcasted_iota(jnp.int32, (TILE, TILE), 0) <= lax.broadcasted_iota(
        jnp.int32, (TILE, TILE), 1
    )
    scale = jnp.asarray(HD**-0.5, jnp.bfloat16)
    keys_col[...] = (proj[1] * scale).T
    gkey[...] = jnp.zeros_like(gkey)
    gvalue[...] = jnp.zeros_like(gvalue)

    def one_head(head, carry):
        mine = lane == head
        cols = pl.ds(pl.multiple_of(head * HD, HD), HD)
        row = pl.ds(pair * (width // HD) + head, 1)
        for start in range(0, rows, TILE):
            here = slice(start, start + TILE)
            query = proj[0, here, :] * scale
            grad = gmix[here, :]
            one = jnp.where(mine, query, jnp.zeros_like(query))
            one_grad = jnp.where(mine, grad, jnp.zeros_like(grad))
            log_sum = log_sums[row, here]
            shared = inner[row, here]
            dquery = gquery_prefix[cols, here]
            for at in range(0, start + TILE, TILE):
                there = slice(at, at + TILE)
                scores = dot(proj[1, there, :], one, NT)
                if at == start:
                    scores = jnp.where(seen, scores, MASKED)
                prob = jnp.exp(scores - log_sum)
                dscore = prob * (dot(proj[2, there, :], one_grad, NT) - shared)
                dscore = dscore.astype(jnp.bfloat16)
                gkey[there, :] += dot(dscore, one, NN)
                gvalue[there, :] += dot(prob.astype(jnp.bfloat16), one_grad, NN)
                dquery = dquery + dot(keys_col[cols, there], dscore, NN)
            gquery[cols, here] = dquery
        return carry

    lax.fori_loop(0, width // HD, one_head, 0)
    gproj[0] = gquery[...].T.astype(jnp.bfloat16)
    gproj[1] = gkey[...].astype(jnp.bfloat16)
    gproj[2] = gvalue[...].astype(jnp.bfloat16)


def attend_back(pair, proj, gmix, log_sums, inner, gquery):
    _, rows, local = proj.shape
    width = 2 * HD
    out = shaped((3, rows, width), jnp.bfloat16)
    return pl.pallas_call(
        functools.partial(attend_back_kernel, pair),
        grid=(1,),
        in_specs=[
            pl.BlockSpec((3, rows, width), lambda i: (0, 0, pair)),
            pl.BlockSpec((rows, width), lambda i: (0, pair)),
            whole_spec(log_sums),
            whole_spec(inner),
            pl.BlockSpec((width, rows), lambda i: (pair, 0)),
        ],
        out_specs=whole_spec(out),
        out_shape=out,
        scratch_shapes=[
            pltpu.VMEM((width, rows), jnp.float32),
            pltpu.VMEM((rows, width), jnp.float32),
            pltpu.VMEM((rows, width), jnp.float32),
            pltpu.VMEM((width, rows), jnp.bfloat16),
        ],
        compiler_params=limited(),
        name="attend_back",
        cost_estimate=cost(12 * rows * rows * width, proj, gmix, gquery, out),
    )(proj, gmix, log_sums, inner, gquery)


def merge_kernel(first, tokens, norms, branch, *refs):
    mixes, merges, earlier, (normed, resid_own) = refs[:4], refs[4:8], refs[8:-2], refs[-2:]
    i = pl.program_id(0)
    merged = sum(dot(m[...], w[...], NT) for m, w in zip(mixes, merges, strict=True))
    resid = tokens[...].astype(jnp.float32) + merged + branch[0:1, :]
    unit, _ = norm_parts(resid)
    normed[...] = (unit * norms[2:3, :] + norms[3:4, :]).astype(jnp.bfloat16)
    if earlier:

        @pl.when(i == 0)
        def _():
            resid_own[...] = earlier[1][...]

    @pl.when(i + first == lax.axis_index("tensor"))
    def _():
        resid_own[...] = resid


def part_spec(shape, first):
    return pl.BlockSpec(shape, lambda i: (first // shape[0] + i, 0))


def fixed_spec(shape, first):
    return pl.BlockSpec(shape, lambda i: (first // shape[0], 0))


def merge_half(tokens, norms, branch, mixes, merges, earlier=()):
    rows, width = tokens.shape
    share = rows // lax.axis_size("tensor")
    local = mixes[0][0].shape[1]
    steps = rows // 2 // share
    first = steps if earlier else 0
    whole = lambda a: pl.BlockSpec(a.shape, lambda i: (0,) * a.ndim)
    outs = (shaped((rows, width), jnp.bfloat16), shaped((share, width), jnp.float32))
    return pl.pallas_call(
        functools.partial(merge_kernel, first),
        grid=(steps,),
        in_specs=[pl.BlockSpec((share, width), lambda i: (i + first, 0)), whole(norms), whole(branch)]
        + [part_spec((share, local), start) for _, start in mixes]
        + [fixed_spec((width, local), start) for _, start in merges]
        + ([pl.BlockSpec(memory_space=pl.ANY), whole(earlier[1])] if earlier else []),
        out_specs=(
            pl.BlockSpec((share, width), lambda i: (i + first, 0)),
            pl.BlockSpec((share, width), lambda i: (0, 0)),
        ),
        out_shape=outs,
        input_output_aliases={11: 0} if earlier else {},
        compiler_params=limited(),
        name="merge_second" if earlier else "merge_first",
        cost_estimate=brief(),
    )(tokens, norms, branch, *[a for a, _ in (*mixes, *merges)], *earlier)


def feed_rows(normed, ghidden, up, bias, act, part, plus=None):
    value = dot(normed[...], up, NN) + bias[...]
    square = value * value
    tanh = jnp.tanh(GELU_COEF * value * (1.0 + 0.044715 * square))
    act[...] = (0.5 * value * (1.0 + tanh)).astype(jnp.bfloat16)
    slope = 0.5 * (1.0 + tanh) + 0.5 * GELU_COEF * value * (1.0 - tanh * tanh) * (
        1.0 + 3.0 * 0.044715 * square
    )
    gpre = (ghidden[...].astype(jnp.float32) * slope).astype(jnp.bfloat16)
    total = dot(gpre, up, NT)
    if plus is not None:
        total = total + plus[...].astype(jnp.float32)
    part[...] = total.astype(jnp.bfloat16)


def feed_first_kernel(bits, normed, ghidden, bias, *refs):
    pieces, (act, part, up) = refs[:-3], refs[-3:]
    assemble_into((up,), (pieces, bits))
    feed_rows(normed, ghidden, up[0], bias, act, part)


def feed_kernel(up, bias, normed, ghidden, *refs):
    feed_rows(normed, ghidden, up[0], bias, *refs[-2:], *refs[:-2])


def block_of(*bits):
    last = len(bits) - 1
    return lambda i: (lax.bitwise_xor(lax.axis_index("tensor"), bits[0] if not last else last - i), 0)


def whole_spec(a):
    return pl.BlockSpec(a.shape, lambda i: (0,) * a.ndim)


def feed_first(bits, normed, ghidden, gathered, bias):
    pieces, places = gathered
    rows, width = normed.shape
    share = rows // lax.axis_size("tensor")
    units = pieces[0].shape[-1]
    outs = (
        shaped((share, units), jnp.bfloat16),
        shaped((share, width), jnp.bfloat16),
        shaped((1, width, units), jnp.bfloat16),
    )
    return pl.pallas_call(
        functools.partial(feed_first_kernel, places),
        grid=(1,),
        in_specs=[
            pl.BlockSpec((share, width), block_of(bits)),
            pl.BlockSpec((share, units), block_of(bits)),
            whole_spec(bias),
        ]
        + [whole_spec(p) for p in pieces],
        out_specs=[whole_spec(o) for o in outs],
        out_shape=outs,
        compiler_params=limited(),
        name="feed_first",
        cost_estimate=brief(),
    )(normed, ghidden, bias, *pieces)


def feed(differ, normed, ghidden, up, bias, *plus):
    rows, width = normed.shape
    share = rows // lax.axis_size("tensor")
    units = up.shape[-1]
    outs = (shaped((share, units), jnp.bfloat16), shaped((share, width), jnp.bfloat16))
    return pl.pallas_call(
        feed_kernel,
        grid=(1,),
        in_specs=[
            whole_spec(up),
            whole_spec(bias),
            pl.BlockSpec((share, width), block_of(differ)),
            pl.BlockSpec((share, units), block_of(differ)),
        ]
        + [whole_spec(p) for p in plus],
        out_specs=[whole_spec(o) for o in outs],
        out_shape=outs,
        compiler_params=limited(),
        name="feed",
        cost_estimate=brief(),
    )(up, bias, normed, ghidden, *plus)


def back_kernel(weight, one, two, *refs):
    total = sum(
        dot(jnp.concatenate([one[i], two[i]], axis=1), weight[i], NT) for i in range(weight.shape[0])
    )
    for plus in refs[:-1]:
        total = total + plus[...].astype(jnp.float32)
    refs[-1][...] = total.astype(jnp.bfloat16)


def project_back(bits, gprojs, attend, *plus):
    _, rows, local = gprojs[0].shape
    width = attend.shape[1]
    share = rows // lax.axis_size("tensor")
    steps = len(bits)
    block = block_of(*bits)
    out = shaped((steps * share, width), jnp.bfloat16)
    return pl.pallas_call(
        back_kernel,
        grid=(steps,),
        in_specs=[whole_spec(attend)]
        + [pl.BlockSpec((3, share, local), lambda i: (0, *block(i)))] * 2
        + [whole_spec(p) for p in plus],
        out_specs=pl.BlockSpec((share, width), lambda i: (i, 0)),
        out_shape=out,
        compiler_params=limited(),
        name="project_back",
        cost_estimate=brief(),
    )(attend, *gprojs, *plus)


def three(own, core, side):
    return own[...].astype(jnp.float32) + core[...].astype(jnp.float32) + side[...].astype(jnp.float32)


def middle_kernel(own, core, side, cotangent, resid, norms, *refs):
    merges, (gresid, keep, send) = refs[:4], refs[4:]
    total = three(own, core, side)
    grad = cotangent[...].astype(jnp.float32) + norm_back(resid[...], norms[2:3, :], total)
    gresid[...] = grad
    low = grad.astype(jnp.bfloat16)
    keep[0] = dot(low, merges[OWN][...], NN).astype(jnp.bfloat16)
    keep[1] = dot(low, merges[CORE][...], NN).astype(jnp.bfloat16)
    send[0] = dot(low, merges[SIDE][...], NN).astype(jnp.bfloat16)
    send[1] = dot(low, merges[BOTH][...], NN).astype(jnp.bfloat16)


def row_of(share, width, step):
    return pl.BlockSpec((share, width), lambda i: (step, 0))


def middle(own, core, side, cotangent, resid, norms, merges):
    share, width = resid.shape
    local = merges[0][0].shape[1]
    outs = (
        shaped((share, width), jnp.float32),
        shaped((2, share, local), jnp.bfloat16),
        shaped((2, share, local), jnp.bfloat16),
    )
    mine = pl.BlockSpec((share, width), block_of(OWN))
    return pl.pallas_call(
        middle_kernel,
        grid=(1,),
        in_specs=[whole_spec(own), whole_spec(core), whole_spec(side), mine]
        + [whole_spec(a) for a in (resid, norms)]
        + [fixed_spec((width, local), start) for _, start in merges],
        out_specs=[whole_spec(o) for o in outs],
        out_shape=outs,
        compiler_params=limited(),
        name="middle",
        cost_estimate=brief(),
    )(own, core, side, cotangent, resid, norms, *[a for a, _ in merges])


def last_kernel(own, core, side, tokens, gresid, norms, out):
    total = three(own, core, side)
    rows = tokens[...].astype(jnp.float32)
    out[...] = (gresid[...] + norm_back(rows, norms[0:1, :], total)).astype(jnp.bfloat16)


def last(own, core, side, tokens, gresid, norms):
    share, width = gresid.shape
    out = shaped((share, width), jnp.bfloat16)
    return pl.pallas_call(
        last_kernel,
        grid=(1,),
        in_specs=[
            row_of(share, width, 1),
            row_of(share, width, 0),
            whole_spec(side),
            pl.BlockSpec((share, width), block_of(OWN)),
            whole_spec(gresid),
            whole_spec(norms),
        ],
        out_specs=whole_spec(out),
        out_shape=out,
        compiler_params=limited(),
        name="last",
        cost_estimate=brief(),
    )(own, core, side, tokens, gresid, norms)


def plus_kernel(one, two, out):
    out[...] = one[...] + two[...]


def plus(one, two):
    return pl.pallas_call(
        plus_kernel,
        out_shape=shaped(one.shape, one.dtype),
        compiler_params=limited(),
        name="plus",
        cost_estimate=brief(),
    )(one, two)


def output_kernel(resid, own, core, side, branch, out):
    out[...] = (resid[...] + three(own, core, side) + branch[1:2, :]).astype(jnp.bfloat16)


def output_rows(resid, own, core, side, branch):
    return pl.pallas_call(
        output_kernel,
        out_shape=shaped(resid.shape, jnp.bfloat16),
        compiler_params=limited(),
        name="output",
        cost_estimate=brief(),
    )(resid, own, core, side, branch)


def tail_kernel(one, two, hidden, decoder, total, joint):
    total[...] = one[...] + two[...]
    low = total[...].astype(jnp.bfloat16)
    held = hidden[...].astype(jnp.bfloat16)
    part = jnp.zeros(joint.shape, jnp.float32)
    square = jnp.zeros((1, 1), jnp.float32)
    for i in range(2):
        part = part + dot(low[i], decoder[i], NT)
        grad = dot(held, low[i], TN)
        square = square + jnp.sum(jnp.sum(grad * grad, 0, keepdims=True), 1, keepdims=True)
        bias = jnp.sum(low[i].astype(jnp.float32), 0, keepdims=True)
        square = square + jnp.sum(bias * bias, 1, keepdims=True)
    row = lax.broadcasted_iota(jnp.int32, joint.shape, 0)
    joint[...] = jnp.where(row == PAD - 1, square, part)


def update_kernel(joint_one, joint_two, hidden, hidden_own, total, selected, selected_own, onehot, encoder, *refs):
    table, enc, enc_bias, dec, dec_bias = (refs[i : i + 3] for i in range(0, 15, 3))
    norm_out, outs = refs[15], refs[16:]
    held = hidden[...]
    row = lax.broadcasted_iota(jnp.int32, held.shape, 0)
    joint = joint_one[...] + joint_two[...]
    grad = jnp.where(row < PRE, joint, 0.0) * (1.0 - held * held)
    grad = grad.astype(jnp.bfloat16)
    square = joint[PAD - 1 : PAD, 0:1]

    def summed(values):
        return jnp.sum(jnp.sum(values * values, 0, keepdims=True), 1, keepdims=True)

    square = square + summed(dot(selected[...], grad, TN))
    grad_bias = jnp.sum(grad.astype(jnp.float32), 0, keepdims=True)
    square = square + summed(grad_bias)
    grad_selected = dot(grad, encoder[...], NT)
    grad_table = dot(onehot[...], grad_selected, TN, lax.Precision.HIGHEST)[:PRE]
    square = square + summed(grad_table)
    norm = jnp.sqrt(square)
    norm_out[...] = norm
    factor = CLIP_LIMIT / (norm + 1e-06)

    def update(old, grad_of, at, index):
        weight, first, second = (ref[index] for ref in old)
        for out, new in zip(
            outs[at : at + 3], adam_update(weight, grad_of, first, second, factor), strict=True
        ):
            out[index] = new

    update(table, grad_table, 0, ...)
    update(enc, dot(selected_own[...], grad, TN), 3, ...)
    update(enc_bias, grad_bias, 6, ...)
    low = total[...].astype(jnp.bfloat16)
    held_own = hidden_own[...].astype(jnp.bfloat16)
    for i in range(2):
        update(dec, dot(held_own, low[i], TN), 9, (slice(None), i, slice(None)))
        bias = jnp.sum(low[i].astype(jnp.float32), 0, keepdims=True)
        update(dec_bias, bias, 12, (slice(i, i + 1), slice(None)))


def on_device(
    tokens,
    cotangent,
    norm_params,
    attention_weight,
    attention_bias,
    merge_weight,
    branch_bias,
    up_weight,
    up_bias,
    down_weight,
    prefix_ids,
    prefix_table,
    encoder_weight,
    encoder_bias,
    decoder_weight,
    decoder_bias,
    first_table,
    second_table,
    first_encoder,
    second_encoder,
    first_encoder_bias,
    second_encoder_bias,
    first_decoder,
    second_decoder,
    first_decoder_bias,
    second_decoder_bias,
):
    highest = lax.Precision.HIGHEST
    dp_index = lax.axis_index("dp")
    rows, width = tokens.shape
    share = rows // lax.axis_size("tensor")
    local = merge_weight.shape[1]
    units = up_weight.shape[1]
    in_rows = attention_weight.shape[0]
    hidden_size = encoder_weight.shape[1]
    dec_rows = decoder_weight.shape[0]
    halves = hidden_size // local

    decoder_low = decoder_weight.astype(jnp.bfloat16)
    attention = jnp.concatenate(
        [
            attention_weight.transpose(1, 0, 2).reshape(3 * in_rows, local),
            decoder_low.transpose(1, 0, 2).reshape(2 * dec_rows, local),
        ]
    )
    onehot = (
        jnp.pad(prefix_ids, (0, PAD - PRE), constant_values=PAD)[:, None]
        == jnp.arange(PAD, dtype=jnp.int32)[None, :]
    ).astype(jnp.float32)
    selected = jnp.dot(onehot[:, :PRE], prefix_table, precision=highest).astype(jnp.bfloat16)
    selected_own = lax.dynamic_slice_in_dim(selected, dp_index * in_rows, in_rows, 1)
    encoder_low = encoder_weight.astype(jnp.bfloat16)
    encoded_own = jnp.dot(selected_own, encoder_low, preferred_element_type=jnp.float32)
    sent = encoded_own.astype(jnp.bfloat16).reshape(PAD, halves, local).transpose(1, 0, 2)
    merging = jnp.concatenate([merge_weight, sent.reshape(halves * PAD, local)])

    own_start = dp_index.astype(jnp.uint32) * dec_rows
    small = lax.axis_size("dp") == 8
    if small:
        y, z, far = 1, 2, 4
        attention_far = swap(attention, "dp", far)
        merging_side = swap(merging, "dp", y)[None]
        up_side = swap(up_weight, "dp", y)[None]
        attention_far, own_start = after((attention_far, own_start), merging_side, up_side)
        pair = jnp.stack([attention, attention_far])
        near = swap(pair, "dp", z)
        pair_side = swap(pair, "dp", y)
        merging_pair = joined(merging[None], merging_side)
        merging_far = swap(after(merging_pair, attention_far), "dp", far)
        near_side = swap(near, "dp", y)
        attention = ((pair, near, pair_side, near_side), ((0, 4), (2, 6), (1, 5), (3, 7)))
        merging_quad = joined(merging_pair, merging_far)
        merging_near = swap(merging_quad, "dp", z)
        merging = ((merging_quad, merging_near), ((0, 1, 4, 5), (2, 3, 6, 7)))
        down_far = swap(after(down_weight, near), "dp", far)[None]
    else:
        gathered = lambda shard: ((lax.all_gather(shard, "dp", axis=0),), None)
        attention, merging, down, up, encoder = map(
            gathered, (attention, merging, down_weight, up_weight, encoder_low)
        )

    projected, attend_full, decoder_full = project(
        tokens, norm_params, attention_bias, attention, hidden_size
    )
    if small:
        down_far = after(down_far, projected)
        down_pair = joined(down_weight[None], down_far)
        down_near = swap(down_pair, "dp", z)
        down_pair_side = swap(down_pair, "dp", y)
        up_far = swap(after(up_weight, down_far), "dp", far)[None]
    pieces, places = merging
    pieces = after(pieces, projected)
    if small:
        pieces = after(pieces, down_far)
    merge_own, encoded = gather_merge(pieces, places, width, hidden_size)
    mix_first, sums_first, hidden, prefix = attend_first(
        projected, encoded, encoder_bias[None], decoder_full, decoder_bias
    )

    merge_side = after(swap(merge_own, "tensor", SIDE), mix_first)
    if small:
        merge_side, up_far, down_near, down_pair_side = after(
            (merge_side, up_far, down_near, down_pair_side)
        )
    mix_side = swap(mix_first, "tensor", SIDE)
    half = rows // 2
    both_cores = joined(merge_own, merge_side, mix_first, mix_side)
    both_cores = swap(both_cores, "tensor", CORE)
    merges = ((merge_own, 0), (both_cores, 0), (merge_side, 0), (both_cores, width))
    mixes_first = (
        (mix_first, 0),
        (both_cores, 2 * width),
        (mix_side, 0),
        (both_cores, 2 * width + half),
    )
    proj_late = projected
    if small:
        proj_late = after(projected, down_near)
        down_near_side = swap(down_near, "dp", y)
        up_near = swap(joined(up_weight[None], up_far), "dp", z)
        up_far_side = swap(up_far, "dp", y)
    mix_second, sums_second = attend_second(proj_late, prefix)
    mix_side = swap(mix_second, "tensor", SIDE)
    branch_late = branch_bias
    if small:
        branch_late, down_near_side, up_near = after((branch_bias, down_near_side, up_near), mix_second)
        down = (
            (down_pair, down_pair_side, down_near, down_near_side),
            ((0, 4), (1, 5), (2, 6), (3, 7)),
        )
        up_near_side = swap(up_near, "dp", y)
    first_half = merge_half(tokens, norm_params, branch_late, mixes_first, merges)
    mix_side = after(mix_side, first_half)
    if small:
        mix_side, up_far_side = after((mix_side, up_far_side))
    mix_cores = swap(joined(mix_second, mix_side), "tensor", CORE)
    mixes_second = ((mix_second, 0), (mix_cores, 0), (mix_side, 0), (mix_cores, half))
    down_full, grad_hidden = down_back(after(cotangent, first_half), down)
    branch_late = after(branch_bias, grad_hidden)
    if small:
        encoder_far = swap(after(encoder_low, first_half), "dp", far)
        up = (
            (up_weight[None], up_side, up_far, up_far_side, up_near, up_near_side),
            ((0,), (1,), (4,), (5,), (2, 6), (3, 7)),
        )
    normed, resid = merge_half(
        tokens, norm_params, branch_late, mixes_second, merges, after(first_half, grad_hidden)
    )
    if small:
        normed = after(normed, encoder_far)

    def branch(act, *plus):
        part = lax.dot_general(
            act, down_full[0], (((1,), (1,)), ((), ())), preferred_element_type=jnp.float32
        )
        for one in plus:
            part = part + one.astype(jnp.float32)
        return part.astype(jnp.bfloat16)

    bias = up_bias[None]
    if small:
        normed = after(normed, encoder_far)
    act_both, up_both, up_full = feed_first(BOTH, normed, grad_hidden, up, bias)
    up_both = swap(up_both, "tensor", CORE)
    if small:
        encoder_pair = jnp.stack([encoder_low, after(encoder_far, act_both)])
        encoder_near = swap(encoder_pair, "dp", z)
    act_side, up_send = feed(SIDE, normed, grad_hidden, up_full, bias, up_both)
    up_from = swap(up_send, "tensor", SIDE)
    act_core, up_core = feed(CORE, after(normed, up_send), grad_hidden, up_full, bias)
    up_core = swap(up_core, "tensor", CORE)
    act_own, up_own = feed(OWN, after(normed, act_core), grad_hidden, up_full, bias)
    out_both = branch(after(act_both, act_own))
    up_from = after(up_from, out_both)
    if small:
        encoder_near = after(encoder_near, act_own)
        encoder_quad = joined(encoder_pair, encoder_near)
        encoder_side = swap(encoder_quad, "dp", y)
        encoder = ((encoder_quad, encoder_side), ((0, 4, 2, 6), (1, 5, 3, 7)))
        up_from = after(up_from, encoder_near)
    out_core = branch(after(act_core, up_from))
    out_own = branch(after(act_own, up_from))
    up_core = after(up_core, out_own, out_core)
    grad_resid, keep, send = middle(up_own, up_core, up_from, cotangent, resid, norm_params, merges)
    out_both = swap(out_both, "tensor", CORE)
    from_side = swap(send, "tensor", SIDE)
    core_keep = swap(keep, "tensor", CORE)
    out_core = swap(out_core, "tensor", CORE)
    out_send = branch(after(act_side, send), out_both)
    out_from = swap(out_send, "tensor", SIDE)
    encoder_full = assemble((after(encoder[0], send), encoder[1]), (1, width, hidden_size))
    hidden_own = lax.dynamic_slice(
        after(hidden, send), (jnp.uint32(0), own_start), (hidden.shape[0], dec_rows)
    )
    from_side = after(from_side, out_send, encoder_full, hidden_own)
    core_side = swap(from_side, "tensor", CORE)
    grad_prefix, grad_mix, log_sums, inner, grad_query = prefix_back(
        projected,
        prefix,
        (mix_first, mix_second),
        (sums_first, sums_second),
        (keep, from_side, core_keep, core_side),
    )
    grad_first = attend_back(0, projected, grad_mix, log_sums, inner, grad_query)
    prefix_total = plus(grad_prefix, swap(grad_prefix, "dp", 1))
    grad_second = attend_back(
        1, projected, after(grad_mix, prefix_total), log_sums, inner, grad_query
    )
    prefix_total = plus(prefix_total, swap(prefix_total, "dp", 2))
    gprojs = after((grad_first, grad_second), prefix_total, out_from, out_core)
    back_both = swap(project_back((BOTH,), gprojs, attend_full), "tensor", CORE)
    back_rest = project_back((CORE, OWN), gprojs, attend_full)
    back_both = after(back_both, back_rest)
    back_send = project_back((SIDE,), gprojs, attend_full, back_both)
    back_from = swap(back_send, "tensor", SIDE)
    bits = 4
    while bits < lax.axis_size("dp") // 2:
        prefix_total = plus(prefix_total, swap(prefix_total, "dp", bits))
        bits *= 2
    prefix_rest = after(swap(prefix_total, "dp", bits), back_send)
    prefix_total, joint = pl.pallas_call(
        tail_kernel,
        out_shape=(
            shaped(grad_prefix.shape, jnp.float32),
            shaped((PAD, hidden_size), jnp.float32),
        ),
        compiler_params=limited(),
        name="tail",
        cost_estimate=brief(),
    )(prefix_total, prefix_rest, hidden, decoder_full)
    joint = plus(joint, swap(joint, "tensor", CORE))
    joint_side = swap(joint, "tensor", SIDE)
    back_core = swap(back_rest, "tensor", CORE)
    output = output_rows(resid, out_own, out_core, out_from, branch_bias)
    input_grad = last(back_rest, back_core, back_from, tokens, grad_resid, norm_params)
    joint_side = after(joint_side, input_grad)

    params = [
        (prefix_table, first_table, second_table),
        (encoder_weight, first_encoder, second_encoder),
        (encoder_bias[None], first_encoder_bias[None], second_encoder_bias[None]),
        (decoder_weight, first_decoder, second_decoder),
        (decoder_bias, first_decoder_bias, second_decoder_bias),
    ]
    params = [array for group in params for array in group]
    grad_norm, *new = pl.pallas_call(
        update_kernel,
        out_shape=[shaped((1, 1), jnp.float32)] + [shaped(p.shape, p.dtype) for p in params],
        compiler_params=limited(),
        name="update",
    )(
        joint,
        joint_side,
        hidden,
        hidden_own,
        prefix_total,
        selected,
        selected_own,
        onehot,
        encoder_full[0],
        *params,
    )
    for i in range(6, 9):
        new[i] = new[i][0]
    return (output, input_grad, grad_norm[0, 0], *new)


def solution(mesh):
    in_specs = (
        P("dp", None),
        P("dp", None),
        P(),
        P("dp", None, "tensor"),
        P(None, "tensor"),
        P("dp", "tensor"),
        P(),
        P("dp", "tensor"),
        P("tensor"),
        P("dp", "tensor"),
        P(),
        P(),
        P("dp", None),
        P(),
        P("dp", None, "tensor"),
        P(None, "tensor"),
        P(),
        P(),
        P("dp", None),
        P("dp", None),
        P(),
        P(),
        P("dp", None, "tensor"),
        P("dp", None, "tensor"),
        P(None, "tensor"),
        P(None, "tensor"),
    )
    out_specs = (
        P(("dp", "tensor"), None),
        P(("dp", "tensor"), None),
        P(),
        P(),
        P(),
        P(),
        P("dp", None),
        P("dp", None),
        P("dp", None),
        P(),
        P(),
        P(),
        P("dp", None, "tensor"),
        P("dp", None, "tensor"),
        P("dp", None, "tensor"),
        P(None, "tensor"),
        P(None, "tensor"),
        P(None, "tensor"),
    )
    return jax.shard_map(
        on_device, mesh=mesh, in_specs=in_specs, out_specs=out_specs, check_vma=False
    )
```

```python
import functools

import jax
import jax.numpy as jnp
from jax import lax
from jax.experimental import pallas as pl
from jax.experimental.pallas import tpu as pltpu
from jax.sharding import PartitionSpec as P

HD = 64
PRE = 10
PAD = 16
STEP = 10
TILE = 256


NORM_EPS = 1e-05
CLIP_LIMIT = 0.001
LEARN_RATE = 0.05
WEIGHT_DECAY = 0.01
BETA_FIRST = 0.9
BETA_SECOND = 0.999
ADAM_EPS = 1e-08
MASKED = -1e30
GELU_COEF = 0.7978845608028654

NN = ((1,), (0,))
NT = ((1,), (1,))
TN = ((0,), (0,))
OWN, CORE, SIDE, BOTH = 0, 1, 2, 3


def dot(left, right, dims, precision=None):
    return lax.dot_general(
        left, right, (dims, ((), ())), precision=precision, preferred_element_type=jnp.float32
    )


def shaped(shape, dtype):
    return jax.ShapeDtypeStruct(shape, dtype)


def limited():
    return pltpu.CompilerParams(vmem_limit_bytes=24 * 2**20)


def cost(flops, *arrays):
    size = sum(a.size * a.dtype.itemsize for a in arrays)
    return pl.CostEstimate(flops=flops, transcendentals=0, bytes_accessed=size)


def brief():
    return pl.CostEstimate(flops=0, transcendentals=0, bytes_accessed=0)


def norm_parts(rows):
    offsets = rows - jnp.mean(rows, axis=-1, keepdims=True)
    scale = lax.rsqrt(jnp.mean(offsets * offsets, axis=-1, keepdims=True) + NORM_EPS)
    return offsets * scale, scale


def norm_back(rows, gain, grad):
    unit, scale = norm_parts(rows)
    grad = grad * gain
    mean = jnp.mean(grad, axis=-1, keepdims=True)
    along = jnp.mean(grad * unit, axis=-1, keepdims=True)
    return scale * (grad - mean - unit * along)


def adam_update(weight, grad, first, second, factor):
    clipped = grad * factor
    new_first = BETA_FIRST * first + (1.0 - BETA_FIRST) * clipped
    new_second = BETA_SECOND * second + (1.0 - BETA_SECOND) * clipped * clipped
    fix_first = 1.0 - BETA_FIRST**STEP
    fix_second = 1.0 - BETA_SECOND**STEP
    new_weight = weight * (1.0 - LEARN_RATE * WEIGHT_DECAY) - LEARN_RATE * (
        new_first / fix_first
    ) / (jnp.sqrt(new_second / fix_second) + ADAM_EPS)
    return (new_weight, new_first, new_second)


def swap(values, axis, bits):
    size = lax.axis_size(axis)
    return lax.ppermute(values, axis, [(i, i ^ bits) for i in range(size)])


def after(values, *others):
    return lax.optimization_barrier((values, *others))[0]


def placed(found):
    refs, bits = found
    if bits is None:
        return [(refs[0].at[i], i) for i in range(refs[0].shape[0])]
    here = lax.axis_index("dp")
    return [
        (ref.at[i], lax.bitwise_xor(here, differ))
        for ref, group in zip(refs, bits, strict=True)
        for i, differ in enumerate(group)
    ]


def joined(*pieces):
    return jnp.concatenate(pieces)


def sum_over(values, axis):
    bits = 1
    while bits < lax.axis_size(axis):
        values = values + swap(values, axis, bits)
        bits *= 2
    return values


def assemble_into(outs, found):
    for piece, place in placed(found):
        start = 0
        for out in outs:
            parts, rows = out.shape[0], out.shape[1] // lax.axis_size("dp")
            for part in range(parts):
                where = pl.ds(pl.multiple_of(place * rows, rows), rows)
                out[part, where, :] = piece[start : start + rows, :]
                start += rows


def assemble_kernel(bits, *refs):
    assemble_into(refs[-1:], (refs[:-1], bits))


def assemble(gathered, shape):
    pieces, bits = gathered
    out = shaped(shape, pieces[0].dtype)
    return pl.pallas_call(
        functools.partial(assemble_kernel, bits),
        out_shape=out,
        compiler_params=limited(),
        name="assemble",
        cost_estimate=brief(),
    )(*pieces)


def merge_weight_kernel(bits, *refs):
    pieces, (weight, encoded) = refs[:-2], refs[-2:]
    rows = weight.shape[0] // lax.axis_size("dp")
    sums = None
    for piece, place in placed((pieces, bits)):
        weight[pl.ds(pl.multiple_of(place * rows, rows), rows), :] = piece[:rows, :]
        sent = piece[rows:, :].astype(jnp.float32)
        sums = sent if sums is None else sums + sent
    width = weight.shape[1]
    for i in range(encoded.shape[1] // width):
        encoded[:, i * width : (i + 1) * width] = sums[i * PAD : (i + 1) * PAD]


def gather_merge(pieces, bits, rows, hidden):
    outs = (shaped((rows, pieces[0].shape[-1]), jnp.bfloat16), shaped((PAD, hidden), jnp.float32))
    return pl.pallas_call(
        functools.partial(merge_weight_kernel, bits),
        out_shape=outs,
        compiler_params=limited(),
        name="gather_merge",
        cost_estimate=brief(),
    )(*pieces)


def project_kernel(bits, tokens, norms, bias, *refs):
    pieces, (projected, attend, decoder) = refs[:-3], refs[-3:]
    assemble_into((attend, decoder), (pieces, bits))
    for start in range(0, tokens.shape[0], TILE):
        rows = slice(start, start + TILE)
        unit, _ = norm_parts(tokens[rows, :].astype(jnp.float32))
        normed = (unit * norms[0:1, :] + norms[1:2, :]).astype(jnp.bfloat16)
        for part in range(3):
            total = dot(normed, attend[part], NN) + bias[part : part + 1, :]
            projected[part, rows, :] = total.astype(jnp.bfloat16)


def project(tokens, norms, bias, gathered, hidden):
    pieces, bits = gathered
    rows, width = tokens.shape
    local = bias.shape[1]
    outs = (
        shaped((3, rows, local), jnp.bfloat16),
        shaped((3, width, local), jnp.bfloat16),
        shaped((2, hidden, local), jnp.bfloat16),
    )
    return pl.pallas_call(
        functools.partial(project_kernel, bits),
        out_shape=outs,
        compiler_params=limited(),
        name="project",
        cost_estimate=brief(),
    )(tokens, norms, bias, *pieces)


def down_kernel(bits, cotangent, *refs):
    pieces, (down, grad) = refs[:-2], refs[-2:]
    assemble_into((down,), (pieces, bits))
    for start in range(0, cotangent.shape[0], TILE):
        rows = slice(start, start + TILE)
        grad[rows, :] = dot(cotangent[rows, :], down[0], NN).astype(jnp.bfloat16)


def down_back(cotangent, gathered):
    pieces, bits = gathered
    rows, width = cotangent.shape
    units = pieces[0].shape[-1]
    outs = (shaped((1, width, units), jnp.bfloat16), shaped((rows, units), jnp.bfloat16))
    return pl.pallas_call(
        functools.partial(down_kernel, bits),
        out_shape=outs,
        compiler_params=limited(),
        name="down_back",
        cost_estimate=brief(),
    )(cotangent, *pieces)


def prefix_kernel(encoded, encoder_bias, decoder, decoder_bias, hidden, prefix):
    held = jnp.tanh(encoded[...] + encoder_bias[...])
    hidden[...] = held
    low = held.astype(jnp.bfloat16)
    for part in range(2):
        total = dot(low, decoder[part], NN) + decoder_bias[part : part + 1, :]
        prefix[part] = total.astype(jnp.bfloat16)


def attend_kernel(first, proj, prefix, mix, sums, mixed):
    rows, width = mix.shape
    lane = lax.broadcasted_iota(jnp.int32, (1, width), 1) // HD
    pre_col = lax.broadcasted_iota(jnp.int32, (TILE, PAD), 1)
    below = lax.broadcasted_iota(jnp.int32, (TILE, TILE), 0) >= lax.broadcasted_iota(
        jnp.int32, (TILE, TILE), 1
    )
    sum_col = lax.broadcasted_iota(jnp.int32, (TILE, 128), 1)
    sums[...] = jnp.zeros_like(sums)
    mixed[...] = jnp.zeros_like(mixed)

    def one_head(head, carry):
        mine = lane == head
        for start in range(first, first + rows, TILE):
            here = slice(start, start + TILE)
            there = slice(start - first, start - first + TILE)
            query = proj[0, here, :] * jnp.asarray(HD**-0.5, jnp.bfloat16)
            one = jnp.where(mine, query, jnp.zeros_like(query))
            scores = [
                jnp.where(pre_col < PRE, dot(one, prefix[0], NT), MASKED),
                jnp.where(below, dot(one, proj[1, here, :], NT), MASKED),
            ]
            values = [prefix[1], proj[2, here, :]]
            if start:
                scores.append(dot(one, proj[1, :start, :], NT))
                values.append(proj[2, :start, :])
            top = functools.reduce(jnp.maximum, [jnp.max(s, 1, keepdims=True) for s in scores])
            exps = [jnp.exp(s - top) for s in scores]
            total = sum(jnp.sum(e, 1, keepdims=True) for e in exps)
            inverse = 1.0 / total
            part = sum(
                dot((e * inverse).astype(jnp.bfloat16), v, NN)
                for e, v in zip(exps, values, strict=True)
            )
            mixed[there, :] = jnp.where(mine, part, mixed[there, :])
            sums[there, :] = jnp.where(sum_col == head, top + jnp.log(total), sums[there, :])
        return carry

    lax.fori_loop(0, width // HD, one_head, 0, unroll=2 if first else 1)
    mix[...] = mixed[...].astype(jnp.bfloat16)


def attend_first_kernel(proj, encoded, encoder_bias, decoder, decoder_bias, mix, sums, hidden, prefix, mixed):
    prefix_kernel(encoded, encoder_bias, decoder, decoder_bias, hidden, prefix)
    attend_kernel(0, proj, prefix, mix, sums, mixed)


def attend_shapes(proj):
    _, rows, width = proj.shape
    return shaped((rows // 2, width), jnp.bfloat16), shaped((rows // 2, 128), jnp.float32)


def attend_first(proj, encoded, encoder_bias, decoder, decoder_bias):
    _, rows, width = proj.shape
    outs = (
        *attend_shapes(proj),
        shaped(encoded.shape, jnp.float32),
        shaped((2, PAD, width), jnp.bfloat16),
    )
    return pl.pallas_call(
        attend_first_kernel,
        out_shape=outs,
        scratch_shapes=[pltpu.VMEM((rows // 2, width), jnp.float32)],
        compiler_params=limited(),
        name="attend_first",
        cost_estimate=brief(),
    )(proj, encoded, encoder_bias, decoder, decoder_bias)


def attend_second(proj, prefix):
    _, rows, width = proj.shape
    outs = attend_shapes(proj)
    return pl.pallas_call(
        functools.partial(attend_kernel, rows // 2),
        out_shape=outs,
        scratch_shapes=[pltpu.VMEM((rows // 2, width), jnp.float32)],
        compiler_params=limited(),
        name="attend_second",
        cost_estimate=brief(),
    )(proj, prefix)


def prefix_back_kernel(
    query, prefix, mix_first, mix_second, sums_first, sums_second, keep, side, core_keep, core_side, *refs
):
    gprefix, gmix, log_sums, inner, gquery = refs
    rows, width = gmix.shape
    half = rows // 2
    quarter = keep.shape[1]
    heads = width // HD
    me = lax.axis_index("tensor")
    for piece, bits in ((keep.at[0], OWN), (core_keep.at[1], CORE), (side.at[0], SIDE), (core_side.at[1], BOTH)):
        place = lax.bitwise_xor(me, bits) * quarter
        gmix[pl.ds(pl.multiple_of(place, quarter), quarter), :] = piece[...]
    head_of = lax.broadcasted_iota(jnp.int32, (8, width), 0) == lax.broadcasted_iota(
        jnp.int32, (8, width), 1
    ) // HD
    for i, (mix, sums) in enumerate(((mix_first, sums_first), (mix_second, sums_second))):
        part = slice(i * half, (i + 1) * half)
        log_sums[:, part] = sums[...].T[:8]
        product = gmix[part, :].astype(jnp.float32) * mix[...].astype(jnp.float32)
        inner[:, part] = dot(head_of.astype(jnp.float32), product, NT, lax.Precision.HIGHEST)
    lane = lax.broadcasted_iota(jnp.int32, (PAD, width), 1) // HD
    zero = jnp.zeros((PAD, width), jnp.bfloat16)
    keys, values = (
        jnp.concatenate([jnp.where(lane == head, prefix[i], zero) for head in range(heads)])
        for i in range(2)
    )
    scale = jnp.asarray(HD**-0.5, jnp.bfloat16)

    def spread(of_heads):
        return jnp.concatenate(
            [jnp.broadcast_to(of_heads[head : head + 1, :], (PAD, rows)) for head in range(heads)]
        )

    scaled = query[0] * scale
    grad = gmix[...]
    position = lax.broadcasted_iota(jnp.int32, (heads * PAD, rows), 0) % PAD
    scores = jnp.where(position < PRE, dot(keys, scaled, NT), MASKED)
    prob = jnp.exp(scores - spread(log_sums))
    dscore = (prob * (dot(values, grad, NT) - spread(inner))).astype(jnp.bfloat16)
    dkeys = dot(dscore, scaled, NN)
    dvalues = dot(prob.astype(jnp.bfloat16), grad, NN)
    for i, found in enumerate((dkeys, dvalues)):
        gprefix[i] = sum(
            jnp.where(lane == head, found[head * PAD : (head + 1) * PAD], 0.0)
            for head in range(heads)
        )
    gquery[...] = dot(keys * scale, dscore, TN)


def prefix_back(proj, prefix, mixes, sums, pieces):
    _, rows, width = proj.shape
    outs = (
        shaped(prefix.shape, jnp.float32),
        shaped((rows, width), jnp.bfloat16),
        shaped((8, rows), jnp.float32),
        shaped((8, rows), jnp.float32),
        shaped((width, rows), jnp.float32),
    )
    return pl.pallas_call(
        prefix_back_kernel,
        grid=(1,),
        in_specs=[pl.BlockSpec((1, rows, width), lambda i: (0, 0, 0))]
        + [whole_spec(a) for a in (prefix, *mixes, *sums, *pieces)],
        out_specs=[whole_spec(o) for o in outs],
        out_shape=outs,
        compiler_params=limited(),
        name="prefix_back",
        cost_estimate=brief(),
    )(proj, prefix, *mixes, *sums, *pieces)


def attend_back_kernel(pair, proj, gmix, log_sums, inner, gquery_prefix, gproj, gquery, gkey, gvalue, keys_col):
    rows, width = gmix.shape
    lane = lax.broadcasted_iota(jnp.int32, (1, width), 1) // HD
    seen = lax.broadcasted_iota(jnp.int32, (TILE, TILE), 0) <= lax.broadcasted_iota(
        jnp.int32, (TILE, TILE), 1
    )
    scale = jnp.asarray(HD**-0.5, jnp.bfloat16)
    keys_col[...] = (proj[1] * scale).T
    gkey[...] = jnp.zeros_like(gkey)
    gvalue[...] = jnp.zeros_like(gvalue)

    def one_head(head, carry):
        mine = lane == head
        cols = pl.ds(pl.multiple_of(head * HD, HD), HD)
        row = pl.ds(pair * (width // HD) + head, 1)
        for start in range(0, rows, TILE):
            here = slice(start, start + TILE)
            query = proj[0, here, :] * scale
            grad = gmix[here, :]
            one = jnp.where(mine, query, jnp.zeros_like(query))
            one_grad = jnp.where(mine, grad, jnp.zeros_like(grad))
            log_sum = log_sums[row, here]
            shared = inner[row, here]
            dquery = gquery_prefix[cols, here]
            for at in range(0, start + TILE, TILE):
                there = slice(at, at + TILE)
                scores = dot(proj[1, there, :], one, NT)
                if at == start:
                    scores = jnp.where(seen, scores, MASKED)
                prob = jnp.exp(scores - log_sum)
                dscore = prob * (dot(proj[2, there, :], one_grad, NT) - shared)
                dscore = dscore.astype(jnp.bfloat16)
                gkey[there, :] += dot(dscore, one, NN)
                gvalue[there, :] += dot(prob.astype(jnp.bfloat16), one_grad, NN)
                dquery = dquery + dot(keys_col[cols, there], dscore, NN)
            gquery[cols, here] = dquery
        return carry

    lax.fori_loop(0, width // HD, one_head, 0)
    gproj[0] = gquery[...].T.astype(jnp.bfloat16)
    gproj[1] = gkey[...].astype(jnp.bfloat16)
    gproj[2] = gvalue[...].astype(jnp.bfloat16)


def attend_back(pair, proj, gmix, log_sums, inner, gquery):
    _, rows, local = proj.shape
    width = 2 * HD
    out = shaped((3, rows, width), jnp.bfloat16)
    return pl.pallas_call(
        functools.partial(attend_back_kernel, pair),
        grid=(1,),
        in_specs=[
            pl.BlockSpec((3, rows, width), lambda i: (0, 0, pair)),
            pl.BlockSpec((rows, width), lambda i: (0, pair)),
            whole_spec(log_sums),
            whole_spec(inner),
            pl.BlockSpec((width, rows), lambda i: (pair, 0)),
        ],
        out_specs=whole_spec(out),
        out_shape=out,
        scratch_shapes=[
            pltpu.VMEM((width, rows), jnp.float32),
            pltpu.VMEM((rows, width), jnp.float32),
            pltpu.VMEM((rows, width), jnp.float32),
            pltpu.VMEM((width, rows), jnp.bfloat16),
        ],
        compiler_params=limited(),
        name="attend_back",
        cost_estimate=cost(12 * rows * rows * width, proj, gmix, gquery, out),
    )(proj, gmix, log_sums, inner, gquery)


def merge_kernel(first, tokens, norms, branch, *refs):
    mixes, merges, earlier, (normed, resid_own) = refs[:4], refs[4:8], refs[8:-2], refs[-2:]
    i = pl.program_id(0)
    merged = sum(dot(m[...], w[...], NT) for m, w in zip(mixes, merges, strict=True))
    resid = tokens[...].astype(jnp.float32) + merged + branch[0:1, :]
    unit, _ = norm_parts(resid)
    normed[...] = (unit * norms[2:3, :] + norms[3:4, :]).astype(jnp.bfloat16)
    if earlier:

        @pl.when(i == 0)
        def _():
            resid_own[...] = earlier[1][...]

    @pl.when(i + first == lax.axis_index("tensor"))
    def _():
        resid_own[...] = resid


def part_spec(shape, first):
    return pl.BlockSpec(shape, lambda i: (first // shape[0] + i, 0))


def fixed_spec(shape, first):
    return pl.BlockSpec(shape, lambda i: (first // shape[0], 0))


def merge_half(tokens, norms, branch, mixes, merges, earlier=()):
    rows, width = tokens.shape
    share = rows // lax.axis_size("tensor")
    local = mixes[0][0].shape[1]
    steps = rows // 2 // share
    first = steps if earlier else 0
    whole = lambda a: pl.BlockSpec(a.shape, lambda i: (0,) * a.ndim)
    outs = (shaped((rows, width), jnp.bfloat16), shaped((share, width), jnp.float32))
    return pl.pallas_call(
        functools.partial(merge_kernel, first),
        grid=(steps,),
        in_specs=[pl.BlockSpec((share, width), lambda i: (i + first, 0)), whole(norms), whole(branch)]
        + [part_spec((share, local), start) for _, start in mixes]
        + [fixed_spec((width, local), start) for _, start in merges]
        + ([pl.BlockSpec(memory_space=pl.ANY), whole(earlier[1])] if earlier else []),
        out_specs=(
            pl.BlockSpec((share, width), lambda i: (i + first, 0)),
            pl.BlockSpec((share, width), lambda i: (0, 0)),
        ),
        out_shape=outs,
        input_output_aliases={11: 0} if earlier else {},
        compiler_params=limited(),
        name="merge_second" if earlier else "merge_first",
        cost_estimate=brief(),
    )(tokens, norms, branch, *[a for a, _ in (*mixes, *merges)], *earlier)


def feed_rows(normed, ghidden, up, bias, act, part, plus=None):
    value = dot(normed[...], up, NN) + bias[...]
    square = value * value
    tanh = jnp.tanh(GELU_COEF * value * (1.0 + 0.044715 * square))
    act[...] = (0.5 * value * (1.0 + tanh)).astype(jnp.bfloat16)
    slope = 0.5 * (1.0 + tanh) + 0.5 * GELU_COEF * value * (1.0 - tanh * tanh) * (
        1.0 + 3.0 * 0.044715 * square
    )
    gpre = (ghidden[...].astype(jnp.float32) * slope).astype(jnp.bfloat16)
    total = dot(gpre, up, NT)
    if plus is not None:
        total = total + plus[...].astype(jnp.float32)
    part[...] = total.astype(jnp.bfloat16)


def feed_first_kernel(bits, normed, ghidden, bias, *refs):
    pieces, (act, part, up) = refs[:-3], refs[-3:]
    assemble_into((up,), (pieces, bits))
    feed_rows(normed, ghidden, up[0], bias, act, part)


def feed_kernel(up, bias, normed, ghidden, *refs):
    feed_rows(normed, ghidden, up[0], bias, *refs[-2:], *refs[:-2])


def block_of(*bits):
    last = len(bits) - 1
    return lambda i: (lax.bitwise_xor(lax.axis_index("tensor"), bits[0] if not last else last - i), 0)


def whole_spec(a):
    return pl.BlockSpec(a.shape, lambda i: (0,) * a.ndim)


def feed_first(bits, normed, ghidden, gathered, bias):
    pieces, places = gathered
    rows, width = normed.shape
    share = rows // lax.axis_size("tensor")
    units = pieces[0].shape[-1]
    outs = (
        shaped((share, units), jnp.bfloat16),
        shaped((share, width), jnp.bfloat16),
        shaped((1, width, units), jnp.bfloat16),
    )
    return pl.pallas_call(
        functools.partial(feed_first_kernel, places),
        grid=(1,),
        in_specs=[
            pl.BlockSpec((share, width), block_of(bits)),
            pl.BlockSpec((share, units), block_of(bits)),
            whole_spec(bias),
        ]
        + [whole_spec(p) for p in pieces],
        out_specs=[whole_spec(o) for o in outs],
        out_shape=outs,
        compiler_params=limited(),
        name="feed_first",
        cost_estimate=brief(),
    )(normed, ghidden, bias, *pieces)


def feed(differ, normed, ghidden, up, bias, *plus):
    rows, width = normed.shape
    share = rows // lax.axis_size("tensor")
    units = up.shape[-1]
    outs = (shaped((share, units), jnp.bfloat16), shaped((share, width), jnp.bfloat16))
    return pl.pallas_call(
        feed_kernel,
        grid=(1,),
        in_specs=[
            whole_spec(up),
            whole_spec(bias),
            pl.BlockSpec((share, width), block_of(differ)),
            pl.BlockSpec((share, units), block_of(differ)),
        ]
        + [whole_spec(p) for p in plus],
        out_specs=[whole_spec(o) for o in outs],
        out_shape=outs,
        compiler_params=limited(),
        name="feed",
        cost_estimate=brief(),
    )(up, bias, normed, ghidden, *plus)


def back_kernel(weight, one, two, *refs):
    total = sum(
        dot(jnp.concatenate([one[i], two[i]], axis=1), weight[i], NT) for i in range(weight.shape[0])
    )
    for plus in refs[:-1]:
        total = total + plus[...].astype(jnp.float32)
    refs[-1][...] = total.astype(jnp.bfloat16)


def project_back(bits, gprojs, attend, *plus):
    _, rows, local = gprojs[0].shape
    width = attend.shape[1]
    share = rows // lax.axis_size("tensor")
    steps = len(bits)
    block = block_of(*bits)
    out = shaped((steps * share, width), jnp.bfloat16)
    return pl.pallas_call(
        back_kernel,
        grid=(steps,),
        in_specs=[whole_spec(attend)]
        + [pl.BlockSpec((3, share, local), lambda i: (0, *block(i)))] * 2
        + [whole_spec(p) for p in plus],
        out_specs=pl.BlockSpec((share, width), lambda i: (i, 0)),
        out_shape=out,
        compiler_params=limited(),
        name="project_back",
        cost_estimate=brief(),
    )(attend, *gprojs, *plus)


def three(own, core, side):
    return own[...].astype(jnp.float32) + core[...].astype(jnp.float32) + side[...].astype(jnp.float32)


def middle_kernel(own, core, side, cotangent, resid, norms, *refs):
    merges, (gresid, keep, send) = refs[:4], refs[4:]
    total = three(own, core, side)
    grad = cotangent[...].astype(jnp.float32) + norm_back(resid[...], norms[2:3, :], total)
    gresid[...] = grad
    low = grad.astype(jnp.bfloat16)
    keep[0] = dot(low, merges[OWN][...], NN).astype(jnp.bfloat16)
    keep[1] = dot(low, merges[CORE][...], NN).astype(jnp.bfloat16)
    send[0] = dot(low, merges[SIDE][...], NN).astype(jnp.bfloat16)
    send[1] = dot(low, merges[BOTH][...], NN).astype(jnp.bfloat16)


def row_of(share, width, step):
    return pl.BlockSpec((share, width), lambda i: (step, 0))


def middle(own, core, side, cotangent, resid, norms, merges):
    share, width = resid.shape
    local = merges[0][0].shape[1]
    outs = (
        shaped((share, width), jnp.float32),
        shaped((2, share, local), jnp.bfloat16),
        shaped((2, share, local), jnp.bfloat16),
    )
    mine = pl.BlockSpec((share, width), block_of(OWN))
    return pl.pallas_call(
        middle_kernel,
        grid=(1,),
        in_specs=[whole_spec(own), whole_spec(core), whole_spec(side), mine]
        + [whole_spec(a) for a in (resid, norms)]
        + [fixed_spec((width, local), start) for _, start in merges],
        out_specs=[whole_spec(o) for o in outs],
        out_shape=outs,
        compiler_params=limited(),
        name="middle",
        cost_estimate=brief(),
    )(own, core, side, cotangent, resid, norms, *[a for a, _ in merges])


def last_kernel(own, core, side, tokens, gresid, norms, out):
    total = three(own, core, side)
    rows = tokens[...].astype(jnp.float32)
    out[...] = (gresid[...] + norm_back(rows, norms[0:1, :], total)).astype(jnp.bfloat16)


def last(own, core, side, tokens, gresid, norms):
    share, width = gresid.shape
    out = shaped((share, width), jnp.bfloat16)
    return pl.pallas_call(
        last_kernel,
        grid=(1,),
        in_specs=[
            row_of(share, width, 1),
            row_of(share, width, 0),
            whole_spec(side),
            pl.BlockSpec((share, width), block_of(OWN)),
            whole_spec(gresid),
            whole_spec(norms),
        ],
        out_specs=whole_spec(out),
        out_shape=out,
        compiler_params=limited(),
        name="last",
        cost_estimate=brief(),
    )(own, core, side, tokens, gresid, norms)


def plus_kernel(one, two, out):
    out[...] = one[...] + two[...]


def plus(one, two):
    return pl.pallas_call(
        plus_kernel,
        out_shape=shaped(one.shape, one.dtype),
        compiler_params=limited(),
        name="plus",
        cost_estimate=brief(),
    )(one, two)


def down_rows_kernel(act, down, *refs):
    total = dot(act[...], down[0], NT)
    for one in refs[:-1]:
        total = total + one[...].astype(jnp.float32)
    refs[-1][...] = total.astype(jnp.bfloat16)


def down_rows(act, down, *rest):
    return pl.pallas_call(
        down_rows_kernel,
        out_shape=shaped((act.shape[0], down.shape[1]), jnp.bfloat16),
        compiler_params=limited(),
        name="down_rows",
        cost_estimate=brief(),
    )(act, down, *rest)


def output_kernel(resid, own, core, side, branch, out):
    out[...] = (resid[...] + three(own, core, side) + branch[1:2, :]).astype(jnp.bfloat16)


def output_rows(resid, own, core, side, branch):
    return pl.pallas_call(
        output_kernel,
        out_shape=shaped(resid.shape, jnp.bfloat16),
        compiler_params=limited(),
        name="output",
        cost_estimate=brief(),
    )(resid, own, core, side, branch)


def tail_kernel(one, two, hidden, decoder, total, joint):
    total[...] = one[...] + two[...]
    low = total[...].astype(jnp.bfloat16)
    held = hidden[...].astype(jnp.bfloat16)
    part = jnp.zeros(joint.shape, jnp.float32)
    square = jnp.zeros((1, 1), jnp.float32)
    for i in range(2):
        part = part + dot(low[i], decoder[i], NT)
        grad = dot(held, low[i], TN)
        square = square + jnp.sum(jnp.sum(grad * grad, 0, keepdims=True), 1, keepdims=True)
        bias = jnp.sum(low[i].astype(jnp.float32), 0, keepdims=True)
        square = square + jnp.sum(bias * bias, 1, keepdims=True)
    row = lax.broadcasted_iota(jnp.int32, joint.shape, 0)
    joint[...] = jnp.where(row == PAD - 1, square, part)


def update_kernel(joint_one, joint_two, hidden, hidden_own, total, selected, selected_own, onehot, encoder, *refs):
    table, enc, enc_bias, dec, dec_bias = (refs[i : i + 3] for i in range(0, 15, 3))
    norm_out, outs = refs[15], refs[16:]
    held = hidden[...]
    row = lax.broadcasted_iota(jnp.int32, held.shape, 0)
    joint = joint_one[...] + joint_two[...]
    grad = jnp.where(row < PRE, joint, 0.0) * (1.0 - held * held)
    grad = grad.astype(jnp.bfloat16)
    square = joint[PAD - 1 : PAD, 0:1]

    def summed(values):
        return jnp.sum(jnp.sum(values * values, 0, keepdims=True), 1, keepdims=True)

    square = square + summed(dot(selected[...], grad, TN))
    grad_bias = jnp.sum(grad.astype(jnp.float32), 0, keepdims=True)
    square = square + summed(grad_bias)
    grad_selected = dot(grad, encoder[...], NT)
    grad_table = dot(onehot[...], grad_selected, TN, lax.Precision.HIGHEST)[:PRE]
    square = square + summed(grad_table)
    norm = jnp.sqrt(square)
    norm_out[...] = norm
    factor = CLIP_LIMIT / (norm + 1e-06)

    def update(old, grad_of, at, index):
        weight, first, second = (ref[index] for ref in old)
        for out, new in zip(
            outs[at : at + 3], adam_update(weight, grad_of, first, second, factor), strict=True
        ):
            out[index] = new

    update(table, grad_table, 0, ...)
    update(enc, dot(selected_own[...], grad, TN), 3, ...)
    update(enc_bias, grad_bias, 6, ...)
    low = total[...].astype(jnp.bfloat16)
    held_own = hidden_own[...].astype(jnp.bfloat16)
    for i in range(2):
        update(dec, dot(held_own, low[i], TN), 9, (slice(None), i, slice(None)))
        bias = jnp.sum(low[i].astype(jnp.float32), 0, keepdims=True)
        update(dec_bias, bias, 12, (slice(i, i + 1), slice(None)))


def on_device(
    tokens,
    cotangent,
    norm_params,
    attention_weight,
    attention_bias,
    merge_weight,
    branch_bias,
    up_weight,
    up_bias,
    down_weight,
    prefix_ids,
    prefix_table,
    encoder_weight,
    encoder_bias,
    decoder_weight,
    decoder_bias,
    first_table,
    second_table,
    first_encoder,
    second_encoder,
    first_encoder_bias,
    second_encoder_bias,
    first_decoder,
    second_decoder,
    first_decoder_bias,
    second_decoder_bias,
):
    highest = lax.Precision.HIGHEST
    dp_index = lax.axis_index("dp")
    rows, width = tokens.shape
    share = rows // lax.axis_size("tensor")
    local = merge_weight.shape[1]
    units = up_weight.shape[1]
    in_rows = attention_weight.shape[0]
    hidden_size = encoder_weight.shape[1]
    dec_rows = decoder_weight.shape[0]
    halves = hidden_size // local

    decoder_low = decoder_weight.astype(jnp.bfloat16)
    attention = jnp.concatenate(
        [
            attention_weight.transpose(1, 0, 2).reshape(3 * in_rows, local),
            decoder_low.transpose(1, 0, 2).reshape(2 * dec_rows, local),
        ]
    )
    onehot = (
        jnp.pad(prefix_ids, (0, PAD - PRE), constant_values=PAD)[:, None]
        == jnp.arange(PAD, dtype=jnp.int32)[None, :]
    ).astype(jnp.float32)
    selected = jnp.dot(onehot[:, :PRE], prefix_table, precision=highest).astype(jnp.bfloat16)
    selected_own = lax.dynamic_slice_in_dim(selected, dp_index * in_rows, in_rows, 1)
    encoder_low = encoder_weight.astype(jnp.bfloat16)
    encoded_own = jnp.dot(selected_own, encoder_low, preferred_element_type=jnp.float32)
    sent = encoded_own.astype(jnp.bfloat16).reshape(PAD, halves, local).transpose(1, 0, 2)
    merging = jnp.concatenate([merge_weight, sent.reshape(halves * PAD, local)])

    own_start = dp_index.astype(jnp.uint32) * dec_rows
    small = lax.axis_size("dp") == 8
    if small:
        y, z, far = 1, 2, 4
        attention_far = swap(attention, "dp", far)
        merging_side = swap(merging, "dp", y)[None]
        up_side = swap(up_weight, "dp", y)[None]
        attention_far, own_start = after((attention_far, own_start), merging_side, up_side)
        pair = jnp.stack([attention, attention_far])
        near = swap(pair, "dp", z)
        pair_side = swap(pair, "dp", y)
        merging_pair = joined(merging[None], merging_side)
        merging_far = swap(after(merging_pair, attention_far), "dp", far)
        near_side = swap(near, "dp", y)
        attention = ((pair, near, pair_side, near_side), ((0, 4), (2, 6), (1, 5), (3, 7)))
        merging_quad = joined(merging_pair, merging_far)
        merging_near = swap(merging_quad, "dp", z)
        merging = ((merging_quad, merging_near), ((0, 1, 4, 5), (2, 3, 6, 7)))
        down_far = swap(after(down_weight, near), "dp", far)[None]
    else:
        gathered = lambda shard: ((lax.all_gather(shard, "dp", axis=0),), None)
        attention, merging, down, up, encoder = map(
            gathered, (attention, merging, down_weight, up_weight, encoder_low)
        )

    projected, attend_full, decoder_full = project(
        tokens, norm_params, attention_bias, attention, hidden_size
    )
    if small:
        down_far = after(down_far, projected)
        down_pair = joined(down_weight[None], down_far)
        down_near = swap(down_pair, "dp", z)
        down_pair_side = swap(down_pair, "dp", y)
        up_far = swap(after(up_weight, down_far), "dp", far)[None]
    pieces, places = merging
    pieces = after(pieces, projected)
    if small:
        pieces = after(pieces, down_far)
    merge_own, encoded = gather_merge(pieces, places, width, hidden_size)
    mix_first, sums_first, hidden, prefix = attend_first(
        projected, encoded, encoder_bias[None], decoder_full, decoder_bias
    )

    merge_side = after(swap(merge_own, "tensor", SIDE), mix_first)
    if small:
        merge_side, up_far, down_near, down_pair_side = after(
            (merge_side, up_far, down_near, down_pair_side)
        )
    mix_side = swap(mix_first, "tensor", SIDE)
    half = rows // 2
    both_cores = joined(merge_own, merge_side, mix_first, mix_side)
    both_cores = swap(both_cores, "tensor", CORE)
    merges = ((merge_own, 0), (both_cores, 0), (merge_side, 0), (both_cores, width))
    mixes_first = (
        (mix_first, 0),
        (both_cores, 2 * width),
        (mix_side, 0),
        (both_cores, 2 * width + half),
    )
    proj_late = projected
    if small:
        proj_late = after(projected, down_near)
        down_near_side = swap(down_near, "dp", y)
        up_near = swap(joined(up_weight[None], up_far), "dp", z)
        up_far_side = swap(up_far, "dp", y)
    mix_second, sums_second = attend_second(proj_late, prefix)
    mix_side = swap(mix_second, "tensor", SIDE)
    branch_late = branch_bias
    if small:
        branch_late, down_near_side, up_near = after((branch_bias, down_near_side, up_near), mix_second)
        down = (
            (down_pair, down_pair_side, down_near, down_near_side),
            ((0, 4), (1, 5), (2, 6), (3, 7)),
        )
        up_near_side = swap(up_near, "dp", y)
    first_half = merge_half(tokens, norm_params, branch_late, mixes_first, merges)
    mix_side = after(mix_side, first_half)
    if small:
        mix_side, up_far_side = after((mix_side, up_far_side))
    mix_cores = swap(joined(mix_second, mix_side), "tensor", CORE)
    mixes_second = ((mix_second, 0), (mix_cores, 0), (mix_side, 0), (mix_cores, half))
    down_full, grad_hidden = down_back(after(cotangent, first_half), down)
    branch_late = after(branch_bias, grad_hidden)
    if small:
        encoder_far = swap(after(encoder_low, first_half), "dp", far)
        up = (
            (up_weight[None], up_side, up_far, up_far_side, up_near, up_near_side),
            ((0,), (1,), (4,), (5,), (2, 6), (3, 7)),
        )
    normed, resid = merge_half(
        tokens, norm_params, branch_late, mixes_second, merges, after(first_half, grad_hidden)
    )
    def branch(act, *rest):
        return down_rows(act, down_full, *rest)

    bias = up_bias[None]
    if small:
        normed = after(normed, encoder_far)
    act_both, up_both, up_full = feed_first(BOTH, normed, grad_hidden, up, bias)
    up_both = swap(up_both, "tensor", CORE)
    if small:
        encoder_pair = jnp.stack([encoder_low, after(encoder_far, act_both)])
        encoder_near = swap(encoder_pair, "dp", z)
    act_side, up_send = feed(SIDE, normed, grad_hidden, up_full, bias, up_both)
    up_from = swap(up_send, "tensor", SIDE)
    act_core, up_core = feed(CORE, after(normed, up_send), grad_hidden, up_full, bias)
    up_core = swap(up_core, "tensor", CORE)
    act_own, up_own = feed(OWN, after(normed, act_core), grad_hidden, up_full, bias)
    out_both = branch(after(act_both, act_own))
    out_core = branch(after(act_core, act_own))
    out_own = branch(act_own)
    up_from = after(up_from, out_both, out_core, out_own)
    if small:
        encoder_near = after(encoder_near, act_own)
        encoder_quad = joined(encoder_pair, encoder_near)
        encoder_side = swap(encoder_quad, "dp", y)
        encoder = ((encoder_quad, encoder_side), ((0, 4, 2, 6), (1, 5, 3, 7)))
        up_from = after(up_from, encoder_near)
    grad_resid, keep, send = middle(up_own, up_core, up_from, cotangent, resid, norm_params, merges)
    out_both = swap(out_both, "tensor", CORE)
    from_side = swap(send, "tensor", SIDE)
    core_keep = swap(keep, "tensor", CORE)
    out_core = swap(out_core, "tensor", CORE)
    out_send = branch(after(act_side, send), out_both)
    out_from = swap(out_send, "tensor", SIDE)
    encoder_full = assemble((after(encoder[0], send), encoder[1]), (1, width, hidden_size))
    hidden_own = lax.dynamic_slice(
        after(hidden, send), (jnp.uint32(0), own_start), (hidden.shape[0], dec_rows)
    )
    from_side = after(from_side, out_send, encoder_full, hidden_own)
    core_side = swap(from_side, "tensor", CORE)
    grad_prefix, grad_mix, log_sums, inner, grad_query = prefix_back(
        projected,
        prefix,
        (mix_first, mix_second),
        (sums_first, sums_second),
        (keep, from_side, core_keep, core_side),
    )
    grad_first = attend_back(0, projected, grad_mix, log_sums, inner, grad_query)
    prefix_total = plus(grad_prefix, swap(grad_prefix, "dp", 1))
    grad_second = attend_back(
        1, projected, after(grad_mix, prefix_total), log_sums, inner, grad_query
    )
    prefix_total = plus(prefix_total, swap(prefix_total, "dp", 2))
    gprojs = after((grad_first, grad_second), prefix_total, out_from, out_core)
    back_both = swap(project_back((BOTH,), gprojs, attend_full), "tensor", CORE)
    back_rest = project_back((CORE, OWN), gprojs, attend_full)
    back_both = after(back_both, back_rest)
    back_send = project_back((SIDE,), gprojs, attend_full, back_both)
    back_from = swap(back_send, "tensor", SIDE)
    bits = 4
    while bits < lax.axis_size("dp") // 2:
        prefix_total = plus(prefix_total, swap(prefix_total, "dp", bits))
        bits *= 2
    prefix_rest = after(swap(prefix_total, "dp", bits), back_send)
    prefix_total, joint = pl.pallas_call(
        tail_kernel,
        out_shape=(
            shaped(grad_prefix.shape, jnp.float32),
            shaped((PAD, hidden_size), jnp.float32),
        ),
        compiler_params=limited(),
        name="tail",
        cost_estimate=brief(),
    )(prefix_total, prefix_rest, hidden, decoder_full)
    joint = plus(joint, swap(joint, "tensor", CORE))
    joint_side = swap(joint, "tensor", SIDE)
    back_core = swap(back_rest, "tensor", CORE)
    output = output_rows(resid, out_own, out_core, out_from, branch_bias)
    input_grad = last(back_rest, back_core, back_from, tokens, grad_resid, norm_params)
    joint_side = after(joint_side, input_grad)

    params = [
        (prefix_table, first_table, second_table),
        (encoder_weight, first_encoder, second_encoder),
        (encoder_bias[None], first_encoder_bias[None], second_encoder_bias[None]),
        (decoder_weight, first_decoder, second_decoder),
        (decoder_bias, first_decoder_bias, second_decoder_bias),
    ]
    params = [array for group in params for array in group]
    grad_norm, *new = pl.pallas_call(
        update_kernel,
        out_shape=[shaped((1, 1), jnp.float32)] + [shaped(p.shape, p.dtype) for p in params],
        compiler_params=limited(),
        name="update",
    )(
        joint,
        joint_side,
        hidden,
        hidden_own,
        prefix_total,
        selected,
        selected_own,
        onehot,
        encoder_full[0],
        *params,
    )
    for i in range(6, 9):
        new[i] = new[i][0]
    return (output, input_grad, grad_norm[0, 0], *new)


def solution(mesh):
    in_specs = (
        P("dp", None),
        P("dp", None),
        P(),
        P("dp", None, "tensor"),
        P(None, "tensor"),
        P("dp", "tensor"),
        P(),
        P("dp", "tensor"),
        P("tensor"),
        P("dp", "tensor"),
        P(),
        P(),
        P("dp", None),
        P(),
        P("dp", None, "tensor"),
        P(None, "tensor"),
        P(),
        P(),
        P("dp", None),
        P("dp", None),
        P(),
        P(),
        P("dp", None, "tensor"),
        P("dp", None, "tensor"),
        P(None, "tensor"),
        P(None, "tensor"),
    )
    out_specs = (
        P(("dp", "tensor"), None),
        P(("dp", "tensor"), None),
        P(),
        P(),
        P(),
        P(),
        P("dp", None),
        P("dp", None),
        P("dp", None),
        P(),
        P(),
        P(),
        P("dp", None, "tensor"),
        P("dp", None, "tensor"),
        P("dp", None, "tensor"),
        P(None, "tensor"),
        P(None, "tensor"),
        P(None, "tensor"),
    )
    return jax.shard_map(
        on_device, mesh=mesh, in_specs=in_specs, out_specs=out_specs, check_vma=False
    )
```

```python
import functools

import jax
import jax.numpy as jnp
from jax import lax
from jax.experimental import pallas as pl
from jax.experimental.pallas import tpu as pltpu
from jax.sharding import PartitionSpec as P

HD = 64
PRE = 10
PAD = 16
STEP = 10
TILE = 256


NORM_EPS = 1e-05
CLIP_LIMIT = 0.001
LEARN_RATE = 0.05
WEIGHT_DECAY = 0.01
BETA_FIRST = 0.9
BETA_SECOND = 0.999
ADAM_EPS = 1e-08
MASKED = -1e30
GELU_COEF = 0.7978845608028654

NN = ((1,), (0,))
NT = ((1,), (1,))
TN = ((0,), (0,))
OWN, CORE, SIDE, BOTH = 0, 1, 2, 3


def dot(left, right, dims, precision=None):
    return lax.dot_general(
        left, right, (dims, ((), ())), precision=precision, preferred_element_type=jnp.float32
    )


def shaped(shape, dtype):
    return jax.ShapeDtypeStruct(shape, dtype)


def limited():
    return pltpu.CompilerParams(vmem_limit_bytes=24 * 2**20)


def cost(flops, *arrays):
    size = sum(a.size * a.dtype.itemsize for a in arrays)
    return pl.CostEstimate(flops=flops, transcendentals=0, bytes_accessed=size)


def brief():
    return pl.CostEstimate(flops=0, transcendentals=0, bytes_accessed=0)


def norm_parts(rows):
    offsets = rows - jnp.mean(rows, axis=-1, keepdims=True)
    scale = lax.rsqrt(jnp.mean(offsets * offsets, axis=-1, keepdims=True) + NORM_EPS)
    return offsets * scale, scale


def norm_back(rows, gain, grad):
    unit, scale = norm_parts(rows)
    grad = grad * gain
    mean = jnp.mean(grad, axis=-1, keepdims=True)
    along = jnp.mean(grad * unit, axis=-1, keepdims=True)
    return scale * (grad - mean - unit * along)


def adam_update(weight, grad, first, second, factor):
    clipped = grad * factor
    new_first = BETA_FIRST * first + (1.0 - BETA_FIRST) * clipped
    new_second = BETA_SECOND * second + (1.0 - BETA_SECOND) * clipped * clipped
    fix_first = 1.0 - BETA_FIRST**STEP
    fix_second = 1.0 - BETA_SECOND**STEP
    new_weight = weight * (1.0 - LEARN_RATE * WEIGHT_DECAY) - LEARN_RATE * (
        new_first / fix_first
    ) / (jnp.sqrt(new_second / fix_second) + ADAM_EPS)
    return (new_weight, new_first, new_second)


def swap(values, axis, bits):
    size = lax.axis_size(axis)
    return lax.ppermute(values, axis, [(i, i ^ bits) for i in range(size)])


def after(values, *others):
    return lax.optimization_barrier((values, *others))[0]


def placed(found):
    refs, bits = found
    if bits is None:
        return [(refs[0].at[i], i) for i in range(refs[0].shape[0])]
    here = lax.axis_index("dp")
    return [
        (ref.at[i], lax.bitwise_xor(here, differ))
        for ref, group in zip(refs, bits, strict=True)
        for i, differ in enumerate(group)
    ]


def joined(*pieces):
    return jnp.concatenate(pieces)


def sum_over(values, axis):
    bits = 1
    while bits < lax.axis_size(axis):
        values = values + swap(values, axis, bits)
        bits *= 2
    return values


def assemble_into(outs, found):
    for piece, place in placed(found):
        start = 0
        for out in outs:
            parts, rows = out.shape[0], out.shape[1] // lax.axis_size("dp")
            for part in range(parts):
                where = pl.ds(pl.multiple_of(place * rows, rows), rows)
                out[part, where, :] = piece[start : start + rows, :]
                start += rows


def assemble_kernel(bits, *refs):
    assemble_into(refs[-1:], (refs[:-1], bits))


def assemble(gathered, shape):
    pieces, bits = gathered
    out = shaped(shape, pieces[0].dtype)
    return pl.pallas_call(
        functools.partial(assemble_kernel, bits),
        out_shape=out,
        compiler_params=limited(),
        name="assemble",
        cost_estimate=brief(),
    )(*pieces)


def merge_weight_kernel(bits, *refs):
    pieces, (weight, encoded) = refs[:-2], refs[-2:]
    rows = weight.shape[0] // lax.axis_size("dp")
    sums = None
    for piece, place in placed((pieces, bits)):
        weight[pl.ds(pl.multiple_of(place * rows, rows), rows), :] = piece[:rows, :]
        sent = piece[rows:, :].astype(jnp.float32)
        sums = sent if sums is None else sums + sent
    width = weight.shape[1]
    for i in range(encoded.shape[1] // width):
        encoded[:, i * width : (i + 1) * width] = sums[i * PAD : (i + 1) * PAD]


def gather_merge(pieces, bits, rows, hidden):
    outs = (shaped((rows, pieces[0].shape[-1]), jnp.bfloat16), shaped((PAD, hidden), jnp.float32))
    return pl.pallas_call(
        functools.partial(merge_weight_kernel, bits),
        out_shape=outs,
        compiler_params=limited(),
        name="gather_merge",
        cost_estimate=brief(),
    )(*pieces)


def project_kernel(bits, tokens, norms, bias, *refs):
    pieces, (projected, attend, decoder) = refs[:-3], refs[-3:]
    assemble_into((attend, decoder), (pieces, bits))
    for start in range(0, tokens.shape[0], TILE):
        rows = slice(start, start + TILE)
        unit, _ = norm_parts(tokens[rows, :].astype(jnp.float32))
        normed = (unit * norms[0:1, :] + norms[1:2, :]).astype(jnp.bfloat16)
        for part in range(3):
            total = dot(normed, attend[part], NN) + bias[part : part + 1, :]
            projected[part, rows, :] = total.astype(jnp.bfloat16)


def project(tokens, norms, bias, gathered, hidden):
    pieces, bits = gathered
    rows, width = tokens.shape
    local = bias.shape[1]
    outs = (
        shaped((3, rows, local), jnp.bfloat16),
        shaped((3, width, local), jnp.bfloat16),
        shaped((2, hidden, local), jnp.bfloat16),
    )
    return pl.pallas_call(
        functools.partial(project_kernel, bits),
        out_shape=outs,
        compiler_params=limited(),
        name="project",
        cost_estimate=brief(),
    )(tokens, norms, bias, *pieces)


def down_kernel(bits, cotangent, *refs):
    pieces, (down, grad) = refs[:-2], refs[-2:]
    assemble_into((down,), (pieces, bits))
    for start in range(0, cotangent.shape[0], TILE):
        rows = slice(start, start + TILE)
        grad[rows, :] = dot(cotangent[rows, :], down[0], NN).astype(jnp.bfloat16)


def down_back(cotangent, gathered):
    pieces, bits = gathered
    rows, width = cotangent.shape
    units = pieces[0].shape[-1]
    outs = (shaped((1, width, units), jnp.bfloat16), shaped((rows, units), jnp.bfloat16))
    return pl.pallas_call(
        functools.partial(down_kernel, bits),
        out_shape=outs,
        compiler_params=limited(),
        name="down_back",
        cost_estimate=brief(),
    )(cotangent, *pieces)


def prefix_kernel(encoded, encoder_bias, decoder, decoder_bias, hidden, prefix):
    held = jnp.tanh(encoded[...] + encoder_bias[...])
    hidden[...] = held
    low = held.astype(jnp.bfloat16)
    for part in range(2):
        total = dot(low, decoder[part], NN) + decoder_bias[part : part + 1, :]
        prefix[part] = total.astype(jnp.bfloat16)


def attend_kernel(first, proj, prefix, mix, sums, mixed):
    rows, width = mix.shape
    lane = lax.broadcasted_iota(jnp.int32, (1, width), 1) // HD
    pre_col = lax.broadcasted_iota(jnp.int32, (TILE, PAD), 1)
    below = lax.broadcasted_iota(jnp.int32, (TILE, TILE), 0) >= lax.broadcasted_iota(
        jnp.int32, (TILE, TILE), 1
    )
    sum_col = lax.broadcasted_iota(jnp.int32, (TILE, 128), 1)
    sums[...] = jnp.zeros_like(sums)
    mixed[...] = jnp.zeros_like(mixed)

    def one_head(head, carry):
        mine = lane == head
        for start in range(first, first + rows, TILE):
            here = slice(start, start + TILE)
            there = slice(start - first, start - first + TILE)
            query = proj[0, here, :] * jnp.asarray(HD**-0.5, jnp.bfloat16)
            one = jnp.where(mine, query, jnp.zeros_like(query))
            scores = [
                jnp.where(pre_col < PRE, dot(one, prefix[0], NT), MASKED),
                jnp.where(below, dot(one, proj[1, here, :], NT), MASKED),
            ]
            values = [prefix[1], proj[2, here, :]]
            if start:
                scores.append(dot(one, proj[1, :start, :], NT))
                values.append(proj[2, :start, :])
            top = functools.reduce(jnp.maximum, [jnp.max(s, 1, keepdims=True) for s in scores])
            exps = [jnp.exp(s - top) for s in scores]
            total = sum(jnp.sum(e, 1, keepdims=True) for e in exps)
            inverse = 1.0 / total
            part = sum(
                dot((e * inverse).astype(jnp.bfloat16), v, NN)
                for e, v in zip(exps, values, strict=True)
            )
            mixed[there, :] = jnp.where(mine, part, mixed[there, :])
            sums[there, :] = jnp.where(sum_col == head, top + jnp.log(total), sums[there, :])
        return carry

    lax.fori_loop(0, width // HD, one_head, 0, unroll=2 if first else 1)
    mix[...] = mixed[...].astype(jnp.bfloat16)


def attend_first_kernel(proj, encoded, encoder_bias, decoder, decoder_bias, mix, sums, hidden, prefix, mixed):
    prefix_kernel(encoded, encoder_bias, decoder, decoder_bias, hidden, prefix)
    attend_kernel(0, proj, prefix, mix, sums, mixed)


def attend_shapes(proj):
    _, rows, width = proj.shape
    return shaped((rows // 2, width), jnp.bfloat16), shaped((rows // 2, 128), jnp.float32)


def attend_first(proj, encoded, encoder_bias, decoder, decoder_bias):
    _, rows, width = proj.shape
    outs = (
        *attend_shapes(proj),
        shaped(encoded.shape, jnp.float32),
        shaped((2, PAD, width), jnp.bfloat16),
    )
    return pl.pallas_call(
        attend_first_kernel,
        out_shape=outs,
        scratch_shapes=[pltpu.VMEM((rows // 2, width), jnp.float32)],
        compiler_params=limited(),
        name="attend_first",
        cost_estimate=brief(),
    )(proj, encoded, encoder_bias, decoder, decoder_bias)


def attend_second(proj, prefix):
    _, rows, width = proj.shape
    outs = attend_shapes(proj)
    return pl.pallas_call(
        functools.partial(attend_kernel, rows // 2),
        out_shape=outs,
        scratch_shapes=[pltpu.VMEM((rows // 2, width), jnp.float32)],
        compiler_params=limited(),
        name="attend_second",
        cost_estimate=brief(),
    )(proj, prefix)


def prefix_back_kernel(
    query, prefix, mix_first, mix_second, sums_first, sums_second, keep, side, core_keep, core_side, *refs
):
    gprefix, gmix, log_sums, inner, gquery = refs
    rows, width = gmix.shape
    half = rows // 2
    quarter = keep.shape[1]
    heads = width // HD
    me = lax.axis_index("tensor")
    for piece, bits in ((keep.at[0], OWN), (core_keep.at[1], CORE), (side.at[0], SIDE), (core_side.at[1], BOTH)):
        place = lax.bitwise_xor(me, bits) * quarter
        gmix[pl.ds(pl.multiple_of(place, quarter), quarter), :] = piece[...]
    head_of = lax.broadcasted_iota(jnp.int32, (8, width), 0) == lax.broadcasted_iota(
        jnp.int32, (8, width), 1
    ) // HD
    for i, (mix, sums) in enumerate(((mix_first, sums_first), (mix_second, sums_second))):
        part = slice(i * half, (i + 1) * half)
        log_sums[:, part] = sums[...].T[:8]
        product = gmix[part, :].astype(jnp.float32) * mix[...].astype(jnp.float32)
        inner[:, part] = dot(head_of.astype(jnp.float32), product, NT, lax.Precision.HIGHEST)
    lane = lax.broadcasted_iota(jnp.int32, (PAD, width), 1) // HD
    zero = jnp.zeros((PAD, width), jnp.bfloat16)
    keys, values = (
        jnp.concatenate([jnp.where(lane == head, prefix[i], zero) for head in range(heads)])
        for i in range(2)
    )
    scale = jnp.asarray(HD**-0.5, jnp.bfloat16)

    def spread(of_heads):
        return jnp.concatenate(
            [jnp.broadcast_to(of_heads[head : head + 1, :], (PAD, rows)) for head in range(heads)]
        )

    scaled = query[0] * scale
    grad = gmix[...]
    position = lax.broadcasted_iota(jnp.int32, (heads * PAD, rows), 0) % PAD
    scores = jnp.where(position < PRE, dot(keys, scaled, NT), MASKED)
    prob = jnp.exp(scores - spread(log_sums))
    dscore = (prob * (dot(values, grad, NT) - spread(inner))).astype(jnp.bfloat16)
    dkeys = dot(dscore, scaled, NN)
    dvalues = dot(prob.astype(jnp.bfloat16), grad, NN)
    for i, found in enumerate((dkeys, dvalues)):
        gprefix[i] = sum(
            jnp.where(lane == head, found[head * PAD : (head + 1) * PAD], 0.0)
            for head in range(heads)
        )
    gquery[...] = dot(keys * scale, dscore, TN)


def prefix_back(proj, prefix, mixes, sums, pieces):
    _, rows, width = proj.shape
    outs = (
        shaped(prefix.shape, jnp.float32),
        shaped((rows, width), jnp.bfloat16),
        shaped((8, rows), jnp.float32),
        shaped((8, rows), jnp.float32),
        shaped((width, rows), jnp.float32),
    )
    return pl.pallas_call(
        prefix_back_kernel,
        grid=(1,),
        in_specs=[pl.BlockSpec((1, rows, width), lambda i: (0, 0, 0))]
        + [whole_spec(a) for a in (prefix, *mixes, *sums, *pieces)],
        out_specs=[whole_spec(o) for o in outs],
        out_shape=outs,
        compiler_params=limited(),
        name="prefix_back",
        cost_estimate=brief(),
    )(proj, prefix, *mixes, *sums, *pieces)


def attend_back_kernel(pair, proj, gmix, log_sums, inner, gquery_prefix, gproj, gquery, gkey, gvalue, keys_col):
    rows, width = gmix.shape
    lane = lax.broadcasted_iota(jnp.int32, (1, width), 1) // HD
    seen = lax.broadcasted_iota(jnp.int32, (TILE, TILE), 0) <= lax.broadcasted_iota(
        jnp.int32, (TILE, TILE), 1
    )
    scale = jnp.asarray(HD**-0.5, jnp.bfloat16)
    keys_col[...] = (proj[1] * scale).T
    gkey[...] = jnp.zeros_like(gkey)
    gvalue[...] = jnp.zeros_like(gvalue)

    def one_head(head, carry):
        mine = lane == head
        cols = pl.ds(pl.multiple_of(head * HD, HD), HD)
        row = pl.ds(pair * (width // HD) + head, 1)
        for start in range(0, rows, TILE):
            here = slice(start, start + TILE)
            query = proj[0, here, :] * scale
            grad = gmix[here, :]
            one = jnp.where(mine, query, jnp.zeros_like(query))
            one_grad = jnp.where(mine, grad, jnp.zeros_like(grad))
            log_sum = log_sums[row, here]
            shared = inner[row, here]
            dquery = gquery_prefix[cols, here]
            for at in range(0, start + TILE, TILE):
                there = slice(at, at + TILE)
                scores = dot(proj[1, there, :], one, NT)
                if at == start:
                    scores = jnp.where(seen, scores, MASKED)
                prob = jnp.exp(scores - log_sum)
                dscore = prob * (dot(proj[2, there, :], one_grad, NT) - shared)
                dscore = dscore.astype(jnp.bfloat16)
                gkey[there, :] += dot(dscore, one, NN)
                gvalue[there, :] += dot(prob.astype(jnp.bfloat16), one_grad, NN)
                dquery = dquery + dot(keys_col[cols, there], dscore, NN)
            gquery[cols, here] = dquery
        return carry

    lax.fori_loop(0, width // HD, one_head, 0)
    gproj[0] = gquery[...].T.astype(jnp.bfloat16)
    gproj[1] = gkey[...].astype(jnp.bfloat16)
    gproj[2] = gvalue[...].astype(jnp.bfloat16)


def attend_back(pair, proj, gmix, log_sums, inner, gquery):
    _, rows, local = proj.shape
    width = 2 * HD
    out = shaped((3, rows, width), jnp.bfloat16)
    return pl.pallas_call(
        functools.partial(attend_back_kernel, pair),
        grid=(1,),
        in_specs=[
            pl.BlockSpec((3, rows, width), lambda i: (0, 0, pair)),
            pl.BlockSpec((rows, width), lambda i: (0, pair)),
            whole_spec(log_sums),
            whole_spec(inner),
            pl.BlockSpec((width, rows), lambda i: (pair, 0)),
        ],
        out_specs=whole_spec(out),
        out_shape=out,
        scratch_shapes=[
            pltpu.VMEM((width, rows), jnp.float32),
            pltpu.VMEM((rows, width), jnp.float32),
            pltpu.VMEM((rows, width), jnp.float32),
            pltpu.VMEM((width, rows), jnp.bfloat16),
        ],
        compiler_params=limited(),
        name="attend_back",
        cost_estimate=cost(12 * rows * rows * width, proj, gmix, gquery, out),
    )(proj, gmix, log_sums, inner, gquery)


def merge_kernel(first, tokens, norms, branch, *refs):
    mixes, merges, earlier, (normed, resid_own) = refs[:4], refs[4:8], refs[8:-2], refs[-2:]
    i = pl.program_id(0)
    merged = sum(dot(m[...], w[...], NT) for m, w in zip(mixes, merges, strict=True))
    resid = tokens[...].astype(jnp.float32) + merged + branch[0:1, :]
    unit, _ = norm_parts(resid)
    normed[...] = (unit * norms[2:3, :] + norms[3:4, :]).astype(jnp.bfloat16)
    if earlier:

        @pl.when(i == 0)
        def _():
            resid_own[...] = earlier[1][...]

    @pl.when(i + first == lax.axis_index("tensor"))
    def _():
        resid_own[...] = resid


def part_spec(shape, first):
    return pl.BlockSpec(shape, lambda i: (first // shape[0] + i, 0))


def fixed_spec(shape, first):
    return pl.BlockSpec(shape, lambda i: (first // shape[0], 0))


def merge_half(tokens, norms, branch, mixes, merges, earlier=()):
    rows, width = tokens.shape
    share = rows // lax.axis_size("tensor")
    local = mixes[0][0].shape[1]
    steps = rows // 2 // share
    first = steps if earlier else 0
    whole = lambda a: pl.BlockSpec(a.shape, lambda i: (0,) * a.ndim)
    outs = (shaped((rows, width), jnp.bfloat16), shaped((share, width), jnp.float32))
    return pl.pallas_call(
        functools.partial(merge_kernel, first),
        grid=(steps,),
        in_specs=[pl.BlockSpec((share, width), lambda i: (i + first, 0)), whole(norms), whole(branch)]
        + [part_spec((share, local), start) for _, start in mixes]
        + [fixed_spec((width, local), start) for _, start in merges]
        + ([pl.BlockSpec(memory_space=pl.ANY), whole(earlier[1])] if earlier else []),
        out_specs=(
            pl.BlockSpec((share, width), lambda i: (i + first, 0)),
            pl.BlockSpec((share, width), lambda i: (0, 0)),
        ),
        out_shape=outs,
        input_output_aliases={11: 0} if earlier else {},
        compiler_params=limited(),
        name="merge_second" if earlier else "merge_first",
        cost_estimate=brief(),
    )(tokens, norms, branch, *[a for a, _ in (*mixes, *merges)], *earlier)


def feed_rows(normed, ghidden, up, bias, act, part, plus=None):
    value = dot(normed[...], up, NN) + bias[...]
    square = value * value
    tanh = jnp.tanh(GELU_COEF * value * (1.0 + 0.044715 * square))
    act[...] = (0.5 * value * (1.0 + tanh)).astype(jnp.bfloat16)
    slope = 0.5 * (1.0 + tanh) + 0.5 * GELU_COEF * value * (1.0 - tanh * tanh) * (
        1.0 + 3.0 * 0.044715 * square
    )
    gpre = (ghidden[...].astype(jnp.float32) * slope).astype(jnp.bfloat16)
    total = dot(gpre, up, NT)
    if plus is not None:
        total = total + plus[...].astype(jnp.float32)
    part[...] = total.astype(jnp.bfloat16)


def feed_first_kernel(bits, normed, ghidden, bias, *refs):
    pieces, (act, part, up) = refs[:-3], refs[-3:]
    assemble_into((up,), (pieces, bits))
    feed_rows(normed, ghidden, up[0], bias, act, part)


def feed_kernel(up, bias, normed, ghidden, *refs):
    feed_rows(normed, ghidden, up[0], bias, *refs[-2:], *refs[:-2])


def block_of(*bits):
    last = len(bits) - 1
    return lambda i: (lax.bitwise_xor(lax.axis_index("tensor"), bits[0] if not last else last - i), 0)


def whole_spec(a):
    return pl.BlockSpec(a.shape, lambda i: (0,) * a.ndim)


def feed_first(bits, normed, ghidden, gathered, bias):
    pieces, places = gathered
    rows, width = normed.shape
    share = rows // lax.axis_size("tensor")
    units = pieces[0].shape[-1]
    outs = (
        shaped((share, units), jnp.bfloat16),
        shaped((share, width), jnp.bfloat16),
        shaped((1, width, units), jnp.bfloat16),
    )
    return pl.pallas_call(
        functools.partial(feed_first_kernel, places),
        grid=(1,),
        in_specs=[
            pl.BlockSpec((share, width), block_of(bits)),
            pl.BlockSpec((share, units), block_of(bits)),
            whole_spec(bias),
        ]
        + [whole_spec(p) for p in pieces],
        out_specs=[whole_spec(o) for o in outs],
        out_shape=outs,
        compiler_params=limited(),
        name="feed_first",
        cost_estimate=brief(),
    )(normed, ghidden, bias, *pieces)


def feed(differ, normed, ghidden, up, bias, *plus):
    rows, width = normed.shape
    share = rows // lax.axis_size("tensor")
    units = up.shape[-1]
    outs = (shaped((share, units), jnp.bfloat16), shaped((share, width), jnp.bfloat16))
    return pl.pallas_call(
        feed_kernel,
        grid=(1,),
        in_specs=[
            whole_spec(up),
            whole_spec(bias),
            pl.BlockSpec((share, width), block_of(differ)),
            pl.BlockSpec((share, units), block_of(differ)),
        ]
        + [whole_spec(p) for p in plus],
        out_specs=[whole_spec(o) for o in outs],
        out_shape=outs,
        compiler_params=limited(),
        name="feed",
        cost_estimate=brief(),
    )(up, bias, normed, ghidden, *plus)


def back_kernel(weight, one, two, *refs):
    total = sum(
        dot(jnp.concatenate([one[i], two[i]], axis=1), weight[i], NT) for i in range(weight.shape[0])
    )
    for plus in refs[:-1]:
        total = total + plus[...].astype(jnp.float32)
    refs[-1][...] = total.astype(jnp.bfloat16)


def project_back(bits, gprojs, attend, *plus):
    _, rows, local = gprojs[0].shape
    width = attend.shape[1]
    share = rows // lax.axis_size("tensor")
    steps = len(bits)
    block = block_of(*bits)
    out = shaped((steps * share, width), jnp.bfloat16)
    return pl.pallas_call(
        back_kernel,
        grid=(steps,),
        in_specs=[whole_spec(attend)]
        + [pl.BlockSpec((3, share, local), lambda i: (0, *block(i)))] * 2
        + [whole_spec(p) for p in plus],
        out_specs=pl.BlockSpec((share, width), lambda i: (i, 0)),
        out_shape=out,
        compiler_params=limited(),
        name="project_back",
        cost_estimate=brief(),
    )(attend, *gprojs, *plus)


def three(own, core, side):
    return own[...].astype(jnp.float32) + core[...].astype(jnp.float32) + side[...].astype(jnp.float32)


def middle_kernel(own, core, side, cotangent, resid, norms, *refs):
    merges, (gresid, keep, send) = refs[:4], refs[4:]
    total = three(own, core, side)
    grad = cotangent[...].astype(jnp.float32) + norm_back(resid[...], norms[2:3, :], total)
    gresid[...] = grad
    low = grad.astype(jnp.bfloat16)
    keep[0] = dot(low, merges[OWN][...], NN).astype(jnp.bfloat16)
    keep[1] = dot(low, merges[CORE][...], NN).astype(jnp.bfloat16)
    send[0] = dot(low, merges[SIDE][...], NN).astype(jnp.bfloat16)
    send[1] = dot(low, merges[BOTH][...], NN).astype(jnp.bfloat16)


def row_of(share, width, step):
    return pl.BlockSpec((share, width), lambda i: (step, 0))


def middle(own, core, side, cotangent, resid, norms, merges):
    share, width = resid.shape
    local = merges[0][0].shape[1]
    outs = (
        shaped((share, width), jnp.float32),
        shaped((2, share, local), jnp.bfloat16),
        shaped((2, share, local), jnp.bfloat16),
    )
    mine = pl.BlockSpec((share, width), block_of(OWN))
    return pl.pallas_call(
        middle_kernel,
        grid=(1,),
        in_specs=[whole_spec(own), whole_spec(core), whole_spec(side), mine]
        + [whole_spec(a) for a in (resid, norms)]
        + [fixed_spec((width, local), start) for _, start in merges],
        out_specs=[whole_spec(o) for o in outs],
        out_shape=outs,
        compiler_params=limited(),
        name="middle",
        cost_estimate=brief(),
    )(own, core, side, cotangent, resid, norms, *[a for a, _ in merges])


def last_kernel(own, core, side, tokens, gresid, norms, out):
    total = three(own, core, side)
    rows = tokens[...].astype(jnp.float32)
    out[...] = (gresid[...] + norm_back(rows, norms[0:1, :], total)).astype(jnp.bfloat16)


def last(own, core, side, tokens, gresid, norms):
    share, width = gresid.shape
    out = shaped((share, width), jnp.bfloat16)
    return pl.pallas_call(
        last_kernel,
        grid=(1,),
        in_specs=[
            row_of(share, width, 1),
            row_of(share, width, 0),
            whole_spec(side),
            pl.BlockSpec((share, width), block_of(OWN)),
            whole_spec(gresid),
            whole_spec(norms),
        ],
        out_specs=whole_spec(out),
        out_shape=out,
        compiler_params=limited(),
        name="last",
        cost_estimate=brief(),
    )(own, core, side, tokens, gresid, norms)


def plus_kernel(one, two, out):
    out[...] = one[...] + two[...]


def plus(one, two):
    return pl.pallas_call(
        plus_kernel,
        out_shape=shaped(one.shape, one.dtype),
        compiler_params=limited(),
        name="plus",
        cost_estimate=brief(),
    )(one, two)


def down_rows_kernel(act, down, *refs):
    total = dot(act[...], down[0], NT)
    for one in refs[:-1]:
        total = total + one[...].astype(jnp.float32)
    refs[-1][...] = total.astype(jnp.bfloat16)


def down_rows(act, down, *rest):
    return pl.pallas_call(
        down_rows_kernel,
        out_shape=shaped((act.shape[0], down.shape[1]), jnp.bfloat16),
        compiler_params=limited(),
        name="down_rows",
        cost_estimate=brief(),
    )(act, down, *rest)


def output_kernel(resid, own, core, side, branch, out):
    out[...] = (resid[...] + three(own, core, side) + branch[1:2, :]).astype(jnp.bfloat16)


def output_rows(resid, own, core, side, branch):
    return pl.pallas_call(
        output_kernel,
        out_shape=shaped(resid.shape, jnp.bfloat16),
        compiler_params=limited(),
        name="output",
        cost_estimate=brief(),
    )(resid, own, core, side, branch)


def tail_kernel(one, two, hidden, decoder, total, joint):
    total[...] = one[...] + two[...]
    low = total[...].astype(jnp.bfloat16)
    held = hidden[...].astype(jnp.bfloat16)
    part = jnp.zeros(joint.shape, jnp.float32)
    square = jnp.zeros((1, 1), jnp.float32)
    for i in range(2):
        part = part + dot(low[i], decoder[i], NT)
        grad = dot(held, low[i], TN)
        square = square + jnp.sum(jnp.sum(grad * grad, 0, keepdims=True), 1, keepdims=True)
        bias = jnp.sum(low[i].astype(jnp.float32), 0, keepdims=True)
        square = square + jnp.sum(bias * bias, 1, keepdims=True)
    row = lax.broadcasted_iota(jnp.int32, joint.shape, 0)
    joint[...] = jnp.where(row == PAD - 1, square, part)


def update_kernel(joint_one, joint_two, hidden, hidden_own, total, selected, selected_own, onehot, encoder, *refs):
    table, enc, enc_bias, dec, dec_bias = (refs[i : i + 3] for i in range(0, 15, 3))
    norm_out, outs = refs[15], refs[16:]
    held = hidden[...]
    row = lax.broadcasted_iota(jnp.int32, held.shape, 0)
    joint = joint_one[...] + joint_two[...]
    grad = jnp.where(row < PRE, joint, 0.0) * (1.0 - held * held)
    grad = grad.astype(jnp.bfloat16)
    square = joint[PAD - 1 : PAD, 0:1]

    def summed(values):
        return jnp.sum(jnp.sum(values * values, 0, keepdims=True), 1, keepdims=True)

    square = square + summed(dot(selected[...], grad, TN))
    grad_bias = jnp.sum(grad.astype(jnp.float32), 0, keepdims=True)
    square = square + summed(grad_bias)
    grad_selected = dot(grad, encoder[...], NT)
    grad_table = dot(onehot[...], grad_selected, TN, lax.Precision.HIGHEST)[:PRE]
    square = square + summed(grad_table)
    norm = jnp.sqrt(square)
    norm_out[...] = norm
    factor = CLIP_LIMIT / (norm + 1e-06)

    def update(old, grad_of, at, index):
        weight, first, second = (ref[index] for ref in old)
        for out, new in zip(
            outs[at : at + 3], adam_update(weight, grad_of, first, second, factor), strict=True
        ):
            out[index] = new

    update(table, grad_table, 0, ...)
    update(enc, dot(selected_own[...], grad, TN), 3, ...)
    update(enc_bias, grad_bias, 6, ...)
    low = total[...].astype(jnp.bfloat16)
    held_own = hidden_own[...].astype(jnp.bfloat16)
    for i in range(2):
        update(dec, dot(held_own, low[i], TN), 9, (slice(None), i, slice(None)))
        bias = jnp.sum(low[i].astype(jnp.float32), 0, keepdims=True)
        update(dec_bias, bias, 12, (slice(i, i + 1), slice(None)))


def on_device(
    tokens,
    cotangent,
    norm_params,
    attention_weight,
    attention_bias,
    merge_weight,
    branch_bias,
    up_weight,
    up_bias,
    down_weight,
    prefix_ids,
    prefix_table,
    encoder_weight,
    encoder_bias,
    decoder_weight,
    decoder_bias,
    first_table,
    second_table,
    first_encoder,
    second_encoder,
    first_encoder_bias,
    second_encoder_bias,
    first_decoder,
    second_decoder,
    first_decoder_bias,
    second_decoder_bias,
):
    highest = lax.Precision.HIGHEST
    dp_index = lax.axis_index("dp")
    rows, width = tokens.shape
    share = rows // lax.axis_size("tensor")
    local = merge_weight.shape[1]
    units = up_weight.shape[1]
    in_rows = attention_weight.shape[0]
    hidden_size = encoder_weight.shape[1]
    dec_rows = decoder_weight.shape[0]
    halves = hidden_size // local

    decoder_low = decoder_weight.astype(jnp.bfloat16)
    attention = jnp.concatenate(
        [
            attention_weight.transpose(1, 0, 2).reshape(3 * in_rows, local),
            decoder_low.transpose(1, 0, 2).reshape(2 * dec_rows, local),
        ]
    )
    onehot = (
        jnp.pad(prefix_ids, (0, PAD - PRE), constant_values=PAD)[:, None]
        == jnp.arange(PAD, dtype=jnp.int32)[None, :]
    ).astype(jnp.float32)
    selected = jnp.dot(onehot[:, :PRE], prefix_table, precision=highest).astype(jnp.bfloat16)
    selected_own = lax.dynamic_slice_in_dim(selected, dp_index * in_rows, in_rows, 1)
    encoder_low = encoder_weight.astype(jnp.bfloat16)
    encoded_own = jnp.dot(selected_own, encoder_low, preferred_element_type=jnp.float32)
    sent = encoded_own.astype(jnp.bfloat16).reshape(PAD, halves, local).transpose(1, 0, 2)
    merging = jnp.concatenate([merge_weight, sent.reshape(halves * PAD, local)])

    own_start = dp_index.astype(jnp.uint32) * dec_rows
    small = lax.axis_size("dp") == 8
    if small:
        y, z, far = 1, 2, 4
        attention_far = swap(attention, "dp", far)
        merging_side = swap(merging, "dp", y)[None]
        up_side = swap(up_weight, "dp", y)[None]
        attention_far, own_start = after((attention_far, own_start), merging_side, up_side)
        pair = jnp.stack([attention, attention_far])
        near = swap(pair, "dp", z)
        pair_side = swap(pair, "dp", y)
        merging_pair = joined(merging[None], merging_side)
        merging_far = swap(after(merging_pair, attention_far), "dp", far)
        near_side = swap(near, "dp", y)
        attention = ((pair, near, pair_side, near_side), ((0, 4), (2, 6), (1, 5), (3, 7)))
        merging_quad = joined(merging_pair, merging_far)
        merging_near = swap(merging_quad, "dp", z)
        merging = ((merging_quad, merging_near), ((0, 1, 4, 5), (2, 3, 6, 7)))
        down_far = swap(after(down_weight, near), "dp", far)[None]
    else:
        gathered = lambda shard: ((lax.all_gather(shard, "dp", axis=0),), None)
        attention, merging, down, up, encoder = map(
            gathered, (attention, merging, down_weight, up_weight, encoder_low)
        )

    projected, attend_full, decoder_full = project(
        tokens, norm_params, attention_bias, attention, hidden_size
    )
    if small:
        down_far = after(down_far, projected)
        down_pair = joined(down_weight[None], down_far)
        down_near = swap(down_pair, "dp", z)
        down_pair_side = swap(down_pair, "dp", y)
        up_far = swap(after(up_weight, down_far), "dp", far)[None]
    pieces, places = merging
    pieces = after(pieces, projected)
    if small:
        pieces = after(pieces, down_far)
    merge_own, encoded = gather_merge(pieces, places, width, hidden_size)
    mix_first, sums_first, hidden, prefix = attend_first(
        projected, encoded, encoder_bias[None], decoder_full, decoder_bias
    )

    merge_side = after(swap(merge_own, "tensor", SIDE), mix_first)
    if small:
        up_far = after(up_far, mix_first)
        up_far_side = swap(up_far, "dp", y)
        merge_side, up_far_side, down_near, down_pair_side = after(
            (merge_side, up_far_side, down_near, down_pair_side)
        )
    mix_side = swap(mix_first, "tensor", SIDE)
    half = rows // 2
    both_cores = joined(merge_own, merge_side, mix_first, mix_side)
    both_cores = swap(both_cores, "tensor", CORE)
    merges = ((merge_own, 0), (both_cores, 0), (merge_side, 0), (both_cores, width))
    mixes_first = (
        (mix_first, 0),
        (both_cores, 2 * width),
        (mix_side, 0),
        (both_cores, 2 * width + half),
    )
    proj_late = projected
    if small:
        proj_late = after(projected, down_near)
        down_near_side = swap(down_near, "dp", y)
        up_near = swap(joined(up_weight[None], up_far), "dp", z)
    mix_second, sums_second = attend_second(proj_late, prefix)
    mix_side = swap(mix_second, "tensor", SIDE)
    branch_late = branch_bias
    if small:
        branch_late, down_near_side, up_near, mix_side = after(
            (branch_bias, down_near_side, up_near, mix_side), mix_second
        )
        down = (
            (down_pair, down_pair_side, down_near, down_near_side),
            ((0, 4), (1, 5), (2, 6), (3, 7)),
        )
        up_near_side = swap(up_near, "dp", y)
    first_half = merge_half(tokens, norm_params, branch_late, mixes_first, merges)
    mix_cores = swap(joined(mix_second, mix_side), "tensor", CORE)
    mixes_second = ((mix_second, 0), (mix_cores, 0), (mix_side, 0), (mix_cores, half))
    down_full, grad_hidden = down_back(after(cotangent, first_half), down)
    branch_late = after(branch_bias, grad_hidden)
    if small:
        encoder_far = swap(after(encoder_low, first_half), "dp", far)
        up = (
            (up_weight[None], up_side, up_far, up_far_side, up_near, up_near_side),
            ((0,), (1,), (4,), (5,), (2, 6), (3, 7)),
        )
    normed, resid = merge_half(
        tokens, norm_params, branch_late, mixes_second, merges, after(first_half, grad_hidden)
    )
    def branch(act, *rest):
        return down_rows(act, down_full, *rest)

    bias = up_bias[None]
    if small:
        normed = after(normed, encoder_far)
    act_both, up_both, up_full = feed_first(BOTH, normed, grad_hidden, up, bias)
    up_both = swap(up_both, "tensor", CORE)
    if small:
        encoder_pair = jnp.stack([encoder_low, after(encoder_far, act_both)])
        encoder_near = swap(encoder_pair, "dp", z)
    act_side, up_send = feed(SIDE, normed, grad_hidden, up_full, bias, up_both)
    up_from = swap(up_send, "tensor", SIDE)
    act_core, up_core = feed(CORE, after(normed, up_send), grad_hidden, up_full, bias)
    up_core = swap(up_core, "tensor", CORE)
    act_own, up_own = feed(OWN, after(normed, act_core), grad_hidden, up_full, bias)
    out_both = branch(after(act_both, act_own))
    out_core = branch(after(act_core, act_own))
    out_own = branch(act_own)
    up_from = after(up_from, out_both, out_core, out_own)
    if small:
        encoder_near = after(encoder_near, act_own)
        encoder_quad = joined(encoder_pair, encoder_near)
        encoder_side = swap(encoder_quad, "dp", y)
        encoder = ((encoder_quad, encoder_side), ((0, 4, 2, 6), (1, 5, 3, 7)))
        up_from = after(up_from, encoder_near)
    grad_resid, keep, send = middle(up_own, up_core, up_from, cotangent, resid, norm_params, merges)
    out_both = swap(out_both, "tensor", CORE)
    from_side = swap(send, "tensor", SIDE)
    core_keep = swap(keep, "tensor", CORE)
    out_core = swap(out_core, "tensor", CORE)
    out_send = branch(after(act_side, send), out_both)
    out_from = swap(out_send, "tensor", SIDE)
    encoder_full = assemble((after(encoder[0], send), encoder[1]), (1, width, hidden_size))
    hidden_own = lax.dynamic_slice(
        after(hidden, send), (jnp.uint32(0), own_start), (hidden.shape[0], dec_rows)
    )
    from_side = after(from_side, out_send, encoder_full, hidden_own)
    core_side = swap(from_side, "tensor", CORE)
    grad_prefix, grad_mix, log_sums, inner, grad_query = prefix_back(
        projected,
        prefix,
        (mix_first, mix_second),
        (sums_first, sums_second),
        (keep, from_side, core_keep, core_side),
    )
    grad_first = attend_back(0, projected, grad_mix, log_sums, inner, grad_query)
    prefix_total = plus(grad_prefix, swap(grad_prefix, "dp", 1))
    grad_second = attend_back(
        1, projected, after(grad_mix, prefix_total), log_sums, inner, grad_query
    )
    prefix_total = plus(prefix_total, swap(prefix_total, "dp", 2))
    gprojs = after((grad_first, grad_second), prefix_total, out_from, out_core)
    back_both = swap(project_back((BOTH,), gprojs, attend_full), "tensor", CORE)
    back_rest = project_back((CORE, OWN), gprojs, attend_full)
    back_both = after(back_both, back_rest)
    back_send = project_back((SIDE,), gprojs, attend_full, back_both)
    back_from = swap(back_send, "tensor", SIDE)
    bits = 4
    while bits < lax.axis_size("dp") // 2:
        prefix_total = plus(prefix_total, swap(prefix_total, "dp", bits))
        bits *= 2
    prefix_rest = after(swap(prefix_total, "dp", bits), back_send)
    prefix_total, joint = pl.pallas_call(
        tail_kernel,
        out_shape=(
            shaped(grad_prefix.shape, jnp.float32),
            shaped((PAD, hidden_size), jnp.float32),
        ),
        compiler_params=limited(),
        name="tail",
        cost_estimate=brief(),
    )(prefix_total, prefix_rest, hidden, decoder_full)
    joint = plus(joint, swap(joint, "tensor", CORE))
    joint_side = swap(joint, "tensor", SIDE)
    back_core = swap(back_rest, "tensor", CORE)
    output = output_rows(resid, out_own, out_core, out_from, branch_bias)
    input_grad = last(back_rest, back_core, back_from, tokens, grad_resid, norm_params)
    joint_side = after(joint_side, input_grad)

    params = [
        (prefix_table, first_table, second_table),
        (encoder_weight, first_encoder, second_encoder),
        (encoder_bias[None], first_encoder_bias[None], second_encoder_bias[None]),
        (decoder_weight, first_decoder, second_decoder),
        (decoder_bias, first_decoder_bias, second_decoder_bias),
    ]
    params = [array for group in params for array in group]
    grad_norm, *new = pl.pallas_call(
        update_kernel,
        out_shape=[shaped((1, 1), jnp.float32)] + [shaped(p.shape, p.dtype) for p in params],
        compiler_params=limited(),
        name="update",
    )(
        joint,
        joint_side,
        hidden,
        hidden_own,
        prefix_total,
        selected,
        selected_own,
        onehot,
        encoder_full[0],
        *params,
    )
    for i in range(6, 9):
        new[i] = new[i][0]
    return (output, input_grad, grad_norm[0, 0], *new)


def solution(mesh):
    in_specs = (
        P("dp", None),
        P("dp", None),
        P(),
        P("dp", None, "tensor"),
        P(None, "tensor"),
        P("dp", "tensor"),
        P(),
        P("dp", "tensor"),
        P("tensor"),
        P("dp", "tensor"),
        P(),
        P(),
        P("dp", None),
        P(),
        P("dp", None, "tensor"),
        P(None, "tensor"),
        P(),
        P(),
        P("dp", None),
        P("dp", None),
        P(),
        P(),
        P("dp", None, "tensor"),
        P("dp", None, "tensor"),
        P(None, "tensor"),
        P(None, "tensor"),
    )
    out_specs = (
        P(("dp", "tensor"), None),
        P(("dp", "tensor"), None),
        P(),
        P(),
        P(),
        P(),
        P("dp", None),
        P("dp", None),
        P("dp", None),
        P(),
        P(),
        P(),
        P("dp", None, "tensor"),
        P("dp", None, "tensor"),
        P("dp", None, "tensor"),
        P(None, "tensor"),
        P(None, "tensor"),
        P(None, "tensor"),
    )
    return jax.shard_map(
        on_device, mesh=mesh, in_specs=in_specs, out_specs=out_specs, check_vma=False
    )
```

```python
import functools

import jax
import jax.numpy as jnp
from jax import lax
from jax.experimental import pallas as pl
from jax.experimental.pallas import tpu as pltpu
from jax.sharding import PartitionSpec as P

HD = 64
PRE = 10
PAD = 16
STEP = 10
TILE = 256


NORM_EPS = 1e-05
CLIP_LIMIT = 0.001
LEARN_RATE = 0.05
WEIGHT_DECAY = 0.01
BETA_FIRST = 0.9
BETA_SECOND = 0.999
ADAM_EPS = 1e-08
MASKED = -1e30
GELU_COEF = 0.7978845608028654

NN = ((1,), (0,))
NT = ((1,), (1,))
TN = ((0,), (0,))
OWN, CORE, SIDE, BOTH = 0, 1, 2, 3


def dot(left, right, dims, precision=None):
    return lax.dot_general(
        left, right, (dims, ((), ())), precision=precision, preferred_element_type=jnp.float32
    )


def shaped(shape, dtype):
    return jax.ShapeDtypeStruct(shape, dtype)


def limited():
    return pltpu.CompilerParams(vmem_limit_bytes=24 * 2**20)


def cost(flops, *arrays):
    size = sum(a.size * a.dtype.itemsize for a in arrays)
    return pl.CostEstimate(flops=flops, transcendentals=0, bytes_accessed=size)


def brief():
    return pl.CostEstimate(flops=0, transcendentals=0, bytes_accessed=0)


def norm_parts(rows):
    offsets = rows - jnp.mean(rows, axis=-1, keepdims=True)
    scale = lax.rsqrt(jnp.mean(offsets * offsets, axis=-1, keepdims=True) + NORM_EPS)
    return offsets * scale, scale


def norm_back(rows, gain, grad):
    unit, scale = norm_parts(rows)
    grad = grad * gain
    mean = jnp.mean(grad, axis=-1, keepdims=True)
    along = jnp.mean(grad * unit, axis=-1, keepdims=True)
    return scale * (grad - mean - unit * along)


def adam_update(weight, grad, first, second, factor):
    clipped = grad * factor
    new_first = BETA_FIRST * first + (1.0 - BETA_FIRST) * clipped
    new_second = BETA_SECOND * second + (1.0 - BETA_SECOND) * clipped * clipped
    fix_first = 1.0 - BETA_FIRST**STEP
    fix_second = 1.0 - BETA_SECOND**STEP
    new_weight = weight * (1.0 - LEARN_RATE * WEIGHT_DECAY) - LEARN_RATE * (
        new_first / fix_first
    ) / (jnp.sqrt(new_second / fix_second) + ADAM_EPS)
    return (new_weight, new_first, new_second)


def swap(values, axis, bits):
    size = lax.axis_size(axis)
    return lax.ppermute(values, axis, [(i, i ^ bits) for i in range(size)])


def after(values, *others):
    return lax.optimization_barrier((values, *others))[0]


def placed(found):
    refs, bits = found
    if bits is None:
        return [(refs[0].at[i], i) for i in range(refs[0].shape[0])]
    here = lax.axis_index("dp")
    return [
        (ref.at[i], lax.bitwise_xor(here, differ))
        for ref, group in zip(refs, bits, strict=True)
        for i, differ in enumerate(group)
    ]


def joined(*pieces):
    return jnp.concatenate(pieces)


def sum_over(values, axis):
    bits = 1
    while bits < lax.axis_size(axis):
        values = values + swap(values, axis, bits)
        bits *= 2
    return values


def assemble_into(outs, found):
    for piece, place in placed(found):
        start = 0
        for out in outs:
            parts, rows = out.shape[0], out.shape[1] // lax.axis_size("dp")
            for part in range(parts):
                where = pl.ds(pl.multiple_of(place * rows, rows), rows)
                out[part, where, :] = piece[start : start + rows, :]
                start += rows


def assemble_kernel(bits, *refs):
    assemble_into(refs[-1:], (refs[:-1], bits))


def assemble(gathered, shape):
    pieces, bits = gathered
    out = shaped(shape, pieces[0].dtype)
    return pl.pallas_call(
        functools.partial(assemble_kernel, bits),
        out_shape=out,
        compiler_params=limited(),
        name="assemble",
        cost_estimate=brief(),
    )(*pieces)


def merge_weight_kernel(bits, *refs):
    pieces, (weight, encoded) = refs[:-2], refs[-2:]
    rows = weight.shape[0] // lax.axis_size("dp")
    sums = None
    for piece, place in placed((pieces, bits)):
        weight[pl.ds(pl.multiple_of(place * rows, rows), rows), :] = piece[:rows, :]
        sent = piece[rows:, :].astype(jnp.float32)
        sums = sent if sums is None else sums + sent
    width = weight.shape[1]
    for i in range(encoded.shape[1] // width):
        encoded[:, i * width : (i + 1) * width] = sums[i * PAD : (i + 1) * PAD]


def gather_merge(pieces, bits, rows, hidden):
    outs = (shaped((rows, pieces[0].shape[-1]), jnp.bfloat16), shaped((PAD, hidden), jnp.float32))
    return pl.pallas_call(
        functools.partial(merge_weight_kernel, bits),
        out_shape=outs,
        compiler_params=limited(),
        name="gather_merge",
        cost_estimate=brief(),
    )(*pieces)


def project_kernel(bits, tokens, norms, bias, *refs):
    pieces, (projected, attend, decoder) = refs[:-3], refs[-3:]
    assemble_into((attend, decoder), (pieces, bits))
    for start in range(0, tokens.shape[0], TILE):
        rows = slice(start, start + TILE)
        unit, _ = norm_parts(tokens[rows, :].astype(jnp.float32))
        normed = (unit * norms[0:1, :] + norms[1:2, :]).astype(jnp.bfloat16)
        for part in range(3):
            total = dot(normed, attend[part], NN) + bias[part : part + 1, :]
            projected[part, rows, :] = total.astype(jnp.bfloat16)


def project(tokens, norms, bias, gathered, hidden):
    pieces, bits = gathered
    rows, width = tokens.shape
    local = bias.shape[1]
    outs = (
        shaped((3, rows, local), jnp.bfloat16),
        shaped((3, width, local), jnp.bfloat16),
        shaped((2, hidden, local), jnp.bfloat16),
    )
    return pl.pallas_call(
        functools.partial(project_kernel, bits),
        out_shape=outs,
        compiler_params=limited(),
        name="project",
        cost_estimate=brief(),
    )(tokens, norms, bias, *pieces)


def down_kernel(bits, cotangent, *refs):
    pieces, (down, grad) = refs[:-2], refs[-2:]
    assemble_into((down,), (pieces, bits))
    for start in range(0, cotangent.shape[0], TILE):
        rows = slice(start, start + TILE)
        grad[rows, :] = dot(cotangent[rows, :], down[0], NN).astype(jnp.bfloat16)


def down_back(cotangent, gathered):
    pieces, bits = gathered
    rows, width = cotangent.shape
    units = pieces[0].shape[-1]
    outs = (shaped((1, width, units), jnp.bfloat16), shaped((rows, units), jnp.bfloat16))
    return pl.pallas_call(
        functools.partial(down_kernel, bits),
        out_shape=outs,
        compiler_params=limited(),
        name="down_back",
        cost_estimate=brief(),
    )(cotangent, *pieces)


def prefix_kernel(encoded, encoder_bias, decoder, decoder_bias, hidden, prefix):
    held = jnp.tanh(encoded[...] + encoder_bias[...])
    hidden[...] = held
    low = held.astype(jnp.bfloat16)
    for part in range(2):
        total = dot(low, decoder[part], NN) + decoder_bias[part : part + 1, :]
        prefix[part] = total.astype(jnp.bfloat16)


def attend_kernel(first, proj, prefix, mix, sums, mixed):
    rows, width = mix.shape
    lane = lax.broadcasted_iota(jnp.int32, (1, width), 1) // HD
    pre_col = lax.broadcasted_iota(jnp.int32, (TILE, PAD), 1)
    below = lax.broadcasted_iota(jnp.int32, (TILE, TILE), 0) >= lax.broadcasted_iota(
        jnp.int32, (TILE, TILE), 1
    )
    sum_col = lax.broadcasted_iota(jnp.int32, (TILE, 128), 1)
    sums[...] = jnp.zeros_like(sums)
    mixed[...] = jnp.zeros_like(mixed)

    def one_head(head, carry):
        mine = lane == head
        for start in range(first, first + rows, TILE):
            here = slice(start, start + TILE)
            there = slice(start - first, start - first + TILE)
            query = proj[0, here, :] * jnp.asarray(HD**-0.5, jnp.bfloat16)
            one = jnp.where(mine, query, jnp.zeros_like(query))
            scores = [
                jnp.where(pre_col < PRE, dot(one, prefix[0], NT), MASKED),
                jnp.where(below, dot(one, proj[1, here, :], NT), MASKED),
            ]
            values = [prefix[1], proj[2, here, :]]
            if start:
                scores.append(dot(one, proj[1, :start, :], NT))
                values.append(proj[2, :start, :])
            top = functools.reduce(jnp.maximum, [jnp.max(s, 1, keepdims=True) for s in scores])
            exps = [jnp.exp(s - top) for s in scores]
            total = sum(jnp.sum(e, 1, keepdims=True) for e in exps)
            inverse = 1.0 / total
            part = sum(
                dot((e * inverse).astype(jnp.bfloat16), v, NN)
                for e, v in zip(exps, values, strict=True)
            )
            mixed[there, :] = jnp.where(mine, part, mixed[there, :])
            sums[there, :] = jnp.where(sum_col == head, top + jnp.log(total), sums[there, :])
        return carry

    lax.fori_loop(0, width // HD, one_head, 0, unroll=2 if first else 1)
    mix[...] = mixed[...].astype(jnp.bfloat16)


def attend_first_kernel(proj, encoded, encoder_bias, decoder, decoder_bias, mix, sums, hidden, prefix, mixed):
    prefix_kernel(encoded, encoder_bias, decoder, decoder_bias, hidden, prefix)
    attend_kernel(0, proj, prefix, mix, sums, mixed)


def attend_shapes(proj):
    _, rows, width = proj.shape
    return shaped((rows // 2, width), jnp.bfloat16), shaped((rows // 2, 128), jnp.float32)


def attend_first(proj, encoded, encoder_bias, decoder, decoder_bias):
    _, rows, width = proj.shape
    outs = (
        *attend_shapes(proj),
        shaped(encoded.shape, jnp.float32),
        shaped((2, PAD, width), jnp.bfloat16),
    )
    return pl.pallas_call(
        attend_first_kernel,
        out_shape=outs,
        scratch_shapes=[pltpu.VMEM((rows // 2, width), jnp.float32)],
        compiler_params=limited(),
        name="attend_first",
        cost_estimate=brief(),
    )(proj, encoded, encoder_bias, decoder, decoder_bias)


def attend_second(proj, prefix):
    _, rows, width = proj.shape
    outs = attend_shapes(proj)
    return pl.pallas_call(
        functools.partial(attend_kernel, rows // 2),
        out_shape=outs,
        scratch_shapes=[pltpu.VMEM((rows // 2, width), jnp.float32)],
        compiler_params=limited(),
        name="attend_second",
        cost_estimate=brief(),
    )(proj, prefix)


def prefix_back_kernel(
    query, prefix, mix_first, mix_second, sums_first, sums_second, keep, side, core_keep, core_side, *refs
):
    gprefix, gmix, log_sums, inner, gquery = refs
    rows, width = gmix.shape
    half = rows // 2
    quarter = keep.shape[1]
    heads = width // HD
    me = lax.axis_index("tensor")
    for piece, bits in ((keep.at[0], OWN), (core_keep.at[1], CORE), (side.at[0], SIDE), (core_side.at[1], BOTH)):
        place = lax.bitwise_xor(me, bits) * quarter
        gmix[pl.ds(pl.multiple_of(place, quarter), quarter), :] = piece[...]
    head_of = lax.broadcasted_iota(jnp.int32, (8, width), 0) == lax.broadcasted_iota(
        jnp.int32, (8, width), 1
    ) // HD
    for i, (mix, sums) in enumerate(((mix_first, sums_first), (mix_second, sums_second))):
        part = slice(i * half, (i + 1) * half)
        log_sums[:, part] = sums[...].T[:8]
        product = gmix[part, :].astype(jnp.float32) * mix[...].astype(jnp.float32)
        inner[:, part] = dot(head_of.astype(jnp.float32), product, NT, lax.Precision.HIGHEST)
    lane = lax.broadcasted_iota(jnp.int32, (PAD, width), 1) // HD
    zero = jnp.zeros((PAD, width), jnp.bfloat16)
    keys, values = (
        jnp.concatenate([jnp.where(lane == head, prefix[i], zero) for head in range(heads)])
        for i in range(2)
    )
    scale = jnp.asarray(HD**-0.5, jnp.bfloat16)

    def spread(of_heads):
        return jnp.concatenate(
            [jnp.broadcast_to(of_heads[head : head + 1, :], (PAD, rows)) for head in range(heads)]
        )

    scaled = query[0] * scale
    grad = gmix[...]
    position = lax.broadcasted_iota(jnp.int32, (heads * PAD, rows), 0) % PAD
    scores = jnp.where(position < PRE, dot(keys, scaled, NT), MASKED)
    prob = jnp.exp(scores - spread(log_sums))
    dscore = (prob * (dot(values, grad, NT) - spread(inner))).astype(jnp.bfloat16)
    dkeys = dot(dscore, scaled, NN)
    dvalues = dot(prob.astype(jnp.bfloat16), grad, NN)
    for i, found in enumerate((dkeys, dvalues)):
        gprefix[i] = sum(
            jnp.where(lane == head, found[head * PAD : (head + 1) * PAD], 0.0)
            for head in range(heads)
        )
    gquery[...] = dot(keys * scale, dscore, TN)


def prefix_back(proj, prefix, mixes, sums, pieces):
    _, rows, width = proj.shape
    outs = (
        shaped(prefix.shape, jnp.float32),
        shaped((rows, width), jnp.bfloat16),
        shaped((8, rows), jnp.float32),
        shaped((8, rows), jnp.float32),
        shaped((width, rows), jnp.float32),
    )
    return pl.pallas_call(
        prefix_back_kernel,
        grid=(1,),
        in_specs=[pl.BlockSpec((1, rows, width), lambda i: (0, 0, 0))]
        + [whole_spec(a) for a in (prefix, *mixes, *sums, *pieces)],
        out_specs=[whole_spec(o) for o in outs],
        out_shape=outs,
        compiler_params=limited(),
        name="prefix_back",
        cost_estimate=brief(),
    )(proj, prefix, *mixes, *sums, *pieces)


def attend_back_kernel(pair, proj, gmix, log_sums, inner, gquery_prefix, gproj, gquery, gkey, gvalue, keys_col):
    rows, width = gmix.shape
    lane = lax.broadcasted_iota(jnp.int32, (1, width), 1) // HD
    seen = lax.broadcasted_iota(jnp.int32, (TILE, TILE), 0) <= lax.broadcasted_iota(
        jnp.int32, (TILE, TILE), 1
    )
    scale = jnp.asarray(HD**-0.5, jnp.bfloat16)
    keys_col[...] = (proj[1] * scale).T
    gkey[...] = jnp.zeros_like(gkey)
    gvalue[...] = jnp.zeros_like(gvalue)

    def one_head(head, carry):
        mine = lane == head
        cols = pl.ds(pl.multiple_of(head * HD, HD), HD)
        row = pl.ds(pair * (width // HD) + head, 1)
        for start in range(0, rows, TILE):
            here = slice(start, start + TILE)
            query = proj[0, here, :] * scale
            grad = gmix[here, :]
            one = jnp.where(mine, query, jnp.zeros_like(query))
            one_grad = jnp.where(mine, grad, jnp.zeros_like(grad))
            log_sum = log_sums[row, here]
            shared = inner[row, here]
            dquery = gquery_prefix[cols, here]
            for at in range(0, start + TILE, TILE):
                there = slice(at, at + TILE)
                scores = dot(proj[1, there, :], one, NT)
                if at == start:
                    scores = jnp.where(seen, scores, MASKED)
                prob = jnp.exp(scores - log_sum)
                dscore = prob * (dot(proj[2, there, :], one_grad, NT) - shared)
                dscore = dscore.astype(jnp.bfloat16)
                gkey[there, :] += dot(dscore, one, NN)
                gvalue[there, :] += dot(prob.astype(jnp.bfloat16), one_grad, NN)
                dquery = dquery + dot(keys_col[cols, there], dscore, NN)
            gquery[cols, here] = dquery
        return carry

    lax.fori_loop(0, width // HD, one_head, 0)
    gproj[0] = gquery[...].T.astype(jnp.bfloat16)
    gproj[1] = gkey[...].astype(jnp.bfloat16)
    gproj[2] = gvalue[...].astype(jnp.bfloat16)


def attend_back(pair, proj, gmix, log_sums, inner, gquery):
    _, rows, local = proj.shape
    width = 2 * HD
    out = shaped((3, rows, width), jnp.bfloat16)
    return pl.pallas_call(
        functools.partial(attend_back_kernel, pair),
        grid=(1,),
        in_specs=[
            pl.BlockSpec((3, rows, width), lambda i: (0, 0, pair)),
            pl.BlockSpec((rows, width), lambda i: (0, pair)),
            whole_spec(log_sums),
            whole_spec(inner),
            pl.BlockSpec((width, rows), lambda i: (pair, 0)),
        ],
        out_specs=whole_spec(out),
        out_shape=out,
        scratch_shapes=[
            pltpu.VMEM((width, rows), jnp.float32),
            pltpu.VMEM((rows, width), jnp.float32),
            pltpu.VMEM((rows, width), jnp.float32),
            pltpu.VMEM((width, rows), jnp.bfloat16),
        ],
        compiler_params=limited(),
        name="attend_back",
        cost_estimate=cost(12 * rows * rows * width, proj, gmix, gquery, out),
    )(proj, gmix, log_sums, inner, gquery)


def merge_kernel(first, tokens, norms, branch, *refs):
    mixes, merges, earlier, (normed, resid_own) = refs[:4], refs[4:8], refs[8:-2], refs[-2:]
    i = pl.program_id(0)
    merged = sum(dot(m[...], w[...], NT) for m, w in zip(mixes, merges, strict=True))
    resid = tokens[...].astype(jnp.float32) + merged + branch[0:1, :]
    unit, _ = norm_parts(resid)
    normed[...] = (unit * norms[2:3, :] + norms[3:4, :]).astype(jnp.bfloat16)
    if earlier:

        @pl.when(i == 0)
        def _():
            resid_own[...] = earlier[1][...]

    @pl.when(i + first == lax.axis_index("tensor"))
    def _():
        resid_own[...] = resid


def part_spec(shape, first):
    return pl.BlockSpec(shape, lambda i: (first // shape[0] + i, 0))


def fixed_spec(shape, first):
    return pl.BlockSpec(shape, lambda i: (first // shape[0], 0))


def merge_half(tokens, norms, branch, mixes, merges, earlier=()):
    rows, width = tokens.shape
    share = rows // lax.axis_size("tensor")
    local = mixes[0][0].shape[1]
    steps = rows // 2 // share
    first = steps if earlier else 0
    whole = lambda a: pl.BlockSpec(a.shape, lambda i: (0,) * a.ndim)
    outs = (shaped((rows, width), jnp.bfloat16), shaped((share, width), jnp.float32))
    return pl.pallas_call(
        functools.partial(merge_kernel, first),
        grid=(steps,),
        in_specs=[pl.BlockSpec((share, width), lambda i: (i + first, 0)), whole(norms), whole(branch)]
        + [part_spec((share, local), start) for _, start in mixes]
        + [fixed_spec((width, local), start) for _, start in merges]
        + ([pl.BlockSpec(memory_space=pl.ANY), whole(earlier[1])] if earlier else []),
        out_specs=(
            pl.BlockSpec((share, width), lambda i: (i + first, 0)),
            pl.BlockSpec((share, width), lambda i: (0, 0)),
        ),
        out_shape=outs,
        input_output_aliases={11: 0} if earlier else {},
        compiler_params=limited(),
        name="merge_second" if earlier else "merge_first",
        cost_estimate=brief(),
    )(tokens, norms, branch, *[a for a, _ in (*mixes, *merges)], *earlier)


def feed_rows(normed, ghidden, up, bias, act, part, plus=None):
    value = dot(normed[...], up, NN) + bias[...]
    square = value * value
    tanh = jnp.tanh(GELU_COEF * value * (1.0 + 0.044715 * square))
    act[...] = (0.5 * value * (1.0 + tanh)).astype(jnp.bfloat16)
    slope = 0.5 * (1.0 + tanh) + 0.5 * GELU_COEF * value * (1.0 - tanh * tanh) * (
        1.0 + 3.0 * 0.044715 * square
    )
    gpre = (ghidden[...].astype(jnp.float32) * slope).astype(jnp.bfloat16)
    total = dot(gpre, up, NT)
    if plus is not None:
        total = total + plus[...].astype(jnp.float32)
    part[...] = total.astype(jnp.bfloat16)


def feed_first_kernel(bits, normed, ghidden, bias, *refs):
    pieces, (act, part, up) = refs[:-3], refs[-3:]
    assemble_into((up,), (pieces, bits))
    feed_rows(normed, ghidden, up[0], bias, act, part)


def feed_kernel(up, bias, normed, ghidden, *refs):
    feed_rows(normed, ghidden, up[0], bias, *refs[-2:], *refs[:-2])


def block_of(*bits):
    last = len(bits) - 1
    return lambda i: (lax.bitwise_xor(lax.axis_index("tensor"), bits[0] if not last else last - i), 0)


def whole_spec(a):
    return pl.BlockSpec(a.shape, lambda i: (0,) * a.ndim)


def feed_first(bits, normed, ghidden, gathered, bias):
    pieces, places = gathered
    rows, width = normed.shape
    share = rows // lax.axis_size("tensor")
    units = pieces[0].shape[-1]
    outs = (
        shaped((share, units), jnp.bfloat16),
        shaped((share, width), jnp.bfloat16),
        shaped((1, width, units), jnp.bfloat16),
    )
    return pl.pallas_call(
        functools.partial(feed_first_kernel, places),
        grid=(1,),
        in_specs=[
            pl.BlockSpec((share, width), block_of(bits)),
            pl.BlockSpec((share, units), block_of(bits)),
            whole_spec(bias),
        ]
        + [whole_spec(p) for p in pieces],
        out_specs=[whole_spec(o) for o in outs],
        out_shape=outs,
        compiler_params=limited(),
        name="feed_first",
        cost_estimate=brief(),
    )(normed, ghidden, bias, *pieces)


def feed(differ, normed, ghidden, up, bias, *plus):
    rows, width = normed.shape
    share = rows // lax.axis_size("tensor")
    units = up.shape[-1]
    outs = (shaped((share, units), jnp.bfloat16), shaped((share, width), jnp.bfloat16))
    return pl.pallas_call(
        feed_kernel,
        grid=(1,),
        in_specs=[
            whole_spec(up),
            whole_spec(bias),
            pl.BlockSpec((share, width), block_of(differ)),
            pl.BlockSpec((share, units), block_of(differ)),
        ]
        + [whole_spec(p) for p in plus],
        out_specs=[whole_spec(o) for o in outs],
        out_shape=outs,
        compiler_params=limited(),
        name="feed",
        cost_estimate=brief(),
    )(up, bias, normed, ghidden, *plus)


def back_kernel(weight, one, two, *refs):
    total = sum(
        dot(jnp.concatenate([one[i], two[i]], axis=1), weight[i], NT) for i in range(weight.shape[0])
    )
    for plus in refs[:-1]:
        total = total + plus[...].astype(jnp.float32)
    refs[-1][...] = total.astype(jnp.bfloat16)


def project_back(bits, gprojs, attend, *plus):
    _, rows, local = gprojs[0].shape
    width = attend.shape[1]
    share = rows // lax.axis_size("tensor")
    steps = len(bits)
    block = block_of(*bits)
    out = shaped((steps * share, width), jnp.bfloat16)
    return pl.pallas_call(
        back_kernel,
        grid=(steps,),
        in_specs=[whole_spec(attend)]
        + [pl.BlockSpec((3, share, local), lambda i: (0, *block(i)))] * 2
        + [whole_spec(p) for p in plus],
        out_specs=pl.BlockSpec((share, width), lambda i: (i, 0)),
        out_shape=out,
        compiler_params=limited(),
        name="project_back",
        cost_estimate=brief(),
    )(attend, *gprojs, *plus)


def three(own, core, side):
    return own[...].astype(jnp.float32) + core[...].astype(jnp.float32) + side[...].astype(jnp.float32)


def middle_kernel(own, core, side, cotangent, resid, norms, *refs):
    merges, (gresid, keep, send) = refs[:4], refs[4:]
    total = three(own, core, side)
    grad = cotangent[...].astype(jnp.float32) + norm_back(resid[...], norms[2:3, :], total)
    gresid[...] = grad
    low = grad.astype(jnp.bfloat16)
    keep[0] = dot(low, merges[OWN][...], NN).astype(jnp.bfloat16)
    keep[1] = dot(low, merges[CORE][...], NN).astype(jnp.bfloat16)
    send[0] = dot(low, merges[SIDE][...], NN).astype(jnp.bfloat16)
    send[1] = dot(low, merges[BOTH][...], NN).astype(jnp.bfloat16)


def row_of(share, width, step):
    return pl.BlockSpec((share, width), lambda i: (step, 0))


def middle(own, core, side, cotangent, resid, norms, merges):
    share, width = resid.shape
    local = merges[0][0].shape[1]
    outs = (
        shaped((share, width), jnp.float32),
        shaped((2, share, local), jnp.bfloat16),
        shaped((2, share, local), jnp.bfloat16),
    )
    mine = pl.BlockSpec((share, width), block_of(OWN))
    return pl.pallas_call(
        middle_kernel,
        grid=(1,),
        in_specs=[whole_spec(own), whole_spec(core), whole_spec(side), mine]
        + [whole_spec(a) for a in (resid, norms)]
        + [fixed_spec((width, local), start) for _, start in merges],
        out_specs=[whole_spec(o) for o in outs],
        out_shape=outs,
        compiler_params=limited(),
        name="middle",
        cost_estimate=brief(),
    )(own, core, side, cotangent, resid, norms, *[a for a, _ in merges])


def last_kernel(own, core, side, tokens, gresid, norms, out):
    total = three(own, core, side)
    rows = tokens[...].astype(jnp.float32)
    out[...] = (gresid[...] + norm_back(rows, norms[0:1, :], total)).astype(jnp.bfloat16)


def last(own, core, side, tokens, gresid, norms):
    share, width = gresid.shape
    out = shaped((share, width), jnp.bfloat16)
    return pl.pallas_call(
        last_kernel,
        grid=(1,),
        in_specs=[
            row_of(share, width, 1),
            row_of(share, width, 0),
            whole_spec(side),
            pl.BlockSpec((share, width), block_of(OWN)),
            whole_spec(gresid),
            whole_spec(norms),
        ],
        out_specs=whole_spec(out),
        out_shape=out,
        compiler_params=limited(),
        name="last",
        cost_estimate=brief(),
    )(own, core, side, tokens, gresid, norms)


def plus_kernel(one, two, out):
    out[...] = one[...] + two[...]


def plus(one, two):
    return pl.pallas_call(
        plus_kernel,
        out_shape=shaped(one.shape, one.dtype),
        compiler_params=limited(),
        name="plus",
        cost_estimate=brief(),
    )(one, two)


def down_rows_kernel(act, down, *refs):
    total = dot(act[...], down[0], NT)
    for one in refs[:-1]:
        total = total + one[...].astype(jnp.float32)
    refs[-1][...] = total.astype(jnp.bfloat16)


def down_rows(act, down, *rest):
    return pl.pallas_call(
        down_rows_kernel,
        out_shape=shaped((act.shape[0], down.shape[1]), jnp.bfloat16),
        compiler_params=limited(),
        name="down_rows",
        cost_estimate=brief(),
    )(act, down, *rest)


def output_kernel(resid, own, core, side, branch, out):
    out[...] = (resid[...] + three(own, core, side) + branch[1:2, :]).astype(jnp.bfloat16)


def output_rows(resid, own, core, side, branch):
    return pl.pallas_call(
        output_kernel,
        out_shape=shaped(resid.shape, jnp.bfloat16),
        compiler_params=limited(),
        name="output",
        cost_estimate=brief(),
    )(resid, own, core, side, branch)


def tail_kernel(one, two, hidden, decoder, total, joint):
    total[...] = one[...] + two[...]
    low = total[...].astype(jnp.bfloat16)
    held = hidden[...].astype(jnp.bfloat16)
    part = jnp.zeros(joint.shape, jnp.float32)
    square = jnp.zeros((1, 1), jnp.float32)
    for i in range(2):
        part = part + dot(low[i], decoder[i], NT)
        grad = dot(held, low[i], TN)
        square = square + jnp.sum(jnp.sum(grad * grad, 0, keepdims=True), 1, keepdims=True)
        bias = jnp.sum(low[i].astype(jnp.float32), 0, keepdims=True)
        square = square + jnp.sum(bias * bias, 1, keepdims=True)
    row = lax.broadcasted_iota(jnp.int32, joint.shape, 0)
    joint[...] = jnp.where(row == PAD - 1, square, part)


def update_kernel(joint_one, joint_two, hidden, hidden_own, total, selected, selected_own, onehot, encoder, *refs):
    table, enc, enc_bias, dec, dec_bias = (refs[i : i + 3] for i in range(0, 15, 3))
    norm_out, outs = refs[15], refs[16:]
    held = hidden[...]
    row = lax.broadcasted_iota(jnp.int32, held.shape, 0)
    joint = joint_one[...] + joint_two[...]
    grad = jnp.where(row < PRE, joint, 0.0) * (1.0 - held * held)
    grad = grad.astype(jnp.bfloat16)
    square = joint[PAD - 1 : PAD, 0:1]

    def summed(values):
        return jnp.sum(jnp.sum(values * values, 0, keepdims=True), 1, keepdims=True)

    square = square + summed(dot(selected[...], grad, TN))
    grad_bias = jnp.sum(grad.astype(jnp.float32), 0, keepdims=True)
    square = square + summed(grad_bias)
    grad_selected = dot(grad, encoder[...], NT)
    grad_table = dot(onehot[...], grad_selected, TN, lax.Precision.HIGHEST)[:PRE]
    square = square + summed(grad_table)
    norm = jnp.sqrt(square)
    norm_out[...] = norm
    factor = CLIP_LIMIT / (norm + 1e-06)

    def update(old, grad_of, at, index):
        weight, first, second = (ref[index] for ref in old)
        for out, new in zip(
            outs[at : at + 3], adam_update(weight, grad_of, first, second, factor), strict=True
        ):
            out[index] = new

    update(table, grad_table, 0, ...)
    update(enc, dot(selected_own[...], grad, TN), 3, ...)
    update(enc_bias, grad_bias, 6, ...)
    low = total[...].astype(jnp.bfloat16)
    held_own = hidden_own[...].astype(jnp.bfloat16)
    for i in range(2):
        update(dec, dot(held_own, low[i], TN), 9, (slice(None), i, slice(None)))
        bias = jnp.sum(low[i].astype(jnp.float32), 0, keepdims=True)
        update(dec_bias, bias, 12, (slice(i, i + 1), slice(None)))


def on_device(
    tokens,
    cotangent,
    norm_params,
    attention_weight,
    attention_bias,
    merge_weight,
    branch_bias,
    up_weight,
    up_bias,
    down_weight,
    prefix_ids,
    prefix_table,
    encoder_weight,
    encoder_bias,
    decoder_weight,
    decoder_bias,
    first_table,
    second_table,
    first_encoder,
    second_encoder,
    first_encoder_bias,
    second_encoder_bias,
    first_decoder,
    second_decoder,
    first_decoder_bias,
    second_decoder_bias,
):
    highest = lax.Precision.HIGHEST
    dp_index = lax.axis_index("dp")
    rows, width = tokens.shape
    share = rows // lax.axis_size("tensor")
    local = merge_weight.shape[1]
    units = up_weight.shape[1]
    in_rows = attention_weight.shape[0]
    hidden_size = encoder_weight.shape[1]
    dec_rows = decoder_weight.shape[0]
    halves = hidden_size // local

    decoder_low = decoder_weight.astype(jnp.bfloat16)
    attention = jnp.concatenate(
        [
            attention_weight.transpose(1, 0, 2).reshape(3 * in_rows, local),
            decoder_low.transpose(1, 0, 2).reshape(2 * dec_rows, local),
        ]
    )
    onehot = (
        jnp.pad(prefix_ids, (0, PAD - PRE), constant_values=PAD)[:, None]
        == jnp.arange(PAD, dtype=jnp.int32)[None, :]
    ).astype(jnp.float32)
    selected = jnp.dot(onehot[:, :PRE], prefix_table, precision=highest).astype(jnp.bfloat16)
    selected_own = lax.dynamic_slice_in_dim(selected, dp_index * in_rows, in_rows, 1)
    encoder_low = encoder_weight.astype(jnp.bfloat16)
    encoded_own = jnp.dot(selected_own, encoder_low, preferred_element_type=jnp.float32)
    sent = encoded_own.astype(jnp.bfloat16).reshape(PAD, halves, local).transpose(1, 0, 2)
    merging = jnp.concatenate([merge_weight, sent.reshape(halves * PAD, local)])

    own_start = dp_index.astype(jnp.uint32) * dec_rows
    small = lax.axis_size("dp") == 8
    if small:
        y, z, far = 1, 2, 4
        attention_far = swap(attention, "dp", far)
        merging_side = swap(merging, "dp", y)[None]
        up_side = swap(up_weight, "dp", y)[None]
        attention_far, own_start = after((attention_far, own_start), merging_side, up_side)
        pair = jnp.stack([attention, attention_far])
        near = swap(pair, "dp", z)
        pair_side = swap(pair, "dp", y)
        merging_pair = joined(merging[None], merging_side)
        merging_far = swap(after(merging_pair, attention_far), "dp", far)
        near_side = swap(near, "dp", y)
        attention = ((pair, near, pair_side, near_side), ((0, 4), (2, 6), (1, 5), (3, 7)))
        merging_quad = joined(merging_pair, merging_far)
        merging_near = swap(merging_quad, "dp", z)
        merging = ((merging_quad, merging_near), ((0, 1, 4, 5), (2, 3, 6, 7)))
        down_far = swap(after(down_weight, near), "dp", far)[None]
    else:
        gathered = lambda shard: ((lax.all_gather(shard, "dp", axis=0),), None)
        attention, merging, down, up, encoder = map(
            gathered, (attention, merging, down_weight, up_weight, encoder_low)
        )

    projected, attend_full, decoder_full = project(
        tokens, norm_params, attention_bias, attention, hidden_size
    )
    if small:
        down_far = after(down_far, projected)
        down_pair = joined(down_weight[None], down_far)
        down_near = swap(down_pair, "dp", z)
        down_pair_side = swap(down_pair, "dp", y)
        up_far = swap(after(up_weight, down_far), "dp", far)[None]
    pieces, places = merging
    pieces = after(pieces, projected)
    if small:
        pieces = after(pieces, down_far)
    merge_own, encoded = gather_merge(pieces, places, width, hidden_size)
    mix_first, sums_first, hidden, prefix = attend_first(
        projected, encoded, encoder_bias[None], decoder_full, decoder_bias
    )

    merge_side = after(swap(merge_own, "tensor", SIDE), mix_first)
    if small:
        up_far = after(up_far, mix_first)
        up_far_side = swap(up_far, "dp", y)
        merge_side, up_far_side, down_near, down_pair_side = after(
            (merge_side, up_far_side, down_near, down_pair_side)
        )
    mix_side = swap(mix_first, "tensor", SIDE)
    half = rows // 2
    both_cores = joined(merge_own, merge_side, mix_first, mix_side)
    both_cores = swap(both_cores, "tensor", CORE)
    merges = ((merge_own, 0), (both_cores, 0), (merge_side, 0), (both_cores, width))
    mixes_first = (
        (mix_first, 0),
        (both_cores, 2 * width),
        (mix_side, 0),
        (both_cores, 2 * width + half),
    )
    proj_late = projected
    if small:
        proj_late = after(projected, down_near)
        down_near_side = swap(down_near, "dp", y)
        up_near = swap(joined(up_weight[None], up_far), "dp", z)
    mix_second, sums_second = attend_second(proj_late, prefix)
    mix_side = swap(mix_second, "tensor", SIDE)
    branch_late = branch_bias
    if small:
        branch_late, down_near_side, up_near, mix_side = after(
            (branch_bias, down_near_side, up_near, mix_side), mix_second
        )
        down = (
            (down_pair, down_pair_side, down_near, down_near_side),
            ((0, 4), (1, 5), (2, 6), (3, 7)),
        )
        up_near_side = swap(up_near, "dp", y)
    first_half = merge_half(tokens, norm_params, branch_late, mixes_first, merges)
    mix_cores = swap(joined(mix_second, mix_side), "tensor", CORE)
    mixes_second = ((mix_second, 0), (mix_cores, 0), (mix_side, 0), (mix_cores, half))
    down_full, grad_hidden = down_back(after(cotangent, first_half), down)
    branch_late = after(branch_bias, grad_hidden)
    if small:
        encoder_far = swap(after(encoder_low, first_half), "dp", far)
        up = (
            (up_weight[None], up_side, up_far, up_far_side, up_near, up_near_side),
            ((0,), (1,), (4,), (5,), (2, 6), (3, 7)),
        )
    normed, resid = merge_half(
        tokens, norm_params, branch_late, mixes_second, merges, after(first_half, grad_hidden)
    )
    def branch(act, *rest):
        return down_rows(act, down_full, *rest)

    bias = up_bias[None]
    if small:
        normed = after(normed, encoder_far)
    act_both, up_both, up_full = feed_first(BOTH, normed, grad_hidden, up, bias)
    up_both = swap(up_both, "tensor", CORE)
    if small:
        encoder_pair = jnp.stack([encoder_low, after(encoder_far, act_both)])
        encoder_near = swap(encoder_pair, "dp", z)
    act_side, up_send = feed(SIDE, normed, grad_hidden, up_full, bias, up_both)
    up_from = swap(up_send, "tensor", SIDE)
    act_core, up_core = feed(CORE, after(normed, up_send), grad_hidden, up_full, bias)
    up_core = swap(up_core, "tensor", CORE)
    act_own, up_own = feed(OWN, after(normed, act_core), grad_hidden, up_full, bias)
    out_both = branch(after(act_both, act_own))
    out_core = branch(after(act_core, act_own))
    out_own = branch(act_own)
    up_from = after(up_from, out_both, out_core, out_own)
    if small:
        encoder_near = after(encoder_near, act_own)
        encoder_quad = joined(encoder_pair, encoder_near)
        encoder_side = swap(encoder_quad, "dp", y)
        encoder = ((encoder_quad, encoder_side), ((0, 4, 2, 6), (1, 5, 3, 7)))
        up_from = after(up_from, encoder_near)
    grad_resid, keep, send = middle(up_own, up_core, up_from, cotangent, resid, norm_params, merges)
    out_both = swap(out_both, "tensor", CORE)
    from_side = swap(send, "tensor", SIDE)
    core_keep = swap(keep, "tensor", CORE)
    out_core = swap(out_core, "tensor", CORE)
    out_send = branch(after(act_side, send), out_both)
    out_from = swap(out_send, "tensor", SIDE)
    encoder_full = assemble((after(encoder[0], send), encoder[1]), (1, width, hidden_size))
    hidden_own = lax.dynamic_slice(
        after(hidden, send), (jnp.uint32(0), own_start), (hidden.shape[0], dec_rows)
    )
    from_side = after(from_side, out_send, encoder_full, hidden_own)
    core_side = swap(from_side, "tensor", CORE)
    grad_prefix, grad_mix, log_sums, inner, grad_query = prefix_back(
        projected,
        prefix,
        (mix_first, mix_second),
        (sums_first, sums_second),
        (keep, from_side, core_keep, core_side),
    )
    grad_first = attend_back(0, projected, grad_mix, log_sums, inner, grad_query)
    prefix_total = plus(grad_prefix, swap(grad_prefix, "dp", 1))
    grad_second = attend_back(
        1, projected, after(grad_mix, prefix_total), log_sums, inner, grad_query
    )
    gprojs = after((grad_first, grad_second), out_from, out_core)
    back_both = swap(project_back((BOTH,), gprojs, attend_full), "tensor", CORE)
    back_rest = project_back((CORE, OWN), gprojs, attend_full)
    back_both = after(back_both, back_rest)
    back_send = project_back((SIDE,), gprojs, attend_full, back_both)
    back_from = swap(back_send, "tensor", SIDE)
    prefix_total = plus(prefix_total, after(swap(prefix_total, "dp", 2), back_send))
    bits = 4
    while bits < lax.axis_size("dp") // 2:
        prefix_total = plus(prefix_total, swap(prefix_total, "dp", bits))
        bits *= 2
    prefix_rest = swap(prefix_total, "dp", bits)
    prefix_total, joint = pl.pallas_call(
        tail_kernel,
        out_shape=(
            shaped(grad_prefix.shape, jnp.float32),
            shaped((PAD, hidden_size), jnp.float32),
        ),
        compiler_params=limited(),
        name="tail",
        cost_estimate=brief(),
    )(prefix_total, prefix_rest, hidden, decoder_full)
    joint = plus(joint, swap(joint, "tensor", CORE))
    joint_side = swap(joint, "tensor", SIDE)
    back_core = swap(back_rest, "tensor", CORE)
    output = output_rows(resid, out_own, out_core, out_from, branch_bias)
    input_grad = last(back_rest, back_core, back_from, tokens, grad_resid, norm_params)
    joint_side = after(joint_side, input_grad)

    params = [
        (prefix_table, first_table, second_table),
        (encoder_weight, first_encoder, second_encoder),
        (encoder_bias[None], first_encoder_bias[None], second_encoder_bias[None]),
        (decoder_weight, first_decoder, second_decoder),
        (decoder_bias, first_decoder_bias, second_decoder_bias),
    ]
    params = [array for group in params for array in group]
    grad_norm, *new = pl.pallas_call(
        update_kernel,
        out_shape=[shaped((1, 1), jnp.float32)] + [shaped(p.shape, p.dtype) for p in params],
        compiler_params=limited(),
        name="update",
    )(
        joint,
        joint_side,
        hidden,
        hidden_own,
        prefix_total,
        selected,
        selected_own,
        onehot,
        encoder_full[0],
        *params,
    )
    for i in range(6, 9):
        new[i] = new[i][0]
    return (output, input_grad, grad_norm[0, 0], *new)


def solution(mesh):
    in_specs = (
        P("dp", None),
        P("dp", None),
        P(),
        P("dp", None, "tensor"),
        P(None, "tensor"),
        P("dp", "tensor"),
        P(),
        P("dp", "tensor"),
        P("tensor"),
        P("dp", "tensor"),
        P(),
        P(),
        P("dp", None),
        P(),
        P("dp", None, "tensor"),
        P(None, "tensor"),
        P(),
        P(),
        P("dp", None),
        P("dp", None),
        P(),
        P(),
        P("dp", None, "tensor"),
        P("dp", None, "tensor"),
        P(None, "tensor"),
        P(None, "tensor"),
    )
    out_specs = (
        P(("dp", "tensor"), None),
        P(("dp", "tensor"), None),
        P(),
        P(),
        P(),
        P(),
        P("dp", None),
        P("dp", None),
        P("dp", None),
        P(),
        P(),
        P(),
        P("dp", None, "tensor"),
        P("dp", None, "tensor"),
        P("dp", None, "tensor"),
        P(None, "tensor"),
        P(None, "tensor"),
        P(None, "tensor"),
    )
    return jax.shard_map(
        on_device, mesh=mesh, in_specs=in_specs, out_specs=out_specs, check_vma=False
    )
```
